256 devices in a mesh: cuts: 64 (over y, x, z_lo, core), grp: 4 (over z_hi).
Axes of the slice: x: 4, y: 4, z: 8 (z_hi: 4, z_lo: 2; z = z_hi * 2 + z_lo), core: 2. Of those that a mesh axis runs over, the one named last changes fastest.
Arguments:
- boundary: float32 [32, 2, 32, 32, 32], P('grp'), may hold values from -12 to 12
- gate_stack: float32 [3, 2, 1024, 1024], P(None, None, 'cuts'), may hold values from -0.125 to 0.125
- layer_order: int32 [3], replicated, may hold values from 0 to 2, each once
- cut_index: int32 [6, 3], replicated, may hold values from 0 to 4, as said below
- slice_bits: int32 [64, 6], P('cuts'), may hold values 0 or 1
- bitstrings: int32 [64, 20], replicated, may hold values 0 or 1
Outputs:
- amplitudes: float32 [64, 2], replicated
The draws below stay inside these ranges and needn't reach their ends.
Inputs may be any that keep to these rules, and one draw needn't show every extreme that they name: Each row of cut_index is (layer 0 to 2, group 0 to 3, bit 0 to 4); no two rows are equal. Rows of slice_bits need not differ.
All inputs are finite; a program needn't handle non-finite values.
Results may differ from the reference program's by a relative error of at most 0.0003.
Values sent between devices are 32-bit elements.
No kernel may reach another device: no remote copies, remote signals or barrier semaphores. Data moves between devices by JAX's collectives and lax.ppermute only.
A program may use at most 320 MiB of HBM per device.

```python
import jax
import jax.numpy as jnp
from jax import lax

GROUP_BITS = 5
GROUP = 32
PAIR = 1024
QUBITS = 20
LAYERS = 3
CUT_COUNT = 6
BITSTRINGS = 64
SLICES = 64


def draw_cut_index(key, part):
    per_layer = 4 * GROUP_BITS
    pool_size = LAYERS * per_layer
    chosen = jax.random.permutation(key, pool_size)[:CUT_COUNT].astype(jnp.int32)
    layer_part = chosen // per_layer
    group_part = chosen % per_layer // GROUP_BITS
    bit_part = chosen % GROUP_BITS
    return jnp.stack((layer_part, group_part, bit_part), axis=1).astype(jnp.int32)


def set_ends(array, key, smallest, high):
    longest = array.shape.index(max(array.shape))
    spots = []
    for shift in (0, 1):
        where = [jax.random.randint(jax.random.fold_in(key, axis), (), 0, length) for axis, length in enumerate(array.shape)]
        where[longest] = (where[longest] + shift) % array.shape[longest]
        spots.append(tuple(where))
    return array.at[spots[0]].set(smallest).at[spots[1]].set(high)


def steps_of(own_key, shape, pieces, low, largest):
    gain, own = 1.0, jax.random.fold_in(own_key, 6)
    for dim, shards_of in pieces:
        steps = jnp.exp(jax.random.uniform(jax.random.fold_in(own, dim), (shards_of,), jnp.float32, low / len(pieces), largest / len(pieces)))
        gain = gain * jnp.repeat(steps, shape[dim] // shards_of).reshape([-1 if axis == dim else 1 for axis in range(len(shape))])
    return gain


def gaussian(rng, shape, spread, reach, shards=(), kind=jnp.bfloat16):
    array = spread * jax.random.normal(rng, shape, jnp.float32)
    if shards:
        array = array * steps_of(rng, shape, shards, -0.22, 0.18)
    return jnp.clip(array, -reach, reach).astype(kind)


def setup_inputs(seed: int = 0) -> dict:
    keys = jax.random.split(jax.random.key(seed), 7)
    return {
        "boundary": gaussian(keys[0], (GROUP, 2, GROUP, GROUP, GROUP), 2.0, 12.0, ((0, 4),), jnp.float32),
        "gate_stack": gaussian(keys[1], (LAYERS, 2, PAIR, PAIR), (2 * PAIR) ** -0.5, 0.125, ((2, 64),), jnp.float32),
        "layer_order": jax.random.permutation(keys[2], LAYERS).astype(jnp.int32),
        "cut_index": draw_cut_index(jax.random.fold_in(keys[6], 71), 0),
        "slice_bits": set_ends((jax.random.randint(keys[4], (SLICES, CUT_COUNT), 0, 2) < 1).astype(jnp.int32), jax.random.fold_in(keys[4], 1), 0, 1),
        "bitstrings": set_ends((jax.random.randint(keys[5], (BITSTRINGS, QUBITS), 0, 2) < 1).astype(jnp.int32), jax.random.fold_in(keys[5], 1), 0, 1),
    }


LAYER_KINDS = (0, 1, 2, 3, 2, 3, 0, 1)
PAIR_GROUPS = ((0, 1), (2, 3), (1, 2), (1, 3))
FULL_PRECISION = lax.Precision.HIGHEST


def slice_factors(cut_index, slice_bits, layer_id, group_id, extent, offset):
    positions = offset + jnp.arange(extent, dtype=jnp.int32)
    active = jnp.logical_and(cut_index[:, 0] == layer_id, cut_index[:, 1] == group_id)
    bit_values = jnp.right_shift(positions[:, None], cut_index[None, :, 2]) & 1
    agrees = bit_values[None, :, :] == slice_bits[:, None, :]
    kept = jnp.logical_or(agrees, jnp.logical_not(active)[None, None, :])
    return jnp.all(kept, axis=2).astype(jnp.float32)


def group_digits(bitstrings, group_bits):
    weights = jnp.left_shift(jnp.ones((group_bits,), jnp.int32), jnp.arange(group_bits, dtype=jnp.int32))
    return [jnp.sum(bitstrings[:, group_id * group_bits:(group_id + 1) * group_bits] * weights, axis=1).astype(jnp.int32) for group_id in range(4)]


def apply_gate(current, layer_gate, first_group, second_group):
    aligned = jnp.moveaxis(current, (1 + first_group, 1 + second_group), (1, 2))
    full_shape = aligned.shape
    matrix = aligned.reshape(2, full_shape[1] * full_shape[2], -1)
    real_part = jnp.dot(layer_gate[0], matrix[0], precision=FULL_PRECISION, preferred_element_type=jnp.float32) - jnp.dot(layer_gate[1], matrix[1], precision=FULL_PRECISION, preferred_element_type=jnp.float32)
    imag_part = jnp.dot(layer_gate[0], matrix[1], precision=FULL_PRECISION, preferred_element_type=jnp.float32) + jnp.dot(layer_gate[1], matrix[0], precision=FULL_PRECISION, preferred_element_type=jnp.float32)
    updated = jnp.stack((real_part, imag_part)).reshape(full_shape)
    return jnp.moveaxis(updated, (1, 2), (1 + first_group, 1 + second_group))


def reference(boundary, gate_stack, layer_order, cut_index, slice_bits, bitstrings):
    initial = jnp.moveaxis(boundary, 1, 0)
    digits = group_digits(bitstrings, GROUP_BITS)

    def add_slice(running, bits_row):
        current = initial
        for layer_id in range(LAYERS):
            first_group, second_group = PAIR_GROUPS[LAYER_KINDS[layer_id % 8]]
            layer_gate = gate_stack[layer_order[layer_id]]
            current = apply_gate(current, layer_gate, first_group, second_group)
            for group_id in range(4):
                factor = slice_factors(cut_index, bits_row[None, :], layer_id, group_id, GROUP, 0)[0]
                target_shape = tuple(GROUP if position == 1 + group_id else 1 for position in range(5))
                current = current * factor.reshape(target_shape)
        amplitude = current[:, digits[0], digits[1], digits[2], digits[3]]
        return running + amplitude.T, None

    running, leftover = lax.scan(add_slice, jnp.zeros((BITSTRINGS, 2), jnp.float32), slice_bits)
    return running
```

```python
from functools import partial

import jax
import jax.numpy as jnp
from jax import lax
from jax.experimental import pallas as pl
from jax.experimental.pallas import tpu as pltpu
from jax.sharding import Mesh
from jax.sharding import PartitionSpec as P

AXES = (4, 4, 2, 2)
CUTS = ("cuts_0", "cuts_1", "cuts_2", "cuts_3")
PLANE = ("cuts_0", "cuts_1")
COLUMN = ("cuts_2", "cuts_3", "grp")

BLOCKS_I, BLOCKS_J = 8, 8
LANES = 128
ROW_SECOND, ROW_THIRD, ROW_FIRST, ROW_BITS, PIECE = 0, 32, 64, 68, 72


def split_high_low(array):
    high = array.astype(jnp.bfloat16)
    return high, (array - high.astype(jnp.float32)).astype(jnp.bfloat16)


def dot(left, right):
    return jnp.dot(left, right, preferred_element_type=jnp.float32)


def pack_kernel(order_ref, bits_ref, gate_ref, boundary_ref, piece_ref, left_ref):
    step = pl.program_id(0)

    @pl.when(step == 0)
    def _():
        first, second, third = order_ref[0], order_ref[1], order_ref[2]
        member = lax.axis_index("grp")
        columns = pl.ds(pl.multiple_of(member * 256, 256), 256)
        real, imag = gate_ref[first, 0, :, columns], gate_ref[first, 1, :, columns]

        def interleaved(even, odd):
            parts = []
            for k0 in range(8):
                parts += [even[:, 32 * k0 : 32 * k0 + 32], odd[:, 32 * k0 : 32 * k0 + 32]]
            return jnp.concatenate(parts, axis=1)

        to_real, to_imag = interleaved(real, -imag), interleaved(imag, real)
        rows = []
        for block in range(BLOCKS_I):
            rows += [to_real[2 * block : 2 * block + 2], to_imag[2 * block : 2 * block + 2]]
        left = jnp.concatenate(rows, axis=0)
        high, low = split_high_low(left)
        left_ref[...] = jnp.concatenate((high, low), axis=0)

        lane = lax.broadcasted_iota(jnp.int32, (1, LANES), 1)
        bits = jnp.zeros((1, LANES), jnp.float32)
        for cut in range(6):
            bits = jnp.where(lane == cut, bits_ref[0, cut].astype(jnp.float32), bits)
        for part in range(2):
            at = 16 * part
            for block_j in range(BLOCKS_J):
                value = gate_ref[second, part, :, LANES * block_j : LANES * block_j + LANES]
                for block_i in range(BLOCKS_I):
                    to = block_i * BLOCKS_J + block_j
                    piece_ref[to, ROW_SECOND + at : ROW_SECOND + at + 16, :] = value
            whole = gate_ref[third, part]
            for block_i in range(BLOCKS_I):
                value = jnp.concatenate(
                    (
                        whole[:, 64 * block_i : 64 * block_i + 64],
                        whole[:, 512 + 64 * block_i : 512 + 64 * block_i + 64],
                    ),
                    axis=1,
                )
                for block_j in range(BLOCKS_J):
                    to = block_i * BLOCKS_J + block_j
                    piece_ref[to, ROW_THIRD + at : ROW_THIRD + at + 16, :] = value
        for to in range(BLOCKS_I * BLOCKS_J):
            piece_ref[to, ROW_BITS : ROW_BITS + 1, :] = bits

    left = left_ref[...]
    for half in range(2):
        pieces = []
        for quarter in range(4):
            right = boundary_ref[:, 4 * half + quarter, :]
            high, low = split_high_low(right)
            by_high = dot(left, high)
            pieces.append(by_high[:32] + by_high[32:] + dot(left[:32], low))
        value = jnp.concatenate(pieces, axis=1)
        for block_i in range(BLOCKS_I):
            to = block_i * BLOCKS_J + 2 * step + half
            piece_ref[to, ROW_FIRST : ROW_FIRST + 4, :] = value[4 * block_i : 4 * block_i + 4]


def amplitude_kernel(digit_ref, cut_ref, string_ref, got_ref, out_ref, pairs_ref, allowed_ref, strings_ref, third_ref, sum_ref):
    place = 0
    for axis, size in zip(CUTS, AXES, strict=True):
        place = place * size + lax.axis_index(axis)
    block_i, block_j = place // BLOCKS_J, place % BLOCKS_J

    bits = got_ref[pl.ds(ROW_BITS, 64, stride=PIECE), :]
    bits_t = jnp.concatenate((bits, jnp.zeros_like(bits)), axis=0).T[:8, :64]

    row = lax.broadcasted_iota(jnp.int32, (LANES, 64), 0)
    i1 = 16 * (row // 64) + 2 * block_i + (row // 32) % 2
    i2 = row % 32
    lane = lax.broadcasted_iota(jnp.int32, (64, LANES), 1)
    j2 = 4 * block_j + lane // 32
    j3 = lane % 32
    strings = string_ref[...]
    string_lane = lax.broadcasted_iota(jnp.int32, strings.shape, 1)
    pairs = jnp.ones((LANES, 64), jnp.float32)
    allowed = jnp.ones((64, LANES), jnp.float32)
    fixed = jnp.ones((64, 64), jnp.float32)
    for cut in range(6):
        layer, group, bit = cut_ref[cut, 0], cut_ref[cut, 1], cut_ref[cut, 2]
        by_row, by_column = bits_t[cut : cut + 1, :], bits[:, cut : cut + 1]
        on_i1 = (group == 1) & (layer < 2)
        on_i2 = (group == 2) & (layer == 1)
        on_j2 = (group == 2) & (layer == 0)
        on_j3 = (group == 3) & (layer == 0)
        index = jnp.where(on_i1, i1, i2)
        agrees = ((index >> bit) & 1).astype(jnp.float32) == by_row
        pairs = jnp.where(agrees | jnp.logical_not(on_i1 | on_i2), pairs, 0.0)
        index = jnp.where(on_j2, j2, j3)
        agrees = ((index >> bit) & 1).astype(jnp.float32) == by_column
        allowed = jnp.where(agrees | jnp.logical_not(on_j2 | on_j3), allowed, 0.0)
        chosen = jnp.where(string_lane == 5 * group + bit, strings, 0)
        digit_bit = jnp.sum(chosen, axis=1, keepdims=True).astype(jnp.float32)
        inner = on_i1 | on_i2 | on_j2 | on_j3
        fixed = jnp.where((digit_bit == by_row) | inner, fixed, 0.0)
    pairs_ref[...] = pairs.astype(jnp.bfloat16)
    allowed_ref[...] = allowed.astype(jnp.bfloat16)
    strings_ref[...] = fixed

    def outer(base, carry):
        for part in range(2):
            for inside in range(8):
                b = base * 8 + inside
                g1, g2 = digit_ref[1, b], digit_ref[2, b]
                source = (2 * g1 + g2 // 16) * PIECE + ROW_THIRD + 16 * part + g2 % 16
                third_ref[part, inside : inside + 1, :] = got_ref[pl.ds(source, 1), :]
        third_real, third_imag = third_ref[0].T, third_ref[1].T
        allowed = allowed_ref[...]
        for inside in range(8):
            b = base * 8 + inside
            g0, g3 = digit_ref[0, b], digit_ref[3, b]
            row_b = strings_ref[pl.ds(b, 1), :].astype(jnp.bfloat16)
            count = dot(pairs_ref[...] * row_b, allowed)
            start = (g3 // 16) * PIECE + ROW_SECOND + g3 % 16
            second_real = got_ref[pl.ds(start, 32, stride=2 * PIECE), :]
            second_imag = got_ref[pl.ds(start + 16, 32, stride=2 * PIECE), :]
            total_real = jnp.zeros((1, LANES), jnp.float32)
            total_imag = jnp.zeros((1, LANES), jnp.float32)
            for q in range(4):
                rows = slice(32 * q, 32 * q + 32)
                weight_real = third_real[rows, inside : inside + 1] * count[rows]
                weight_imag = third_imag[rows, inside : inside + 1] * count[rows]
                real = jnp.sum(weight_real * second_real - weight_imag * second_imag, axis=0, keepdims=True)
                imag = jnp.sum(weight_real * second_imag + weight_imag * second_real, axis=0, keepdims=True)
                source = (2 * g0 + q // 2) * PIECE + ROW_FIRST + q % 2
                first_real = got_ref[pl.ds(source, 1), :]
                first_imag = got_ref[pl.ds(source + 2, 1), :]
                total_real += real * first_real - imag * first_imag
                total_imag += real * first_imag + imag * first_real
            sum_ref[pl.ds(b, 1), :] = total_real
            sum_ref[pl.ds(64 + b, 1), :] = total_imag
        return carry

    lax.fori_loop(0, 8, outer, 0)
    result = jnp.sum(sum_ref[...].T, axis=0, keepdims=True)
    for to in range(16):
        out_ref[to] = result


def all_reduced(copies, axes, rows):
    got = lax.all_to_all(copies, axes, 0, 0, tiled=True)
    total = jnp.sum(got, axis=0, keepdims=True)
    return jnp.broadcast_to(total, (rows,) + total.shape[1:])


def on_device(boundary, gate_stack, layer_order, cut_index, slice_bits, bitstrings):
    smem = pl.BlockSpec(memory_space=pltpu.SMEM)
    vmem = pl.BlockSpec(memory_space=pltpu.VMEM)
    right = boundary.reshape(512, 32, 32)
    pieces = pl.pallas_call(
        pack_kernel,
        grid=(4,),
        out_shape=jax.ShapeDtypeStruct((64, PIECE, LANES), jnp.float32),
        in_specs=[
            smem,
            smem,
            pl.BlockSpec((3, 2, 16, 1024), lambda step: (0, 0, 0, 0)),
            pl.BlockSpec((512, 8, 32), lambda step: (0, step, 0)),
        ],
        out_specs=pl.BlockSpec((64, PIECE, LANES), lambda step: (0, 0, 0)),
        scratch_shapes=[pltpu.VMEM((64, 512), jnp.bfloat16)],
        name="pack",
    )(layer_order, slice_bits, gate_stack, right)
    got = lax.all_to_all(pieces, CUTS, 0, 0, tiled=True).reshape(64 * PIECE, LANES)

    weights = jnp.left_shift(jnp.ones((5,), jnp.int32), jnp.arange(5, dtype=jnp.int32))
    digits = jnp.sum(bitstrings.reshape(64, 4, 5) * weights, axis=2).T
    partial_sums = pl.pallas_call(
        amplitude_kernel,
        out_shape=jax.ShapeDtypeStruct((16, 1, LANES), jnp.float32),
        in_specs=[smem, smem, vmem, vmem],
        out_specs=vmem,
        scratch_shapes=[
            pltpu.VMEM((LANES, 64), jnp.bfloat16),
            pltpu.VMEM((64, LANES), jnp.bfloat16),
            pltpu.VMEM((64, 64), jnp.float32),
            pltpu.VMEM((2, 8, LANES), jnp.float32),
            pltpu.VMEM((LANES, LANES), jnp.float32),
        ],
        name="amplitude",
    )(digits, cut_index, bitstrings, got)
    total = all_reduced(partial_sums, COLUMN, 16)
    total = all_reduced(total, PLANE, 1)
    return total.reshape(2, 64).T


def solution(mesh):
    finer = Mesh(
        mesh.devices.reshape(AXES + (mesh.shape["grp"],)),
        CUTS + ("grp",),
    )
    return jax.shard_map(
        on_device,
        mesh=finer,
        in_specs=(
            P("grp", None, None, None, None),
            P(None, None, CUTS, None),
            P(),
            P(),
            P(CUTS, None),
            P(),
        ),
        out_specs=P(),
        check_vma=False,
    )
```

```python
from functools import partial

import jax
import jax.numpy as jnp
from jax import lax
from jax.experimental import pallas as pl
from jax.experimental.pallas import tpu as pltpu
from jax.sharding import Mesh
from jax.sharding import PartitionSpec as P

AXES = (4, 4, 2, 2)
CUTS = ("cuts_0", "cuts_1", "cuts_2", "cuts_3")
PLANE = ("cuts_0", "cuts_1")
COLUMN = ("cuts_2", "cuts_3", "grp")

BLOCKS_I, BLOCKS_J = 8, 8
LANES = 128
ROW_SECOND, ROW_THIRD, ROW_FIRST, ROW_BITS, PIECE = 0, 32, 64, 68, 72


def split_high_low(array):
    high = array.astype(jnp.bfloat16)
    return high, (array - high.astype(jnp.float32)).astype(jnp.bfloat16)


def dot(left, right):
    return jnp.dot(left, right, preferred_element_type=jnp.float32)


def pack_kernel(order_hbm, bits_hbm, string_hbm, gate_hbm, boundary_hbm, piece_ref, row_ref, order_ref, bits_ref, string_ref, gate_ref, boundary_ref, left_ref, sems):
    small = [
        pltpu.make_async_copy(order_hbm, order_ref, sems.at[0]),
        pltpu.make_async_copy(bits_hbm, bits_ref, sems.at[1]),
        pltpu.make_async_copy(string_hbm, string_ref, sems.at[2]),
        pltpu.make_async_copy(gate_hbm, gate_ref, sems.at[3]),
    ]
    large = [
        pltpu.make_async_copy(boundary_hbm.at[:, pl.ds(8 * step, 8), :], boundary_ref.at[step], sems.at[4 + step])
        for step in range(4)
    ]
    for copy in small + large:
        copy.start()
    for copy in small:
        copy.wait()

    first, second, third = order_ref[0], order_ref[1], order_ref[2]
    member = lax.axis_index("grp")
    columns = pl.ds(pl.multiple_of(member * 256, 256), 256)
    real, imag = gate_ref[first, 0, :, columns], gate_ref[first, 1, :, columns]

    def interleaved(even, odd):
        parts = []
        for k0 in range(8):
            parts += [even[:, 32 * k0 : 32 * k0 + 32], odd[:, 32 * k0 : 32 * k0 + 32]]
        return jnp.concatenate(parts, axis=1)

    to_real, to_imag = interleaved(real, -imag), interleaved(imag, real)
    rows = []
    for block in range(BLOCKS_I):
        rows += [to_real[2 * block : 2 * block + 2], to_imag[2 * block : 2 * block + 2]]
    left = jnp.concatenate(rows, axis=0)
    high, low = split_high_low(left)
    left_ref[...] = jnp.concatenate((high, low), axis=0)

    strings = string_ref[...]

    def digit(group):
        total = strings[5 * group : 5 * group + 1]
        for bit in range(1, 5):
            total = total + (strings[5 * group + bit : 5 * group + bit + 1] << bit)
        return total

    g0, g1, g2, g3 = (digit(group) for group in range(4))
    row_ref[0:1, :] = 2 * g0 * PIECE + ROW_FIRST
    row_ref[1:2, :] = (g3 >> 4) * PIECE + ROW_SECOND + (g3 & 15)
    row_ref[2:3, :] = (2 * g1 + (g2 >> 4)) * PIECE + ROW_THIRD + (g2 & 15)

    lane = lax.broadcasted_iota(jnp.int32, (1, LANES), 1)
    bits = jnp.zeros((1, LANES), jnp.float32)
    for cut in range(6):
        bits = jnp.where(lane == cut, bits_ref[0, cut].astype(jnp.float32), bits)
    for part in range(2):
        at = 16 * part
        for block_j in range(BLOCKS_J):
            value = gate_ref[second, part, :, LANES * block_j : LANES * block_j + LANES]
            for block_i in range(BLOCKS_I):
                to = block_i * BLOCKS_J + block_j
                piece_ref[to, ROW_SECOND + at : ROW_SECOND + at + 16, :] = value
        whole = gate_ref[third, part]
        for block_i in range(BLOCKS_I):
            value = jnp.concatenate(
                (
                    whole[:, 64 * block_i : 64 * block_i + 64],
                    whole[:, 512 + 64 * block_i : 512 + 64 * block_i + 64],
                ),
                axis=1,
            )
            for block_j in range(BLOCKS_J):
                to = block_i * BLOCKS_J + block_j
                piece_ref[to, ROW_THIRD + at : ROW_THIRD + at + 16, :] = value
    for to in range(BLOCKS_I * BLOCKS_J):
        piece_ref[to, ROW_BITS : ROW_BITS + 1, :] = bits

    left = left_ref[...]
    for step in range(4):
        large[step].wait()
        flat = boundary_ref.at[step].reshape(4096, 32)
        for half in range(2):
            right = jnp.concatenate(
                [flat[pl.ds(4 * half + quarter, 512, stride=8), :] for quarter in range(4)], axis=1
            )
            high, low = split_high_low(right)
            by_high = dot(left, high)
            value = by_high[:32] + by_high[32:] + dot(left[:32], low)
            for block_i in range(BLOCKS_I):
                to = block_i * BLOCKS_J + 2 * step + half
                piece_ref[to, ROW_FIRST : ROW_FIRST + 4, :] = value[4 * block_i : 4 * block_i + 4]


def amplitude_kernel(row_ref, cut_ref, string_ref, got_ref, out_ref, pairs_ref, allowed_ref, fixed_ref, third_ref, sum_ref):
    place = 0
    for axis, size in zip(CUTS, AXES, strict=True):
        place = place * size + lax.axis_index(axis)
    block_i, block_j = place // BLOCKS_J, place % BLOCKS_J

    bits = got_ref[pl.ds(ROW_BITS, 64, stride=PIECE), :]
    bits_t = jnp.concatenate((bits, jnp.zeros_like(bits)), axis=0).T[:8, :64]

    row = lax.broadcasted_iota(jnp.int32, (LANES, 64), 0)
    i1 = 16 * (row >> 6) + 2 * block_i + ((row >> 5) & 1)
    i2 = row & 31
    lane = lax.broadcasted_iota(jnp.int32, (64, LANES), 1)
    j2 = 4 * block_j + (lane >> 5)
    j3 = lane & 31
    pairs = jnp.ones((LANES, 64), jnp.float32)
    allowed = jnp.ones((64, LANES), jnp.float32)
    fixed = jnp.ones((64, 64), jnp.float32)
    for cut in range(6):
        layer, group, bit = cut_ref[0, cut], cut_ref[1, cut], cut_ref[2, cut]
        by_row, by_column = bits_t[cut : cut + 1, :], bits[:, cut : cut + 1]
        on_i1 = (group == 1) & (layer < 2)
        on_i2 = (group == 2) & (layer == 1)
        on_j2 = (group == 2) & (layer == 0)
        on_j3 = (group == 3) & (layer == 0)
        index = jnp.where(on_i1, i1, i2)
        agrees = ((index >> bit) & 1).astype(jnp.float32) == by_row
        pairs = jnp.where(agrees | jnp.logical_not(on_i1 | on_i2), pairs, 0.0)
        index = jnp.where(on_j2, j2, j3)
        agrees = ((index >> bit) & 1).astype(jnp.float32) == by_column
        allowed = jnp.where(agrees | jnp.logical_not(on_j2 | on_j3), allowed, 0.0)
        chosen = string_ref[pl.ds(5 * group + bit, 1), :].astype(jnp.float32)
        inner = on_i1 | on_i2 | on_j2 | on_j3
        fixed = jnp.where((chosen == bits[:, cut : cut + 1]) | inner, fixed, 0.0)
    pairs_ref[...] = pairs.astype(jnp.bfloat16)
    allowed_ref[...] = allowed.astype(jnp.bfloat16)
    fixed = jnp.concatenate((fixed, jnp.zeros_like(fixed)), axis=1)
    fixed_ref[...] = jnp.concatenate((fixed, jnp.zeros_like(fixed)), axis=0).T[:64, :64]

    def outer(base, carry):
        for part in range(2):
            for inside in range(8):
                source = row_ref[2, base * 8 + inside] + 16 * part
                third_ref[part, inside : inside + 1, :] = got_ref[pl.ds(source, 1), :]
        third_real, third_imag = third_ref[0].T, third_ref[1].T
        for inside in range(8):
            b = base * 8 + inside
            row_b = fixed_ref[pl.ds(b, 1), :].astype(jnp.bfloat16)
            count = dot(pairs_ref[...] * row_b, allowed_ref[...])
            start, source = row_ref[1, b], row_ref[0, b]
            total_real = jnp.zeros((8, LANES), jnp.float32)
            total_imag = jnp.zeros((8, LANES), jnp.float32)
            for q in range(4):
                real = jnp.zeros((8, LANES), jnp.float32)
                imag = jnp.zeros((8, LANES), jnp.float32)
                for part in range(4):
                    rows = slice(32 * q + 8 * part, 32 * q + 8 * part + 8)
                    at = start + 16 * PIECE * part
                    second_real = got_ref[pl.ds(at, 8, stride=2 * PIECE), :]
                    second_imag = got_ref[pl.ds(at + 16, 8, stride=2 * PIECE), :]
                    weight_real = third_real[rows, inside : inside + 1] * count[rows]
                    weight_imag = third_imag[rows, inside : inside + 1] * count[rows]
                    real += weight_real * second_real - weight_imag * second_imag
                    imag += weight_real * second_imag + weight_imag * second_real
                at = source + (q // 2) * PIECE + q % 2
                first_real = got_ref[pl.ds(at, 1), :]
                first_imag = got_ref[pl.ds(at + 2, 1), :]
                total_real += real * first_real - imag * first_imag
                total_imag += real * first_imag + imag * first_real
            sum_ref[pl.ds(b, 1), :] = jnp.sum(total_real, axis=0, keepdims=True)
            sum_ref[pl.ds(64 + b, 1), :] = jnp.sum(total_imag, axis=0, keepdims=True)
        return carry

    lax.fori_loop(0, 8, outer, 0)
    result = jnp.sum(sum_ref[...].T, axis=0, keepdims=True)
    for to in range(16):
        out_ref[to] = result


def all_reduced(copies, axes, rows):
    got = lax.all_to_all(copies, axes, 0, 0, tiled=True)
    total = jnp.sum(got, axis=0, keepdims=True)
    return jnp.broadcast_to(total, (rows,) + total.shape[1:])


def on_device(boundary, gate_stack, layer_order, cut_index, slice_bits, bitstrings):
    smem = pl.BlockSpec(memory_space=pltpu.SMEM)
    vmem = pl.BlockSpec(memory_space=pltpu.VMEM)
    strings = bitstrings.T
    in_hbm = partial(pltpu.with_memory_space_constraint, memory_space=pltpu.HBM)
    hbm = pl.BlockSpec(memory_space=pltpu.HBM)
    pieces, rows = pl.pallas_call(
        pack_kernel,
        out_shape=(
            jax.ShapeDtypeStruct((64, PIECE, LANES), jnp.float32),
            jax.ShapeDtypeStruct((8, 64), jnp.int32),
        ),
        in_specs=[hbm] * 5,
        out_specs=(vmem, vmem),
        scratch_shapes=[
            pltpu.SMEM((3,), jnp.int32),
            pltpu.SMEM((1, 6), jnp.int32),
            pltpu.VMEM((20, 64), jnp.int32),
            pltpu.VMEM((3, 2, 16, 1024), jnp.float32),
            pltpu.VMEM((4, 512, 8, 32), jnp.float32),
            pltpu.VMEM((64, 512), jnp.bfloat16),
            pltpu.SemaphoreType.DMA((8,)),
        ],
        compiler_params=pltpu.CompilerParams(vmem_limit_bytes=24 << 20),
        name="pack",
    )(*(in_hbm(x) for x in (layer_order, slice_bits, strings, gate_stack, boundary.reshape(512, 32, 32))))
    got = lax.all_to_all(pieces, CUTS, 0, 0, tiled=True).reshape(64 * PIECE, LANES)
    partial_sums = pl.pallas_call(
        amplitude_kernel,
        out_shape=jax.ShapeDtypeStruct((16, 1, LANES), jnp.float32),
        in_specs=[smem, smem, vmem, vmem],
        out_specs=vmem,
        scratch_shapes=[
            pltpu.VMEM((LANES, 64), jnp.bfloat16),
            pltpu.VMEM((64, LANES), jnp.bfloat16),
            pltpu.VMEM((64, 64), jnp.float32),
            pltpu.VMEM((2, 8, LANES), jnp.float32),
            pltpu.VMEM((LANES, LANES), jnp.float32),
        ],
        compiler_params=pltpu.CompilerParams(vmem_limit_bytes=12 << 20),
        name="amplitude",
    )(rows, in_hbm(cut_index.T), in_hbm(strings), got)
    total = all_reduced(partial_sums, COLUMN, 16)
    total = all_reduced(total, PLANE, 1)
    return total.reshape(2, 64).T


def solution(mesh):
    finer = Mesh(
        mesh.devices.reshape(AXES + (mesh.shape["grp"],)),
        CUTS + ("grp",),
    )
    return jax.shard_map(
        on_device,
        mesh=finer,
        in_specs=(
            P("grp", None, None, None, None),
            P(None, None, CUTS, None),
            P(),
            P(),
            P(CUTS, None),
            P(),
        ),
        out_specs=P(),
        check_vma=False,
    )
```

```python
from functools import partial

import jax
import jax.numpy as jnp
from jax import lax
from jax.experimental import pallas as pl
from jax.experimental.pallas import tpu as pltpu
from jax.sharding import Mesh
from jax.sharding import PartitionSpec as P

AXES = (4, 4, 2, 2)
CUTS = ("cuts_0", "cuts_1", "cuts_2", "cuts_3")
WAVE = ("cuts_1", "cuts_2", "cuts_3")
PLANE = ("cuts_0", "cuts_1")
COLUMN = ("cuts_2", "cuts_3", "grp")

BLOCKS_I, BLOCKS_J = 4, 16
LANES = 128
UNROLL = 2
ROW_SECOND, ROW_FIRST, ROW_THIRD, ROW_BITS, PIECE = 0, 16, 20, 24, 25


def split_high_low(array):
    high = array.astype(jnp.bfloat16)
    return high, (array - high.astype(jnp.float32)).astype(jnp.bfloat16)


def dot(left, right):
    return jnp.dot(left, right, preferred_element_type=jnp.float32)


def lane_of(shape):
    return lax.broadcasted_iota(jnp.int32, shape, 1)


def side_by_side(real, imag):
    low = lane_of(real.shape) < 64
    return jnp.where(low, real, pltpu.roll(imag, 64, 1)), jnp.where(low, pltpu.roll(real, 64, 1), imag)


def regrouped(parts, group):
    lane = lane_of(parts[0].shape)
    result = None
    for place, part in enumerate(parts):
        shift = 16 * (place - group) % LANES
        moved = pltpu.roll(part, shift, 1) if shift else part
        result = moved if place == 0 else jnp.where(lane >= 16 * place, moved, result)
    return result


def pack_kernel(order_hbm, bits_hbm, string_hbm, gate_hbm, boundary_hbm, piece_ref, row_ref, order_ref, bits_ref, string_ref, gate_ref, boundary_ref, left_ref, sems):
    small = [
        pltpu.make_async_copy(order_hbm, order_ref, sems.at[0]),
        pltpu.make_async_copy(bits_hbm, bits_ref, sems.at[1]),
        pltpu.make_async_copy(string_hbm, string_ref, sems.at[2]),
        pltpu.make_async_copy(gate_hbm, gate_ref, sems.at[3]),
    ]
    large = [
        pltpu.make_async_copy(boundary_hbm.at[:, pl.ds(8 * step, 8), :], boundary_ref.at[step], sems.at[4 + step])
        for step in range(4)
    ]
    for copy in small + large:
        copy.start()
    for copy in small:
        copy.wait()

    first, second, third = order_ref[0], order_ref[1], order_ref[2]
    member = lax.axis_index("grp")
    columns = pl.ds(pl.multiple_of(member * 256, 256), 256)
    real, imag = gate_ref[first, 0, :, columns], gate_ref[first, 1, :, columns]

    def interleaved(even, odd):
        parts = []
        for k0 in range(8):
            parts += [even[:, 32 * k0 : 32 * k0 + 32], odd[:, 32 * k0 : 32 * k0 + 32]]
        return jnp.concatenate(parts, axis=1)

    left = jnp.concatenate((interleaved(real, -imag), interleaved(imag, real)), axis=0)
    high, low = split_high_low(left)
    left_ref[...] = jnp.concatenate((high, low), axis=0)

    strings = string_ref[...]

    def digit(group):
        total = strings[5 * group : 5 * group + 1]
        for bit in range(1, 5):
            total = total + (strings[5 * group + bit : 5 * group + bit + 1] << bit)
        return total

    g0, g1, g2, g3 = (digit(group) for group in range(4))
    row_ref[0:1, :] = 2 * g0 * PIECE + ROW_FIRST
    row_ref[1:2, :] = (g3 >> 4) * PIECE + ROW_SECOND + (g3 & 15)
    row_ref[2:3, :] = (2 * g1 + (g2 >> 4)) * PIECE + ROW_THIRD + (g2 & 3)
    row_ref[3:4, :] = 32 * (((lane_of((1, 64)) >> 4) - ((g2 & 15) >> 2)) & 3)

    lane = lane_of((1, LANES))
    bits = jnp.zeros((1, LANES), jnp.float32)
    for cut in range(6):
        bits = jnp.where(lane == cut, bits_ref[0, cut].astype(jnp.float32), bits)

    def put(block_i, block_j, at, value):
        start = (block_i * BLOCKS_J + block_j) * PIECE + at
        piece_ref[start : start + value.shape[0], :] = value

    for tile in range(8):
        lanes = slice(LANES * tile, LANES * tile + LANES)
        values = side_by_side(gate_ref[second, 0, :, lanes], gate_ref[second, 1, :, lanes])
        for half in range(2):
            for block_i in range(BLOCKS_I):
                put(block_i, 2 * tile + half, ROW_SECOND, values[half])
    for block_i in range(BLOCKS_I):
        parts = []
        for four in range(4):
            for part in range(2):
                rows = slice(4 * four, 4 * four + 4)
                parts.append(
                    jnp.concatenate(
                        [
                            gate_ref[third, part, rows, 512 * h + LANES * block_i : 512 * h + LANES * block_i + LANES]
                            for h in range(2)
                        ],
                        axis=0,
                    )
                )
        for group in range(8):
            value = regrouped(parts, group)
            put(block_i, group, ROW_THIRD, value[:4])
            put(block_i, 8 + group, ROW_THIRD, value[4:])
    for block_i in range(BLOCKS_I):
        for block_j in range(BLOCKS_J):
            put(block_i, block_j, ROW_BITS, bits)

    left = left_ref[...]
    for step in range(4):
        large[step].wait()
        flat = boundary_ref.at[step].reshape(4096, 32)
        for half in range(2):
            right = jnp.concatenate(
                [flat[pl.ds(4 * half + quarter, 512, stride=8), :] for quarter in range(4)], axis=1
            )
            high, low = split_high_low(right)
            by_high = dot(left, high)
            value = by_high[:32] + by_high[32:] + dot(left[:32], low)
            values = side_by_side(value[:16], value[16:])
            for side in range(2):
                for block_i in range(BLOCKS_I):
                    rows = values[side][4 * block_i : 4 * block_i + 4]
                    put(block_i, 4 * step + 2 * half + side, ROW_FIRST, rows)


def inner_kernel(row_ref, cut_ref, string_ref, got_ref, out_ref, third_ref, pairs_ref, allowed_ref, fixed_ref, sum_ref, whole_ref):
    place = 0
    for axis, size in zip(CUTS, AXES, strict=True):
        place = place * size + lax.axis_index(axis)
    block_i, block_j = place // BLOCKS_J, place % BLOCKS_J

    bits = got_ref[pl.ds(ROW_BITS, 64, stride=PIECE), :]
    bits_t = jnp.concatenate((bits, jnp.zeros_like(bits)), axis=0).T[:8, :64]

    row = lax.broadcasted_iota(jnp.int32, (256, 64), 0)
    i1 = 16 * (row >> 7) + 4 * block_i + ((row >> 5) & 3)
    i2 = row & 31
    j = lane_of((64, LANES)) & 63
    j2 = 2 * block_j + (j >> 5)
    j3 = j & 31
    pairs = jnp.ones((256, 64), jnp.float32)
    allowed = jnp.ones((64, LANES), jnp.float32)
    fixed = jnp.ones((64, 64), jnp.float32)
    for cut in range(6):
        layer, group, bit = cut_ref[0, cut], cut_ref[1, cut], cut_ref[2, cut]
        by_row, by_column = bits_t[cut : cut + 1, :], bits[:, cut : cut + 1]
        on_i1 = (group == 1) & (layer < 2)
        on_i2 = (group == 2) & (layer == 1)
        on_j2 = (group == 2) & (layer == 0)
        on_j3 = (group == 3) & (layer == 0)
        index = jnp.where(on_i1, i1, i2)
        agrees = ((index >> bit) & 1).astype(jnp.float32) == by_row
        pairs = jnp.where(agrees | jnp.logical_not(on_i1 | on_i2), pairs, 0.0)
        index = jnp.where(on_j2, j2, j3)
        agrees = ((index >> bit) & 1).astype(jnp.float32) == by_column
        allowed = jnp.where(agrees | jnp.logical_not(on_j2 | on_j3), allowed, 0.0)
        chosen = string_ref[pl.ds(5 * group + bit, 1), :].astype(jnp.float32)
        inner = on_i1 | on_i2 | on_j2 | on_j3
        fixed = jnp.where((chosen == by_column) | inner, fixed, 0.0)
    pairs_ref[...] = pairs.astype(jnp.bfloat16)
    allowed_ref[...] = allowed.astype(jnp.bfloat16)
    fixed = jnp.concatenate((fixed, jnp.zeros_like(fixed)), axis=1)
    fixed_ref[...] = jnp.concatenate((fixed, jnp.zeros_like(fixed)), axis=0).T[:64, :64]

    lane = lane_of((1, LANES))
    for row in range(16):
        value = None
        for four in range(4):
            b = 16 * four + row
            moved = pltpu.roll(got_ref[pl.ds(row_ref[2, b], 1), :], row_ref[3, b], 1)
            value = moved if four == 0 else jnp.where(lane >= 32 * four, moved, value)
        third_ref[row : row + 1, :] = value

    low = lane_of((8, LANES)) < 64

    def one(b):
        row_b = fixed_ref[pl.ds(b, 1), :].astype(jnp.bfloat16)
        start, source = row_ref[1, b], row_ref[0, b]
        first = jnp.concatenate((got_ref[pl.ds(source, 4), :], got_ref[pl.ds(source + PIECE, 4), :]), axis=0)
        turned = pltpu.roll(first, 64, 1)
        by_same = jnp.where(low, first, turned)
        by_other = jnp.where(low, -turned, first)
        second = got_ref[pl.ds(start, 32, stride=2 * PIECE), :]
        other = pltpu.roll(second, 64, 1)
        for h in range(2):
            rows = slice(128 * h, 128 * h + 128)
            count = dot(pairs_ref[rows, :] * row_b, allowed_ref[...])
            terms = []
            for e in range(4):
                q = 4 * h + e
                term = by_same[q : q + 1] * second + by_other[q : q + 1] * other
                terms.append(term * count[32 * e : 32 * e + 32])
            columns = jnp.concatenate(terms, axis=0).T
            for part in range(2):
                total = jnp.sum(columns[64 * part : 64 * part + 64].reshape(8, 8, LANES), axis=0)
                sum_ref[2 * part + h, pl.ds(pl.multiple_of(8 * b, 8), 8), :] = total

    def several(base, carry):
        for inside in range(UNROLL):
            one(base * UNROLL + inside)
        return carry

    lax.fori_loop(0, 64 // UNROLL, several, 0)
    for part in range(2):
        for h in range(2):
            total = jnp.zeros((64, LANES), jnp.float32)
            for sublane in range(8):
                total += sum_ref[2 * part + h, pl.ds(sublane, 64, stride=8), :]
            whole_ref[2 * part + h] = total
    for h in range(2):
        parts = [whole_ref[2 * part + h, 16 * four : 16 * four + 16] for four in range(4) for part in range(2)]
        for group in range(8):
            out_ref[8 * h + group] = regrouped(parts, group)


def outer_kernel(third_ref, got_ref, out_ref):
    total = jnp.sum(got_ref[...], axis=0)
    second_half = (lane_of((16, LANES)) & 16) != 0
    other = jnp.where(second_half, pltpu.roll(total, 16, 1), pltpu.roll(total, LANES - 16, 1))
    third = third_ref[...]
    real = third * jnp.where(second_half, -total, total)
    imag = third * other
    columns = jnp.concatenate((real, imag, jnp.zeros((96, LANES), jnp.float32)), axis=0).T
    sums = [jnp.sum(columns[32 * four : 32 * four + 32, :32], axis=0, keepdims=True) for four in range(4)]
    result = jnp.concatenate([x[:, :16] for x in sums] + [x[:, 16:] for x in sums], axis=1)
    for to in range(16):
        out_ref[to] = result


def all_reduced(copies, axes, rows):
    got = lax.all_to_all(copies, axes, 0, 0, tiled=True)
    total = jnp.sum(got, axis=0, keepdims=True)
    return jnp.broadcast_to(total, (rows,) + total.shape[1:])


def on_device(boundary, gate_stack, layer_order, cut_index, slice_bits, bitstrings):
    smem = pl.BlockSpec(memory_space=pltpu.SMEM)
    vmem = pl.BlockSpec(memory_space=pltpu.VMEM)
    hbm = pl.BlockSpec(memory_space=pltpu.HBM)
    in_hbm = partial(pltpu.with_memory_space_constraint, memory_space=pltpu.HBM)
    strings = bitstrings.T
    pieces, rows = pl.pallas_call(
        pack_kernel,
        out_shape=(
            jax.ShapeDtypeStruct((64 * PIECE, LANES), jnp.float32),
            jax.ShapeDtypeStruct((8, 64), jnp.int32),
        ),
        in_specs=[hbm] * 5,
        out_specs=(vmem, vmem),
        scratch_shapes=[
            pltpu.SMEM((3,), jnp.int32),
            pltpu.SMEM((1, 6), jnp.int32),
            pltpu.VMEM((20, 64), jnp.int32),
            pltpu.VMEM((3, 2, 16, 1024), jnp.float32),
            pltpu.VMEM((4, 512, 8, 32), jnp.float32),
            pltpu.VMEM((64, 512), jnp.bfloat16),
            pltpu.SemaphoreType.DMA((8,)),
        ],
        compiler_params=pltpu.CompilerParams(vmem_limit_bytes=24 << 20),
        name="pack",
    )(*(in_hbm(x) for x in (layer_order, slice_bits, strings, gate_stack, boundary.reshape(512, 32, 32))))
    pieces = pieces.reshape(64, 1, PIECE * LANES)
    got = lax.all_to_all(pieces, CUTS, 0, 0, tiled=True).reshape(64 * PIECE, LANES)
    inner, third = pl.pallas_call(
        inner_kernel,
        out_shape=(
            jax.ShapeDtypeStruct((16, 16, LANES), jnp.float32),
            jax.ShapeDtypeStruct((16, LANES), jnp.float32),
        ),
        in_specs=[smem, smem, vmem, vmem],
        out_specs=(vmem, vmem),
        scratch_shapes=[
            pltpu.VMEM((256, 64), jnp.bfloat16),
            pltpu.VMEM((64, LANES), jnp.bfloat16),
            pltpu.VMEM((64, 64), jnp.float32),
            pltpu.VMEM((4, 512, LANES), jnp.float32),
            pltpu.VMEM((4, 64, LANES), jnp.float32),
        ],
        compiler_params=pltpu.CompilerParams(vmem_limit_bytes=16 << 20),
        name="inner",
    )(rows, in_hbm(cut_index.T), in_hbm(strings), got)
    inner = lax.all_to_all(inner, WAVE, 0, 0, tiled=True)
    partial_sums = pl.pallas_call(
        outer_kernel,
        out_shape=jax.ShapeDtypeStruct((16, 1, LANES), jnp.float32),
        in_specs=[vmem, vmem],
        out_specs=vmem,
        compiler_params=pltpu.CompilerParams(vmem_limit_bytes=8 << 20),
        name="outer",
    )(third, inner)
    total = all_reduced(partial_sums, COLUMN, 16)
    total = all_reduced(total, PLANE, 1)
    return total.reshape(2, 64).T


def solution(mesh):
    finer = Mesh(
        mesh.devices.reshape(AXES + (mesh.shape["grp"],)),
        CUTS + ("grp",),
    )
    return jax.shard_map(
        on_device,
        mesh=finer,
        in_specs=(
            P("grp", None, None, None, None),
            P(None, None, CUTS, None),
            P(),
            P(),
            P(CUTS, None),
            P(),
        ),
        out_specs=P(),
        check_vma=False,
    )
```

```python
from functools import partial

import jax
import jax.numpy as jnp
from jax import lax
from jax.experimental import pallas as pl
from jax.experimental.pallas import tpu as pltpu
from jax.sharding import Mesh
from jax.sharding import PartitionSpec as P

AXES = (4, 4, 2, 2)
CUTS = ("cuts_0", "cuts_1", "cuts_2", "cuts_3")
WAVE = ("cuts_1", "cuts_2", "cuts_3")
PLANE = ("cuts_0", "cuts_1")
COLUMN = ("cuts_2", "cuts_3", "grp")

BLOCKS_I, BLOCKS_J = 4, 16
LANES = 128
UNROLL = 8
ROW_SECOND, ROW_FIRST, ROW_THIRD, ROW_BITS, PIECE = 0, 16, 20, 24, 25


def split_high_low(array):
    high = array.astype(jnp.bfloat16)
    return high, (array - high.astype(jnp.float32)).astype(jnp.bfloat16)


def dot(left, right):
    return jnp.dot(left, right, preferred_element_type=jnp.float32)


def lane_of(shape):
    return lax.broadcasted_iota(jnp.int32, shape, 1)


def side_by_side(real, imag):
    low = lane_of(real.shape) < 64
    return jnp.where(low, real, pltpu.roll(imag, 64, 1)), jnp.where(low, pltpu.roll(real, 64, 1), imag)


def regrouped(parts, group):
    lane = lane_of(parts[0].shape)
    result = None
    for place, part in enumerate(parts):
        shift = 16 * (place - group) % LANES
        moved = pltpu.roll(part, shift, 1) if shift else part
        result = moved if place == 0 else jnp.where(lane >= 16 * place, moved, result)
    return result


def pack_kernel(order_hbm, bits_hbm, string_hbm, gate_hbm, boundary_hbm, piece_ref, row_ref, order_ref, bits_ref, string_ref, gate_ref, boundary_ref, left_ref, sems):
    small = [
        pltpu.make_async_copy(order_hbm, order_ref, sems.at[0]),
        pltpu.make_async_copy(bits_hbm, bits_ref, sems.at[1]),
        pltpu.make_async_copy(string_hbm, string_ref, sems.at[2]),
        pltpu.make_async_copy(gate_hbm, gate_ref, sems.at[3]),
    ]
    large = [
        pltpu.make_async_copy(boundary_hbm.at[:, pl.ds(8 * step, 8), :], boundary_ref.at[step], sems.at[4 + step])
        for step in range(4)
    ]
    for copy in small + large:
        copy.start()
    for copy in small:
        copy.wait()

    first, second, third = order_ref[0], order_ref[1], order_ref[2]
    member = lax.axis_index("grp")
    columns = pl.ds(pl.multiple_of(member * 256, 256), 256)
    real, imag = gate_ref[first, 0, :, columns], gate_ref[first, 1, :, columns]

    def interleaved(even, odd):
        parts = []
        for k0 in range(8):
            parts += [even[:, 32 * k0 : 32 * k0 + 32], odd[:, 32 * k0 : 32 * k0 + 32]]
        return jnp.concatenate(parts, axis=1)

    left = jnp.concatenate((interleaved(real, -imag), interleaved(imag, real)), axis=0)
    high, low = split_high_low(left)
    left_ref[...] = jnp.concatenate((high, low), axis=0)

    strings = string_ref[...]

    def digit(group):
        total = strings[5 * group : 5 * group + 1]
        for bit in range(1, 5):
            total = total + (strings[5 * group + bit : 5 * group + bit + 1] << bit)
        return total

    g0, g1, g2, g3 = (digit(group) for group in range(4))
    row_ref[0:1, :] = 2 * g0 * PIECE + ROW_FIRST
    row_ref[1:2, :] = (g3 >> 4) * PIECE + ROW_SECOND + (g3 & 15)
    row_ref[2:3, :] = (2 * g1 + (g2 >> 4)) * PIECE + ROW_THIRD + (g2 & 3)
    row_ref[3:4, :] = 32 * (((lane_of((1, 64)) >> 4) - ((g2 & 15) >> 2)) & 3)

    lane = lane_of((1, LANES))
    bits = jnp.zeros((1, LANES), jnp.float32)
    for cut in range(6):
        bits = jnp.where(lane == cut, bits_ref[0, cut].astype(jnp.float32), bits)

    def put(block_i, block_j, at, value):
        start = (block_i * BLOCKS_J + block_j) * PIECE + at
        piece_ref[start : start + value.shape[0], :] = value

    for tile in range(8):
        lanes = slice(LANES * tile, LANES * tile + LANES)
        values = side_by_side(gate_ref[second, 0, :, lanes], gate_ref[second, 1, :, lanes])
        for half in range(2):
            for block_i in range(BLOCKS_I):
                put(block_i, 2 * tile + half, ROW_SECOND, values[half])
    for block_i in range(BLOCKS_I):
        parts = []
        for four in range(4):
            for part in range(2):
                rows = slice(4 * four, 4 * four + 4)
                parts.append(
                    jnp.concatenate(
                        [
                            gate_ref[third, part, rows, 512 * h + LANES * block_i : 512 * h + LANES * block_i + LANES]
                            for h in range(2)
                        ],
                        axis=0,
                    )
                )
        for group in range(8):
            value = regrouped(parts, group)
            put(block_i, group, ROW_THIRD, value[:4])
            put(block_i, 8 + group, ROW_THIRD, value[4:])
    for block_i in range(BLOCKS_I):
        for block_j in range(BLOCKS_J):
            put(block_i, block_j, ROW_BITS, bits)

    left = left_ref[...]
    for step in range(4):
        large[step].wait()
        flat = boundary_ref.at[step].reshape(4096, 32)
        for half in range(2):
            right = jnp.concatenate(
                [flat[pl.ds(4 * half + quarter, 512, stride=8), :] for quarter in range(4)], axis=1
            )
            high, low = split_high_low(right)
            by_high = dot(left, high)
            value = by_high[:32] + by_high[32:] + dot(left[:32], low)
            values = side_by_side(value[:16], value[16:])
            for side in range(2):
                for block_i in range(BLOCKS_I):
                    rows = values[side][4 * block_i : 4 * block_i + 4]
                    put(block_i, 4 * step + 2 * half + side, ROW_FIRST, rows)


def inner_kernel(row_ref, cut_ref, string_ref, got_ref, out_ref, third_ref, pairs_ref, allowed_ref, fixed_ref, sum_ref, whole_ref, turned_ref, even_ref, odd_ref):
    place = 0
    for axis, size in zip(CUTS, AXES, strict=True):
        place = place * size + lax.axis_index(axis)
    block_i, block_j = place // BLOCKS_J, place % BLOCKS_J

    bits = got_ref[pl.ds(ROW_BITS, 64, stride=PIECE), :]
    bits_t = jnp.concatenate((bits, jnp.zeros_like(bits)), axis=0).T[:8, :64]

    row = lax.broadcasted_iota(jnp.int32, (256, 64), 0)
    i1 = 16 * (row >> 7) + 4 * block_i + ((row >> 5) & 3)
    i2 = row & 31
    j = lane_of((64, LANES)) & 63
    j2 = 2 * block_j + (j >> 5)
    j3 = j & 31
    pairs = jnp.ones((256, 64), jnp.float32)
    allowed = jnp.ones((64, LANES), jnp.float32)
    fixed = jnp.ones((64, 64), jnp.float32)
    for cut in range(6):
        layer, group, bit = cut_ref[0, cut], cut_ref[1, cut], cut_ref[2, cut]
        by_row, by_column = bits_t[cut : cut + 1, :], bits[:, cut : cut + 1]
        on_i1 = (group == 1) & (layer < 2)
        on_i2 = (group == 2) & (layer == 1)
        on_j2 = (group == 2) & (layer == 0)
        on_j3 = (group == 3) & (layer == 0)
        index = jnp.where(on_i1, i1, i2)
        agrees = ((index >> bit) & 1).astype(jnp.float32) == by_row
        pairs = jnp.where(agrees | jnp.logical_not(on_i1 | on_i2), pairs, 0.0)
        index = jnp.where(on_j2, j2, j3)
        agrees = ((index >> bit) & 1).astype(jnp.float32) == by_column
        allowed = jnp.where(agrees | jnp.logical_not(on_j2 | on_j3), allowed, 0.0)
        chosen = string_ref[pl.ds(5 * group + bit, 1), :].astype(jnp.float32)
        inner = on_i1 | on_i2 | on_j2 | on_j3
        fixed = jnp.where((chosen == by_column) | inner, fixed, 0.0)
    pairs_ref[...] = pairs.astype(jnp.bfloat16)
    allowed_ref[...] = allowed.astype(jnp.bfloat16)
    fixed = jnp.concatenate((fixed, jnp.zeros_like(fixed)), axis=1)
    fixed_ref[...] = jnp.concatenate((fixed, jnp.zeros_like(fixed)), axis=0).T[:64, :64]

    lane = lane_of((1, LANES))
    for row in range(16):
        value = None
        for four in range(4):
            b = 16 * four + row
            moved = pltpu.roll(got_ref[pl.ds(row_ref[2, b], 1), :], row_ref[3, b], 1)
            value = moved if four == 0 else jnp.where(lane >= 32 * four, moved, value)
        third_ref[row : row + 1, :] = value

    low = lane_of((8, LANES)) < 64
    for start in range(0, 64 * PIECE, 200):
        turned_ref[start : start + 200, :] = pltpu.roll(got_ref[start : start + 200, :], 64, 1)

    def counted(count_ref, b, inside):
        row_b = fixed_ref[pl.ds(b, 1), :].astype(jnp.bfloat16)
        count_ref[256 * inside : 256 * inside + 256, :] = dot(pairs_ref[...] * row_b, allowed_ref[...])

    def summed(count_ref, b, inside):
        start, source = row_ref[1, b], row_ref[0, b]

        def first_rows(ref):
            return jnp.concatenate((ref[pl.ds(source, 4), :], ref[pl.ds(source + PIECE, 4), :]), axis=0)

        first, turned = first_rows(got_ref), first_rows(turned_ref)
        by_same = jnp.where(low, first, turned)
        by_other = jnp.where(low, -turned, first)
        second = got_ref[pl.ds(start, 32, stride=2 * PIECE), :]
        other = turned_ref[pl.ds(start, 32, stride=2 * PIECE), :]
        for h in range(2):
            terms = []
            for e in range(4):
                q = 4 * h + e
                term = by_same[q : q + 1] * second + by_other[q : q + 1] * other
                terms.append(term * count_ref[256 * inside + 32 * q : 256 * inside + 32 * q + 32, :])
            columns = jnp.concatenate(terms, axis=0).T
            for part in range(2):
                total = jnp.sum(columns[64 * part : 64 * part + 64].reshape(8, 8, LANES), axis=0)
                sum_ref[2 * part + h, pl.ds(pl.multiple_of(8 * b, 8), 8), :] = total

    def several(base, carry):
        b = 2 * UNROLL * base
        for inside in range(UNROLL):
            counted(odd_ref, b + UNROLL + inside, inside)
            summed(even_ref, b + inside, inside)
        for inside in range(UNROLL):
            counted(even_ref, (b + 2 * UNROLL + inside) % 64, inside)
            summed(odd_ref, b + UNROLL + inside, inside)
        return carry

    for inside in range(UNROLL):
        counted(even_ref, inside, inside)
    lax.fori_loop(0, 32 // UNROLL, several, 0)
    for part in range(2):
        for h in range(2):
            total = jnp.zeros((64, LANES), jnp.float32)
            for sublane in range(8):
                total += sum_ref[2 * part + h, pl.ds(sublane, 64, stride=8), :]
            whole_ref[2 * part + h] = total
    for h in range(2):
        parts = [whole_ref[2 * part + h, 16 * four : 16 * four + 16] for four in range(4) for part in range(2)]
        for group in range(8):
            out_ref[8 * h + group] = regrouped(parts, group)


def outer_kernel(third_ref, got_ref, out_ref):
    total = jnp.sum(got_ref[...], axis=0)
    second_half = (lane_of((16, LANES)) & 16) != 0
    other = jnp.where(second_half, pltpu.roll(total, 16, 1), pltpu.roll(total, LANES - 16, 1))
    third = third_ref[...]
    real = third * jnp.where(second_half, -total, total)
    imag = third * other
    columns = jnp.concatenate((real, imag, jnp.zeros((96, LANES), jnp.float32)), axis=0).T
    sums = [jnp.sum(columns[32 * four : 32 * four + 32, :32], axis=0, keepdims=True) for four in range(4)]
    result = jnp.concatenate([x[:, :16] for x in sums] + [x[:, 16:] for x in sums], axis=1)
    for to in range(16):
        out_ref[to] = result


def all_reduced(copies, axes, rows):
    got = lax.all_to_all(copies, axes, 0, 0, tiled=True)
    total = jnp.sum(got, axis=0, keepdims=True)
    return jnp.broadcast_to(total, (rows,) + total.shape[1:])


def on_device(boundary, gate_stack, layer_order, cut_index, slice_bits, bitstrings):
    smem = pl.BlockSpec(memory_space=pltpu.SMEM)
    vmem = pl.BlockSpec(memory_space=pltpu.VMEM)
    hbm = pl.BlockSpec(memory_space=pltpu.HBM)
    in_hbm = partial(pltpu.with_memory_space_constraint, memory_space=pltpu.HBM)
    strings = bitstrings.T
    pieces, rows = pl.pallas_call(
        pack_kernel,
        out_shape=(
            jax.ShapeDtypeStruct((64 * PIECE, LANES), jnp.float32),
            jax.ShapeDtypeStruct((8, 64), jnp.int32),
        ),
        in_specs=[hbm] * 5,
        out_specs=(vmem, vmem),
        scratch_shapes=[
            pltpu.SMEM((3,), jnp.int32),
            pltpu.SMEM((1, 6), jnp.int32),
            pltpu.VMEM((20, 64), jnp.int32),
            pltpu.VMEM((3, 2, 16, 1024), jnp.float32),
            pltpu.VMEM((4, 512, 8, 32), jnp.float32),
            pltpu.VMEM((64, 512), jnp.bfloat16),
            pltpu.SemaphoreType.DMA((8,)),
        ],
        compiler_params=pltpu.CompilerParams(vmem_limit_bytes=24 << 20),
        name="pack",
    )(*(in_hbm(x) for x in (layer_order, slice_bits, strings, gate_stack, boundary.reshape(512, 32, 32))))
    pieces = pieces.reshape(64, 1, PIECE * LANES)
    got = lax.all_to_all(pieces, CUTS, 0, 0, tiled=True).reshape(64 * PIECE, LANES)
    inner, third = pl.pallas_call(
        inner_kernel,
        out_shape=(
            jax.ShapeDtypeStruct((16, 16, LANES), jnp.float32),
            jax.ShapeDtypeStruct((16, LANES), jnp.float32),
        ),
        in_specs=[smem, smem, vmem, vmem],
        out_specs=(vmem, vmem),
        scratch_shapes=[
            pltpu.VMEM((256, 64), jnp.bfloat16),
            pltpu.VMEM((64, LANES), jnp.bfloat16),
            pltpu.VMEM((64, 64), jnp.float32),
            pltpu.VMEM((4, 512, LANES), jnp.float32),
            pltpu.VMEM((4, 64, LANES), jnp.float32),
            pltpu.VMEM((64 * PIECE, LANES), jnp.float32),
            pltpu.VMEM((256 * UNROLL, LANES), jnp.float32),
            pltpu.VMEM((256 * UNROLL, LANES), jnp.float32),
        ],
        compiler_params=pltpu.CompilerParams(vmem_limit_bytes=16 << 20),
        name="inner",
    )(rows, in_hbm(cut_index.T), in_hbm(strings), got)
    inner = lax.all_to_all(inner, WAVE, 0, 0, tiled=True)
    partial_sums = pl.pallas_call(
        outer_kernel,
        out_shape=jax.ShapeDtypeStruct((16, 1, LANES), jnp.float32),
        in_specs=[vmem, vmem],
        out_specs=vmem,
        compiler_params=pltpu.CompilerParams(vmem_limit_bytes=8 << 20),
        name="outer",
    )(third, inner)
    total = all_reduced(partial_sums, COLUMN, 16)
    total = all_reduced(total, PLANE, 1)
    return total.reshape(2, 64).T


def solution(mesh):
    finer = Mesh(
        mesh.devices.reshape(AXES + (mesh.shape["grp"],)),
        CUTS + ("grp",),
    )
    return jax.shard_map(
        on_device,
        mesh=finer,
        in_specs=(
            P("grp", None, None, None, None),
            P(None, None, CUTS, None),
            P(),
            P(),
            P(CUTS, None),
            P(),
        ),
        out_specs=P(),
        check_vma=False,
    )
```

```python
from functools import partial

import jax
import jax.numpy as jnp
from jax import lax
from jax.experimental import pallas as pl
from jax.experimental.pallas import tpu as pltpu
from jax.sharding import Mesh
from jax.sharding import PartitionSpec as P

AXES = (4, 4, 2, 2)
CUTS = ("cuts_0", "cuts_1", "cuts_2", "cuts_3")
WAVE = ("cuts_1", "cuts_2", "cuts_3")
PLANE = ("cuts_0", "cuts_1")
COLUMN = ("cuts_2", "cuts_3", "grp")

BLOCKS_I, BLOCKS_J = 4, 16
LANES = 128
UNROLL = 8
ROW_SECOND, ROW_FIRST, ROW_THIRD, ROW_BITS, PIECE = 0, 16, 20, 24, 25


def split_high_low(array):
    high = array.astype(jnp.bfloat16)
    return high, (array - high.astype(jnp.float32)).astype(jnp.bfloat16)


def dot(left, right):
    return jnp.dot(left, right, preferred_element_type=jnp.float32)


def lane_of(shape):
    return lax.broadcasted_iota(jnp.int32, shape, 1)


def side_by_side(real, imag):
    low = lane_of(real.shape) < 64
    return jnp.where(low, real, pltpu.roll(imag, 64, 1)), jnp.where(low, pltpu.roll(real, 64, 1), imag)


def regrouped(parts, group):
    lane = lane_of(parts[0].shape)
    result = None
    for place, part in enumerate(parts):
        shift = 16 * (place - group) % LANES
        moved = pltpu.roll(part, shift, 1) if shift else part
        result = moved if place == 0 else jnp.where(lane >= 16 * place, moved, result)
    return result


def place_in_blocks():
    place = 0
    for axis, size in zip(CUTS, AXES, strict=True):
        place = place * size + lax.axis_index(axis)
    return place // BLOCKS_J, place % BLOCKS_J


def sign_tables(cut_ref, string_ref, pair_ref, j_ref, fixed_ref):
    block_i, block_j = place_in_blocks()
    lane, sublane = lane_of((1, LANES)), lax.broadcasted_iota(jnp.int32, (8, 1), 0)
    zero_row, zero_column = jnp.zeros((1, LANES), jnp.int32), jnp.zeros((8, 1), jnp.int32)
    pair_on, pair_bit, pair_i1 = zero_row, zero_row, zero_row
    j_on, j_bit, j_j2 = zero_column, zero_column, zero_column
    pair_count, j_count, fixed_count = 0, 0, 0
    strings = jnp.zeros((8, 64), jnp.int32)
    for cut in range(6):
        layer, group, bit = cut_ref[0, cut], cut_ref[1, cut], cut_ref[2, cut]
        on_i1 = jnp.where((group == 1) & (layer < 2), 1, 0)
        on_i2 = jnp.where((group == 2) & (layer == 1), 1, 0)
        on_j2 = jnp.where((group == 2) & (layer == 0), 1, 0)
        on_j3 = jnp.where((group == 3) & (layer == 0), 1, 0)
        on_fixed = 1 - on_i1 - on_i2 - on_j2 - on_j3
        pair_on = jnp.where(lane == cut, on_i1 + on_i2, pair_on)
        pair_bit = jnp.where(lane == cut, bit, pair_bit)
        pair_i1 = jnp.where(lane == cut, on_i1, pair_i1)
        j_on = jnp.where(sublane == cut, on_j2 + on_j3, j_on)
        j_bit = jnp.where(sublane == cut, bit, j_bit)
        j_j2 = jnp.where(sublane == cut, on_j2, j_j2)
        pair_count, j_count, fixed_count = pair_count + on_i1 + on_i2, j_count + on_j2 + on_j3, fixed_count + on_fixed
        sign = on_fixed * (1 - 2 * string_ref[pl.ds(5 * group + bit, 1), :])
        strings = jnp.where(sublane == cut, sign, strings)

    row = lax.broadcasted_iota(jnp.int32, (256, 1), 0)
    i1 = 16 * (row >> 7) + 4 * block_i + ((row >> 5) & 3)
    index = jnp.where(pair_i1 != 0, i1, row & 31)
    signs = jnp.where(lane == 6, -pair_count, pair_on * (1 - 2 * ((index >> pair_bit) & 1)))
    pair_ref[...] = signs.astype(jnp.float32).astype(jnp.bfloat16)
    j = lane & 63
    index = jnp.where(j_j2 != 0, 2 * block_j + (j >> 5), j & 31)
    signs = jnp.where(sublane == 6, -j_count, j_on * (1 - 2 * ((index >> j_bit) & 1)))
    j_ref[...] = signs.astype(jnp.float32)
    strings = jnp.where(sublane == 6, -fixed_count, strings).astype(jnp.float32)
    strings = jnp.concatenate((strings, jnp.zeros_like(strings)), axis=1)
    fixed_ref[...] = jnp.concatenate((strings, jnp.zeros((120, LANES), jnp.float32)), axis=0).T[:64]


def pack_kernel(order_hbm, cut_hbm, bits_hbm, string_hbm, gate_hbm, boundary_hbm, piece_ref, row_ref, pair_ref, j_ref, fixed_ref, order_ref, cut_ref, bits_ref, string_ref, gate_ref, boundary_ref, left_ref, high_ref, low_ref, sems):
    small = [
        pltpu.make_async_copy(order_hbm, order_ref, sems.at[0]),
        pltpu.make_async_copy(bits_hbm, bits_ref, sems.at[1]),
        pltpu.make_async_copy(string_hbm, string_ref, sems.at[2]),
        pltpu.make_async_copy(gate_hbm, gate_ref, sems.at[3]),
        pltpu.make_async_copy(cut_hbm, cut_ref, sems.at[8]),
    ]
    large = [
        pltpu.make_async_copy(boundary_hbm.at[:, pl.ds(8 * step, 8), :], boundary_ref.at[step], sems.at[4 + step])
        for step in range(4)
    ]
    for copy in small + large:
        copy.start()
    for copy in small:
        copy.wait()

    first, second, third = order_ref[0], order_ref[1], order_ref[2]
    member = lax.axis_index("grp")
    columns = pl.ds(pl.multiple_of(member * 256, 256), 256)
    real, imag = gate_ref[first, 0, :, columns], gate_ref[first, 1, :, columns]

    def interleaved(even, odd):
        parts = []
        for k0 in range(8):
            parts += [even[:, 32 * k0 : 32 * k0 + 32], odd[:, 32 * k0 : 32 * k0 + 32]]
        return jnp.concatenate(parts, axis=1)

    left = jnp.concatenate((interleaved(real, -imag), interleaved(imag, real)), axis=0)
    high, low = split_high_low(left)
    left_ref[...] = jnp.concatenate((high, low), axis=0)

    strings = string_ref[...]

    def digit(group):
        total = strings[5 * group : 5 * group + 1]
        for bit in range(1, 5):
            total = total + (strings[5 * group + bit : 5 * group + bit + 1] << bit)
        return total

    g0, g1, g2, g3 = (digit(group) for group in range(4))
    row_ref[0:1, :] = 2 * g0 * PIECE + ROW_FIRST
    row_ref[1:2, :] = (g3 >> 4) * PIECE + ROW_SECOND + (g3 & 15)
    row_ref[2:3, :] = (2 * g1 + (g2 >> 4)) * PIECE + ROW_THIRD + (g2 & 3)
    row_ref[3:4, :] = 32 * (((lane_of((1, 64)) >> 4) - ((g2 & 15) >> 2)) & 3)

    lane = lane_of((1, LANES))
    bits = jnp.zeros((1, LANES), jnp.float32)
    for cut in range(6):
        bits = jnp.where(lane == cut, bits_ref[0, cut].astype(jnp.float32), bits)

    def put(block_i, block_j, at, value):
        start = (block_i * BLOCKS_J + block_j) * PIECE + at
        piece_ref[start : start + value.shape[0], :] = value

    for tile in range(8):
        lanes = slice(LANES * tile, LANES * tile + LANES)
        values = side_by_side(gate_ref[second, 0, :, lanes], gate_ref[second, 1, :, lanes])
        for half in range(2):
            for block_i in range(BLOCKS_I):
                put(block_i, 2 * tile + half, ROW_SECOND, values[half])
    for block_i in range(BLOCKS_I):
        parts = []
        for four in range(4):
            for part in range(2):
                rows = slice(4 * four, 4 * four + 4)
                parts.append(
                    jnp.concatenate(
                        [
                            gate_ref[third, part, rows, 512 * h + LANES * block_i : 512 * h + LANES * block_i + LANES]
                            for h in range(2)
                        ],
                        axis=0,
                    )
                )
        for group in range(8):
            value = regrouped(parts, group)
            put(block_i, group, ROW_THIRD, value[:4])
            put(block_i, 8 + group, ROW_THIRD, value[4:])
    for block_i in range(BLOCKS_I):
        for block_j in range(BLOCKS_J):
            put(block_i, block_j, ROW_BITS, bits)

    sign_tables(cut_ref, string_ref, pair_ref, j_ref, fixed_ref)

    def split(step):
        large[step].wait()
        flat = boundary_ref.at[step].reshape(4096, 32)
        for half in range(2):
            right = jnp.concatenate(
                [flat[pl.ds(4 * half + quarter, 512, stride=8), :] for quarter in range(4)], axis=1
            )
            high_ref[2 * step + half], low_ref[2 * step + half] = split_high_low(right)

    def multiplied(step):
        for tile in (2 * step, 2 * step + 1):
            by_high = dot(left_ref[...], high_ref[tile])
            value = by_high[:32] + by_high[32:] + dot(left_ref[:32], low_ref[tile])
            values = side_by_side(value[:16], value[16:])
            for side in range(2):
                for block_i in range(BLOCKS_I):
                    put(block_i, 2 * tile + side, ROW_FIRST, values[side][4 * block_i : 4 * block_i + 4])

    split(0)
    for step in range(1, 4):
        split(step)
        multiplied(step - 1)
    multiplied(3)


def select_kernel(row_ref, got_ref, out_ref):
    lane = lane_of((1, LANES))
    for row in range(16):
        value = None
        for four in range(4):
            b = 16 * four + row
            moved = pltpu.roll(got_ref[pl.ds(row_ref[2, b], 1), :], row_ref[3, b], 1)
            value = moved if four == 0 else jnp.where(lane >= 32 * four, moved, value)
        for to in range(16):
            out_ref[to, row : row + 1, :] = value


def inner_kernel(row_ref, pair_ref, j_ref, string_ref, got_ref, same_ref, other_ref, pairs_ref, allowed_ref, fixed_ref, sum_ref, whole_ref, turned_ref, even_ref, odd_ref):
    lane = lane_of((1, LANES))
    signs = 1.0 - 2.0 * got_ref[pl.ds(ROW_BITS, 64, stride=PIECE), :]
    signs = jnp.where(lane < 6, signs, jnp.where(lane == 6, 1.0, 0.0)).astype(jnp.bfloat16)

    def one_if_all(differing, kind):
        return jnp.where(differing == 0.0, 1.0, 0.0).astype(kind)

    def against_slices(table):
        return lax.dot_general(table, signs, (((1,), (1,)), ((), ())), preferred_element_type=jnp.float32)

    fixed_ref[...] = one_if_all(against_slices(string_ref[...].astype(jnp.bfloat16)), jnp.float32)
    pairs_ref[...] = one_if_all(against_slices(pair_ref[...]), jnp.bfloat16)
    allowed_ref[...] = one_if_all(dot(signs[:, :8], j_ref[...].astype(jnp.bfloat16)), jnp.bfloat16)

    low = lane_of((8, LANES)) < 64
    for start in range(0, 64 * PIECE, 200):
        turned_ref[start : start + 200, :] = pltpu.roll(got_ref[start : start + 200, :], 64, 1)

    def counted(count_ref, b, inside):
        row_b = fixed_ref[pl.ds(b, 1), :].astype(jnp.bfloat16)
        count_ref[256 * inside : 256 * inside + 256, :] = dot(pairs_ref[...] * row_b, allowed_ref[...])

    def summed(count_ref, b, inside):
        start, source = row_ref[1, b], row_ref[0, b]

        def first_rows(ref):
            return jnp.concatenate((ref[pl.ds(source, 4), :], ref[pl.ds(source + PIECE, 4), :]), axis=0)

        first, turned = first_rows(got_ref), first_rows(turned_ref)
        by_same = jnp.where(low, first, turned)
        by_other = jnp.where(low, -turned, first)
        second = got_ref[pl.ds(start, 32, stride=2 * PIECE), :]
        other = turned_ref[pl.ds(start, 32, stride=2 * PIECE), :]
        for h in range(2):
            terms = []
            for e in range(4):
                q = 4 * h + e
                term = by_same[q : q + 1] * second + by_other[q : q + 1] * other
                terms.append(term * count_ref[256 * inside + 32 * q : 256 * inside + 32 * q + 32, :])
            columns = jnp.concatenate(terms, axis=0).T
            for part in range(2):
                total = jnp.sum(columns[64 * part : 64 * part + 64].reshape(8, 8, LANES), axis=0)
                sum_ref[2 * part + h, pl.ds(pl.multiple_of(8 * b, 8), 8), :] = total

    def several(base, carry):
        b = 2 * UNROLL * base
        for inside in range(UNROLL):
            counted(odd_ref, b + UNROLL + inside, inside)
            summed(even_ref, b + inside, inside)
        for inside in range(UNROLL):
            counted(even_ref, (b + 2 * UNROLL + inside) % 64, inside)
            summed(odd_ref, b + UNROLL + inside, inside)
        return carry

    for inside in range(UNROLL):
        counted(even_ref, inside, inside)
    lax.fori_loop(0, 32 // UNROLL, several, 0)
    for part in range(2):
        for h in range(2):
            total = jnp.zeros((64, LANES), jnp.float32)
            for sublane in range(8):
                total += sum_ref[2 * part + h, pl.ds(sublane, 64, stride=8), :]
            whole_ref[2 * part + h] = total
    for h in range(2):
        parts = [whole_ref[2 * part + h, 16 * four : 16 * four + 16] for four in range(4) for part in range(2)]
        for group in range(8):
            value = regrouped(parts, group)
            imag = (lane_of(value.shape) & 16) != 0
            same_ref[8 * h + group] = jnp.where(imag, -value, value)
            other_ref[8 * h + group] = jnp.where(imag, pltpu.roll(value, 16, 1), pltpu.roll(value, LANES - 16, 1))


def outer_kernel(third_ref, same_ref, other_ref, out_ref):
    third = third_ref[...]
    real = jnp.sum(third * same_ref[...], axis=0)
    imag = jnp.sum(third * other_ref[...], axis=0)
    columns = jnp.concatenate((real, imag, jnp.zeros((96, LANES), jnp.float32)), axis=0).T
    sums = [jnp.sum(columns[32 * four : 32 * four + 32, :32], axis=0, keepdims=True) for four in range(4)]
    unused = [jnp.zeros((1, 64), jnp.float32)]
    real = jnp.concatenate([x[:, :16] for x in sums] + unused, axis=1)
    imag = jnp.concatenate([x[:, 16:] for x in sums] + unused, axis=1)
    for to in range(16):
        out_ref[to, 0:1, :] = real
        out_ref[to, 1:2, :] = imag


def all_reduced(copies, axes, rows):
    got = lax.all_to_all(copies, axes, 0, 0, tiled=True)
    total = jnp.sum(got, axis=0, keepdims=True)
    return jnp.broadcast_to(total, (rows,) + total.shape[1:])


def on_device(boundary, gate_stack, layer_order, cut_index, slice_bits, bitstrings):
    smem = pl.BlockSpec(memory_space=pltpu.SMEM)
    vmem = pl.BlockSpec(memory_space=pltpu.VMEM)
    hbm = pl.BlockSpec(memory_space=pltpu.HBM)
    in_hbm = partial(pltpu.with_memory_space_constraint, memory_space=pltpu.HBM)
    strings = bitstrings.T
    pieces, rows, *tables = pl.pallas_call(
        pack_kernel,
        out_shape=(
            jax.ShapeDtypeStruct((64 * PIECE, LANES), jnp.float32),
            jax.ShapeDtypeStruct((8, 64), jnp.int32),
            jax.ShapeDtypeStruct((256, LANES), jnp.bfloat16),
            jax.ShapeDtypeStruct((8, LANES), jnp.float32),
            jax.ShapeDtypeStruct((64, LANES), jnp.float32),
        ),
        in_specs=[hbm] * 6,
        out_specs=(vmem,) * 5,
        scratch_shapes=[
            pltpu.SMEM((3,), jnp.int32),
            pltpu.SMEM((3, 6), jnp.int32),
            pltpu.SMEM((1, 6), jnp.int32),
            pltpu.VMEM((20, 64), jnp.int32),
            pltpu.VMEM((3, 2, 16, 1024), jnp.float32),
            pltpu.VMEM((4, 512, 8, 32), jnp.float32),
            pltpu.VMEM((64, 512), jnp.bfloat16),
            pltpu.VMEM((8, 512, LANES), jnp.bfloat16),
            pltpu.VMEM((8, 512, LANES), jnp.bfloat16),
            pltpu.SemaphoreType.DMA((9,)),
        ],
        compiler_params=pltpu.CompilerParams(vmem_limit_bytes=24 << 20),
        name="pack",
    )(*(in_hbm(x) for x in (layer_order, cut_index.T, slice_bits, strings, gate_stack, boundary.reshape(512, 32, 32))))
    pieces = pieces.reshape(64, 1, PIECE * LANES)
    got = lax.all_to_all(pieces, CUTS, 0, 0, tiled=True).reshape(64 * PIECE, LANES)
    third = pl.pallas_call(
        select_kernel,
        out_shape=jax.ShapeDtypeStruct((16, 16, LANES), jnp.float32),
        in_specs=[smem, vmem],
        out_specs=vmem,
        compiler_params=pltpu.CompilerParams(vmem_limit_bytes=8 << 20),
        name="select",
    )(rows, got)
    third = lax.all_to_all(third, WAVE, 0, 0, tiled=True)
    same, other = pl.pallas_call(
        inner_kernel,
        out_shape=(jax.ShapeDtypeStruct((16, 16, LANES), jnp.float32),) * 2,
        in_specs=[smem] + [vmem] * 4,
        out_specs=(vmem, vmem),
        scratch_shapes=[
            pltpu.VMEM((256, 64), jnp.bfloat16),
            pltpu.VMEM((64, LANES), jnp.bfloat16),
            pltpu.VMEM((64, 64), jnp.float32),
            pltpu.VMEM((4, 512, LANES), jnp.float32),
            pltpu.VMEM((4, 64, LANES), jnp.float32),
            pltpu.VMEM((64 * PIECE, LANES), jnp.float32),
            pltpu.VMEM((256 * UNROLL, LANES), jnp.float32),
            pltpu.VMEM((256 * UNROLL, LANES), jnp.float32),
        ],
        compiler_params=pltpu.CompilerParams(vmem_limit_bytes=16 << 20),
        cost_estimate=pl.CostEstimate(flops=1 << 30, bytes_accessed=1 << 20, transcendentals=0),
        name="inner",
    )(rows, *tables, got)
    partial_sums = pl.pallas_call(
        outer_kernel,
        out_shape=jax.ShapeDtypeStruct((16, 2, LANES), jnp.float32),
        in_specs=[vmem, vmem, vmem],
        out_specs=vmem,
        compiler_params=pltpu.CompilerParams(vmem_limit_bytes=8 << 20),
        name="outer",
    )(third, same, other)
    total = all_reduced(partial_sums, COLUMN, 16)
    total = all_reduced(total, PLANE, 1)
    return total[0, :, :64].T


def solution(mesh):
    finer = Mesh(
        mesh.devices.reshape(AXES + (mesh.shape["grp"],)),
        CUTS + ("grp",),
    )
    return jax.shard_map(
        on_device,
        mesh=finer,
        in_specs=(
            P("grp", None, None, None, None),
            P(None, None, CUTS, None),
            P(),
            P(),
            P(CUTS, None),
            P(),
        ),
        out_specs=P(),
        check_vma=False,
    )
```

```python
from functools import partial

import jax
import jax.numpy as jnp
from jax import lax
from jax.experimental import pallas as pl
from jax.experimental.pallas import tpu as pltpu
from jax.sharding import Mesh
from jax.sharding import PartitionSpec as P

AXES = (2, 2, 4, 2, 2)
CUTS = ("cuts_0", "cuts_1", "cuts_2", "cuts_3", "cuts_4")
WAVE = ("cuts_1", "cuts_2", "cuts_3")
CORES = "cuts_4"
PLANE = ("cuts_0", "cuts_1", "cuts_2")
COLUMN = ("cuts_3", "cuts_4", "grp")

BLOCKS_I, BLOCKS_J = 4, 16
LANES = 128
UNROLL = 8
ROW_SECOND, ROW_FIRST, ROW_THIRD, ROW_BITS, PIECE = 0, 8, 12, 16, 17
SPACED, HALF = 9, 64 * 9


def split_high_rest(array):
    high = array.astype(jnp.bfloat16)
    return high, array - high.astype(jnp.float32)


def split_high_low(array):
    high, rest = split_high_rest(array)
    return high, rest.astype(jnp.bfloat16)


def dot(left, right):
    return jnp.dot(left, right, preferred_element_type=jnp.float32)


def lane_of(shape):
    return lax.broadcasted_iota(jnp.int32, shape, 1)


def side_by_side(real, imag):
    low = lane_of(real.shape) < 64
    return jnp.where(low, real, pltpu.roll(imag, 64, 1)), jnp.where(low, pltpu.roll(real, 64, 1), imag)


def regrouped(parts, group):
    lane = lane_of(parts[0].shape)
    result = None
    for place, part in enumerate(parts):
        shift = 16 * (place - group) % LANES
        moved = pltpu.roll(part, shift, 1) if shift else part
        result = moved if place == 0 else jnp.where(lane >= 16 * place, moved, result)
    return result


def place_in_blocks():
    block_j = 0
    for axis, size in zip(WAVE, AXES[1:4], strict=True):
        block_j = block_j * size + lax.axis_index(axis)
    return 2 * lax.axis_index(CUTS[0]) + lax.axis_index(CORES), block_j


def sign_tables(cut_ref, string_ref, third_row, third_move, pair_ref, j_ref, fixed_ref, chosen_ref):
    block_i, block_j = place_in_blocks()
    lane, sublane = lane_of((1, LANES)), lax.broadcasted_iota(jnp.int32, (8, 1), 0)
    zero_row, zero_column = jnp.zeros((1, LANES), jnp.int32), jnp.zeros((8, 1), jnp.int32)
    pair_on, pair_bit, pair_i1 = zero_row, zero_row, zero_row
    j_on, j_bit, j_j2 = zero_column, zero_column, zero_column
    pair_count, j_count, fixed_count = 0, 0, 0
    strings = jnp.zeros((8, 64), jnp.int32)
    for cut in range(6):
        layer, group, bit = cut_ref[0, cut], cut_ref[1, cut], cut_ref[2, cut]
        on_i1 = jnp.where((group == 1) & (layer < 2), 1, 0)
        on_i2 = jnp.where((group == 2) & (layer == 1), 1, 0)
        on_j2 = jnp.where((group == 2) & (layer == 0), 1, 0)
        on_j3 = jnp.where((group == 3) & (layer == 0), 1, 0)
        on_fixed = 1 - on_i1 - on_i2 - on_j2 - on_j3
        pair_on = jnp.where(lane == cut, on_i1 + on_i2, pair_on)
        pair_bit = jnp.where(lane == cut, bit, pair_bit)
        pair_i1 = jnp.where(lane == cut, on_i1, pair_i1)
        j_on = jnp.where(sublane == cut, on_j2 + on_j3, j_on)
        j_bit = jnp.where(sublane == cut, bit, j_bit)
        j_j2 = jnp.where(sublane == cut, on_j2, j_j2)
        pair_count, j_count, fixed_count = pair_count + on_i1 + on_i2, j_count + on_j2 + on_j3, fixed_count + on_fixed
        sign = on_fixed * (1 - 2 * string_ref[pl.ds(5 * group + bit, 1), :])
        strings = jnp.where(sublane == cut, sign, strings)

    row = lax.broadcasted_iota(jnp.int32, (256, 1), 0)
    i1 = 16 * (row >> 7) + 4 * block_i + ((row >> 5) & 3)
    index = jnp.where(pair_i1 != 0, i1, row & 31)
    signs = jnp.where(lane == 6, -pair_count, pair_on * (1 - 2 * ((index >> pair_bit) & 1)))
    pair_ref[...] = signs.astype(jnp.float32).astype(jnp.bfloat16)
    j = lane & 63
    index = jnp.where(j_j2 != 0, 2 * block_j + (j >> 5), j & 31)
    signs = jnp.where(sublane == 6, -j_count, j_on * (1 - 2 * ((index >> j_bit) & 1)))
    j_ref[...] = signs.astype(jnp.float32)
    strings = jnp.where(sublane == 6, -fixed_count, strings)
    strings = jnp.concatenate((strings, third_row, third_move), axis=0).astype(jnp.float32)
    strings = jnp.concatenate((strings, jnp.zeros((118, 64), jnp.float32)), axis=0)
    columns = jnp.concatenate((strings, jnp.zeros_like(strings)), axis=1).T[:64]
    fixed_ref[...] = columns
    hit = lane_of((64, 256)).astype(jnp.float32) == columns[:, 8:9]
    for move in range(4):
        one = jnp.where(hit & (columns[:, 9:10] == move), 1.0, 0.0)
        chosen_ref[64 * move : 64 * move + 64, :] = one.astype(jnp.bfloat16)


def pack_kernel(order_hbm, cut_hbm, bits_hbm, string_hbm, gate_hbm, boundary_hbm, piece_ref, row_ref, chosen_ref, pair_ref, j_ref, fixed_ref, order_ref, cut_ref, bits_ref, string_ref, gate_ref, boundary_ref, left_ref, high_ref, low_ref, sems):
    small = [
        pltpu.make_async_copy(order_hbm, order_ref, sems.at[0]),
        pltpu.make_async_copy(bits_hbm, bits_ref, sems.at[1]),
        pltpu.make_async_copy(string_hbm, string_ref, sems.at[2]),
        pltpu.make_async_copy(gate_hbm, gate_ref, sems.at[3]),
        pltpu.make_async_copy(cut_hbm, cut_ref, sems.at[8]),
    ]
    large = [
        pltpu.make_async_copy(boundary_hbm.at[:, pl.ds(8 * step, 8), :], boundary_ref.at[step], sems.at[4 + step])
        for step in range(4)
    ]
    for copy in small + large:
        copy.start()
    for copy in small:
        copy.wait()

    first, second, third = order_ref[0], order_ref[1], order_ref[2]
    member = lax.axis_index("grp")
    columns = pl.ds(pl.multiple_of(member * 256, 256), 256)
    real, imag = gate_ref[first, 0, :, columns], gate_ref[first, 1, :, columns]

    def interleaved(even, odd):
        parts = []
        for k0 in range(8):
            parts += [even[:, 32 * k0 : 32 * k0 + 32], odd[:, 32 * k0 : 32 * k0 + 32]]
        return jnp.concatenate(parts, axis=1)

    left = jnp.concatenate((interleaved(real, -imag), interleaved(imag, real)), axis=0)
    high, low = split_high_low(left)
    left_ref[...] = jnp.concatenate((high, low), axis=0)

    strings = string_ref[...]

    def digit(group):
        total = strings[5 * group : 5 * group + 1]
        for bit in range(1, 5):
            total = total + (strings[5 * group + bit : 5 * group + bit + 1] << bit)
        return total

    g0, g1, g2, g3 = (digit(group) for group in range(4))
    row_ref[0:1, :] = 8 * g0
    row_ref[1:2, :] = ((g3 & 15) >> 3) * HALF + (g3 >> 4) * SPACED + (g3 & 7)
    third_row = (g2 & 3) * 64 + 2 * g1 + (g2 >> 4)
    third_move = ((lane_of((1, 64)) >> 4) - ((g2 & 15) >> 2)) & 3

    lane = lane_of((1, LANES))
    bits = jnp.zeros((1, LANES), jnp.float32)
    for cut in range(6):
        bits = jnp.where(lane == cut, bits_ref[0, cut].astype(jnp.float32), bits)

    def put(block_i, block_j, at, value):
        start = ((block_i // 2 * BLOCKS_J + block_j) * 2 + block_i % 2) * PIECE + at
        piece_ref[start : start + value.shape[0], :] = value

    for tile in range(8):
        lanes = slice(LANES * tile, LANES * tile + LANES)
        values = side_by_side(gate_ref[second, 0, :, lanes], gate_ref[second, 1, :, lanes])
        for half in range(2):
            for block_i in range(BLOCKS_I):
                eight = 8 * (block_i % 2)
                put(block_i, 2 * tile + half, ROW_SECOND, values[half][eight : eight + 8])
    for block_i in range(BLOCKS_I):
        parts = []
        for four in range(4):
            for part in range(2):
                rows = slice(4 * four, 4 * four + 4)
                parts.append(
                    jnp.concatenate(
                        [
                            gate_ref[third, part, rows, 512 * h + LANES * block_i : 512 * h + LANES * block_i + LANES]
                            for h in range(2)
                        ],
                        axis=0,
                    )
                )
        for group in range(8):
            value = regrouped(parts, group)
            put(block_i, group, ROW_THIRD, value[:4])
            put(block_i, 8 + group, ROW_THIRD, value[4:])
    for block_i in range(BLOCKS_I):
        for block_j in range(BLOCKS_J):
            put(block_i, block_j, ROW_BITS, bits)

    sign_tables(cut_ref, string_ref, third_row, third_move, pair_ref, j_ref, fixed_ref, chosen_ref)

    def split(step):
        large[step].wait()
        flat = boundary_ref.at[step].reshape(4096, 32)
        for half in range(2):
            right = jnp.concatenate(
                [flat[pl.ds(4 * half + quarter, 512, stride=8), :] for quarter in range(4)], axis=1
            )
            high_ref[2 * step + half], low_ref[2 * step + half] = split_high_low(right)

    def multiplied(step):
        for tile in (2 * step, 2 * step + 1):
            by_high = dot(left_ref[...], high_ref[tile])
            value = by_high[:32] + by_high[32:] + dot(left_ref[:32], low_ref[tile])
            values = side_by_side(value[:16], value[16:])
            for side in range(2):
                for block_i in range(BLOCKS_I):
                    put(block_i, 2 * tile + side, ROW_FIRST, values[side][4 * block_i : 4 * block_i + 4])

    split(0)
    for step in range(1, 4):
        split(step)
        multiplied(step - 1)
    multiplied(3)


def select_kernel(chosen_ref, got_ref, out_ref, half_ref):
    rows = [got_ref[pl.ds(ROW_THIRD + row, 64, stride=PIECE), :] for row in range(4)]
    high, rest = split_high_rest(jnp.concatenate(rows, axis=0))
    middle, rest = split_high_rest(rest)
    chosen = chosen_ref[...]
    found = dot(chosen, high) + (dot(chosen, middle) + dot(chosen, rest.astype(jnp.bfloat16)))
    total = found[:64]
    for move in range(1, 4):
        total = total + pltpu.roll(found[64 * move : 64 * move + 64], 32 * move, 1)
    lane, value = lane_of((16, LANES)), total[:16]
    for four in range(1, 4):
        value = jnp.where(lane >= 32 * four, total[16 * four : 16 * four + 16], value)
    for to in range(16):
        out_ref[to] = value
    for source in range(64):
        half_ref[8 * source : 8 * source + 8, :] = got_ref[PIECE * source : PIECE * source + 8, :]


def inner_kernel(row_ref, pair_ref, j_ref, string_ref, got_ref, mine_ref, theirs_ref, same_ref, other_ref, pairs_ref, allowed_ref, fixed_ref, sum_ref, whole_ref, second_ref, turned_ref, by_same_ref, by_other_ref, even_ref, odd_ref):
    lane = lane_of((1, LANES))
    signs = 1.0 - 2.0 * got_ref[pl.ds(ROW_BITS, 64, stride=PIECE), :]
    signs = jnp.where(lane < 6, signs, jnp.where(lane == 6, 1.0, 0.0)).astype(jnp.bfloat16)

    def one_if_all(differing, kind):
        return jnp.where(differing == 0.0, 1.0, 0.0).astype(kind)

    def against_slices(table):
        return lax.dot_general(table, signs, (((1,), (1,)), ((), ())), preferred_element_type=jnp.float32)

    fixed_ref[...] = one_if_all(against_slices(string_ref[...].astype(jnp.bfloat16)), jnp.float32)
    pairs_ref[...] = one_if_all(against_slices(pair_ref[...]), jnp.bfloat16)
    allowed_ref[...] = one_if_all(dot(signs[:, :8], j_ref[...].astype(jnp.bfloat16)), jnp.bfloat16)

    core = lax.axis_index(CORES)
    for ref, half in ((mine_ref, core), (theirs_ref, 1 - core)):
        for source in range(64):
            rows = ref[8 * source : 8 * source + 8, :]
            at = pl.ds(half * HALF + SPACED * source, 8)
            second_ref[at, :] = rows
            turned_ref[at, :] = pltpu.roll(rows, 64, 1)
    low = lane_of((8, LANES)) < 64
    for g0 in range(32):
        start = 2 * g0 * PIECE + ROW_FIRST
        first = jnp.concatenate((got_ref[start : start + 4, :], got_ref[start + PIECE : start + PIECE + 4, :]), axis=0)
        turned = pltpu.roll(first, 64, 1)
        by_same_ref[8 * g0 : 8 * g0 + 8, :] = jnp.where(low, first, turned)
        by_other_ref[8 * g0 : 8 * g0 + 8, :] = jnp.where(low, -turned, first)

    def counted(count_ref, b, inside):
        row_b = fixed_ref[pl.ds(b, 1), :].astype(jnp.bfloat16)
        count_ref[256 * inside : 256 * inside + 256, :] = dot(pairs_ref[...] * row_b, allowed_ref[...])

    def summed(count_ref, b, inside):
        start = row_ref[1, b]
        eight = pl.ds(pl.multiple_of(row_ref[0, b], 8), 8)
        by_same, by_other = by_same_ref[eight, :], by_other_ref[eight, :]
        second = second_ref[pl.ds(start, 32, stride=2 * SPACED), :]
        other = turned_ref[pl.ds(start, 32, stride=2 * SPACED), :]
        for h in range(2):
            terms = []
            for e in range(4):
                q = 4 * h + e
                term = by_same[q : q + 1] * second + by_other[q : q + 1] * other
                terms.append(term * count_ref[256 * inside + 32 * q : 256 * inside + 32 * q + 32, :])
            columns = jnp.concatenate(terms, axis=0).T
            for part in range(2):
                total = jnp.sum(columns[64 * part : 64 * part + 64].reshape(8, 8, LANES), axis=0)
                sum_ref[2 * part + h, pl.ds(pl.multiple_of(8 * b, 8), 8), :] = total

    def several(base, carry):
        b = 2 * UNROLL * base
        for inside in range(UNROLL):
            counted(odd_ref, b + UNROLL + inside, inside)
            summed(even_ref, b + inside, inside)
        for inside in range(UNROLL):
            counted(even_ref, (b + 2 * UNROLL + inside) % 64, inside)
            summed(odd_ref, b + UNROLL + inside, inside)
        return carry

    for inside in range(UNROLL):
        counted(even_ref, inside, inside)
    lax.fori_loop(0, 32 // UNROLL, several, 0)
    for part in range(2):
        for h in range(2):
            total = jnp.zeros((64, LANES), jnp.float32)
            for sublane in range(8):
                total += sum_ref[2 * part + h, pl.ds(sublane, 64, stride=8), :]
            whole_ref[2 * part + h] = total
    for h in range(2):
        parts = [whole_ref[2 * part + h, 16 * four : 16 * four + 16] for four in range(4) for part in range(2)]
        for group in range(8):
            value = regrouped(parts, group)
            imag = (lane_of(value.shape) & 16) != 0
            same_ref[8 * h + group] = jnp.where(imag, -value, value)
            other_ref[8 * h + group] = jnp.where(imag, pltpu.roll(value, 16, 1), pltpu.roll(value, LANES - 16, 1))


def outer_kernel(third_ref, same_ref, other_ref, out_ref):
    third = third_ref[...]
    real = jnp.sum(third * same_ref[...], axis=0)
    imag = jnp.sum(third * other_ref[...], axis=0)
    columns = jnp.concatenate((real, imag, jnp.zeros((96, LANES), jnp.float32)), axis=0).T
    sums = [jnp.sum(columns[32 * four : 32 * four + 32, :32], axis=0, keepdims=True) for four in range(4)]
    unused = [jnp.zeros((1, 64), jnp.float32)]
    real = jnp.concatenate([x[:, :16] for x in sums] + unused, axis=1)
    imag = jnp.concatenate([x[:, 16:] for x in sums] + unused, axis=1)
    for to in range(16):
        out_ref[to, 0:1, :] = real
        out_ref[to, 1:2, :] = imag


def all_reduced(copies, axes, rows):
    got = lax.all_to_all(copies, axes, 0, 0, tiled=True)
    total = jnp.sum(got, axis=0, keepdims=True)
    return jnp.broadcast_to(total, (rows,) + total.shape[1:])


def on_device(boundary, gate_stack, layer_order, cut_index, slice_bits, bitstrings):
    smem = pl.BlockSpec(memory_space=pltpu.SMEM)
    vmem = pl.BlockSpec(memory_space=pltpu.VMEM)
    hbm = pl.BlockSpec(memory_space=pltpu.HBM)
    in_hbm = partial(pltpu.with_memory_space_constraint, memory_space=pltpu.HBM)
    strings = bitstrings.T
    pieces, rows, chosen, *tables = pl.pallas_call(
        pack_kernel,
        out_shape=(
            jax.ShapeDtypeStruct((64 * PIECE, LANES), jnp.float32),
            jax.ShapeDtypeStruct((8, 64), jnp.int32),
            jax.ShapeDtypeStruct((256, 256), jnp.bfloat16),
            jax.ShapeDtypeStruct((256, LANES), jnp.bfloat16),
            jax.ShapeDtypeStruct((8, LANES), jnp.float32),
            jax.ShapeDtypeStruct((64, LANES), jnp.float32),
        ),
        in_specs=[hbm] * 6,
        out_specs=(vmem,) * 6,
        scratch_shapes=[
            pltpu.SMEM((3,), jnp.int32),
            pltpu.SMEM((3, 6), jnp.int32),
            pltpu.SMEM((1, 6), jnp.int32),
            pltpu.VMEM((20, 64), jnp.int32),
            pltpu.VMEM((3, 2, 16, 1024), jnp.float32),
            pltpu.VMEM((4, 512, 8, 32), jnp.float32),
            pltpu.VMEM((64, 512), jnp.bfloat16),
            pltpu.VMEM((8, 512, LANES), jnp.bfloat16),
            pltpu.VMEM((8, 512, LANES), jnp.bfloat16),
            pltpu.SemaphoreType.DMA((9,)),
        ],
        compiler_params=pltpu.CompilerParams(vmem_limit_bytes=24 << 20),
        name="pack",
    )(*(in_hbm(x) for x in (layer_order, cut_index.T, slice_bits, strings, gate_stack, boundary.reshape(512, 32, 32))))
    pieces = pieces.reshape(64, 1, PIECE * LANES)
    got = lax.all_to_all(pieces, CUTS, 0, 0, tiled=True).reshape(64 * PIECE, LANES)
    third, mine = pl.pallas_call(
        select_kernel,
        out_shape=(
            jax.ShapeDtypeStruct((16, 16, LANES), jnp.float32),
            jax.ShapeDtypeStruct((512, LANES), jnp.float32),
        ),
        in_specs=[vmem, vmem],
        out_specs=(vmem, vmem),
        compiler_params=pltpu.CompilerParams(vmem_limit_bytes=8 << 20),
        name="select",
    )(chosen, got)
    theirs = lax.ppermute(mine, CORES, [(0, 1), (1, 0)])
    third = lax.all_to_all(third, WAVE, 0, 0, tiled=True)
    same, other = pl.pallas_call(
        inner_kernel,
        out_shape=(jax.ShapeDtypeStruct((16, 16, LANES), jnp.float32),) * 2,
        in_specs=[smem] + [vmem] * 6,
        out_specs=(vmem, vmem),
        scratch_shapes=[
            pltpu.VMEM((256, 64), jnp.bfloat16),
            pltpu.VMEM((64, LANES), jnp.bfloat16),
            pltpu.VMEM((64, 64), jnp.float32),
            pltpu.VMEM((4, 512, LANES), jnp.float32),
            pltpu.VMEM((4, 64, LANES), jnp.float32),
            pltpu.VMEM((2 * HALF, LANES), jnp.float32),
            pltpu.VMEM((2 * HALF, LANES), jnp.float32),
            pltpu.VMEM((256, LANES), jnp.float32),
            pltpu.VMEM((256, LANES), jnp.float32),
            pltpu.VMEM((256 * UNROLL, LANES), jnp.float32),
            pltpu.VMEM((256 * UNROLL, LANES), jnp.float32),
        ],
        compiler_params=pltpu.CompilerParams(vmem_limit_bytes=16 << 20),
        cost_estimate=pl.CostEstimate(flops=1 << 30, bytes_accessed=1 << 20, transcendentals=0),
        name="inner",
    )(rows, *tables, got, mine, theirs)
    partial_sums = pl.pallas_call(
        outer_kernel,
        out_shape=jax.ShapeDtypeStruct((16, 2, LANES), jnp.float32),
        in_specs=[vmem, vmem, vmem],
        out_specs=vmem,
        compiler_params=pltpu.CompilerParams(vmem_limit_bytes=8 << 20),
        name="outer",
    )(third, same, other)
    total = all_reduced(partial_sums, COLUMN, 16)
    total = all_reduced(total, PLANE, 1)
    return total[0, :, :64].T


def solution(mesh):
    finer = Mesh(
        mesh.devices.reshape(AXES + (mesh.shape["grp"],)),
        CUTS + ("grp",),
    )
    return jax.shard_map(
        on_device,
        mesh=finer,
        in_specs=(
            P("grp", None, None, None, None),
            P(None, None, CUTS, None),
            P(),
            P(),
            P(CUTS, None),
            P(),
        ),
        out_specs=P(),
        check_vma=False,
    )
```

```python
from functools import partial

import jax
import jax.numpy as jnp
from jax import lax
from jax.experimental import pallas as pl
from jax.experimental.pallas import tpu as pltpu
from jax.sharding import Mesh
from jax.sharding import PartitionSpec as P

AXES = (2, 2, 4, 2, 2)
CUTS = ("cuts_0", "cuts_1", "cuts_2", "cuts_3", "cuts_4")
WAVE = ("cuts_1", "cuts_2", "cuts_3")
CORES = "cuts_4"
PLANE = ("cuts_0", "cuts_1", "cuts_2")
COLUMN = ("cuts_3", "cuts_4", "grp")

BLOCKS_I, BLOCKS_J = 4, 16
LANES = 128
UNROLL = 8
ROW_SECOND, ROW_FIRST, ROW_THIRD, ROW_BITS, PIECE = 0, 8, 12, 16, 17
SPACED, HALF = 9, 64 * 9


def split_high_rest(array):
    high = array.astype(jnp.bfloat16)
    return high, array - high.astype(jnp.float32)


def split_high_low(array):
    high, rest = split_high_rest(array)
    return high, rest.astype(jnp.bfloat16)


def dot(left, right):
    return jnp.dot(left, right, preferred_element_type=jnp.float32)


def lane_of(shape):
    return lax.broadcasted_iota(jnp.int32, shape, 1)


def side_by_side(real, imag):
    low = lane_of(real.shape) < 64
    return jnp.where(low, real, pltpu.roll(imag, 64, 1)), jnp.where(low, pltpu.roll(real, 64, 1), imag)


def regrouped(parts, group):
    lane = lane_of(parts[0].shape)
    result = None
    for place, part in enumerate(parts):
        shift = 16 * (place - group) % LANES
        moved = pltpu.roll(part, shift, 1) if shift else part
        result = moved if place == 0 else jnp.where(lane >= 16 * place, moved, result)
    return result


def place_in_blocks():
    block_j = 0
    for axis, size in zip(WAVE, AXES[1:4], strict=True):
        block_j = block_j * size + lax.axis_index(axis)
    return 2 * lax.axis_index(CUTS[0]) + lax.axis_index(CORES), block_j


def sign_tables(cut_ref, string_ref, third_row, third_move, pair_ref, j_ref, fixed_ref, chosen_ref):
    block_i, block_j = place_in_blocks()
    lane, sublane = lane_of((1, LANES)), lax.broadcasted_iota(jnp.int32, (8, 1), 0)
    zero_row, zero_column = jnp.zeros((1, LANES), jnp.int32), jnp.zeros((8, 1), jnp.int32)
    pair_on, pair_bit, pair_i1 = zero_row, zero_row, zero_row
    j_on, j_bit, j_j2 = zero_column, zero_column, zero_column
    pair_count, j_count, fixed_count = 0, 0, 0
    strings = jnp.zeros((8, 64), jnp.int32)
    for cut in range(6):
        layer, group, bit = cut_ref[0, cut], cut_ref[1, cut], cut_ref[2, cut]
        on_i1 = jnp.where((group == 1) & (layer < 2), 1, 0)
        on_i2 = jnp.where((group == 2) & (layer == 1), 1, 0)
        on_j2 = jnp.where((group == 2) & (layer == 0), 1, 0)
        on_j3 = jnp.where((group == 3) & (layer == 0), 1, 0)
        on_fixed = 1 - on_i1 - on_i2 - on_j2 - on_j3
        pair_on = jnp.where(lane == cut, on_i1 + on_i2, pair_on)
        pair_bit = jnp.where(lane == cut, bit, pair_bit)
        pair_i1 = jnp.where(lane == cut, on_i1, pair_i1)
        j_on = jnp.where(sublane == cut, on_j2 + on_j3, j_on)
        j_bit = jnp.where(sublane == cut, bit, j_bit)
        j_j2 = jnp.where(sublane == cut, on_j2, j_j2)
        pair_count, j_count, fixed_count = pair_count + on_i1 + on_i2, j_count + on_j2 + on_j3, fixed_count + on_fixed
        sign = on_fixed * (1 - 2 * string_ref[pl.ds(5 * group + bit, 1), :])
        strings = jnp.where(sublane == cut, sign, strings)

    row = lax.broadcasted_iota(jnp.int32, (256, 1), 0)
    i1 = 16 * (row >> 7) + 4 * block_i + ((row >> 5) & 3)
    index = jnp.where(pair_i1 != 0, i1, row & 31)
    signs = jnp.where(lane == 6, -pair_count, pair_on * (1 - 2 * ((index >> pair_bit) & 1)))
    pair_ref[...] = signs.astype(jnp.float32).astype(jnp.bfloat16)
    j = lane & 63
    index = jnp.where(j_j2 != 0, 2 * block_j + (j >> 5), j & 31)
    signs = jnp.where(sublane == 6, -j_count, j_on * (1 - 2 * ((index >> j_bit) & 1)))
    j_ref[...] = signs.astype(jnp.float32)
    strings = jnp.where(sublane == 6, -fixed_count, strings)
    strings = jnp.concatenate((strings, third_row, third_move), axis=0).astype(jnp.float32)
    strings = jnp.concatenate((strings, jnp.zeros((118, 64), jnp.float32)), axis=0)
    columns = jnp.concatenate((strings, jnp.zeros_like(strings)), axis=1).T[:64]
    fixed_ref[...] = columns
    hit = lane_of((64, 256)).astype(jnp.float32) == columns[:, 8:9]
    for move in range(4):
        one = jnp.where(hit & (columns[:, 9:10] == move), 1.0, 0.0)
        chosen_ref[64 * move : 64 * move + 64, :] = one.astype(jnp.bfloat16)


def pack_kernel(order_hbm, cut_hbm, bits_hbm, string_hbm, gate_hbm, boundary_hbm, piece_ref, row_ref, chosen_ref, pair_ref, j_ref, fixed_ref, order_ref, cut_ref, bits_ref, string_ref, gate_ref, boundary_ref, left_ref, high_ref, low_ref, sems):
    small = [
        pltpu.make_async_copy(order_hbm, order_ref, sems.at[0]),
        pltpu.make_async_copy(bits_hbm, bits_ref, sems.at[1]),
        pltpu.make_async_copy(string_hbm, string_ref, sems.at[2]),
        pltpu.make_async_copy(gate_hbm, gate_ref, sems.at[3]),
        pltpu.make_async_copy(cut_hbm, cut_ref, sems.at[4]),
    ]
    large = [
        pltpu.make_async_copy(boundary_hbm.at[:, pl.ds(4 * step, 4), :], boundary_ref.at[step], sems.at[5 + step])
        for step in range(8)
    ]
    for copy in small + large:
        copy.start()
    for copy in small:
        copy.wait()

    first, second, third = order_ref[0], order_ref[1], order_ref[2]
    member = lax.axis_index("grp")
    columns = pl.ds(pl.multiple_of(member * 256, 256), 256)
    real, imag = gate_ref[first, 0, :, columns], gate_ref[first, 1, :, columns]

    def interleaved(even, odd):
        parts = []
        for k0 in range(8):
            parts += [even[:, 32 * k0 : 32 * k0 + 32], odd[:, 32 * k0 : 32 * k0 + 32]]
        return jnp.concatenate(parts, axis=1)

    left = jnp.concatenate((interleaved(real, -imag), interleaved(imag, real)), axis=0)
    high, low = split_high_low(left)
    left_ref[...] = jnp.concatenate((high, low), axis=0)

    strings = string_ref[...]

    def digit(group):
        total = strings[5 * group : 5 * group + 1]
        for bit in range(1, 5):
            total = total + (strings[5 * group + bit : 5 * group + bit + 1] << bit)
        return total

    g0, g1, g2, g3 = (digit(group) for group in range(4))
    row_ref[0:1, :] = 8 * g0
    row_ref[1:2, :] = ((g3 & 15) >> 3) * HALF + (g3 >> 4) * SPACED + (g3 & 7)
    third_row = (g2 & 3) * 64 + 2 * g1 + (g2 >> 4)
    third_move = ((lane_of((1, 64)) >> 4) - ((g2 & 15) >> 2)) & 3

    lane = lane_of((1, LANES))
    bits = jnp.zeros((1, LANES), jnp.float32)
    for cut in range(6):
        bits = jnp.where(lane == cut, bits_ref[0, cut].astype(jnp.float32), bits)

    def put(block_i, block_j, at, value):
        start = ((block_i // 2 * BLOCKS_J + block_j) * 2 + block_i % 2) * PIECE + at
        piece_ref[start : start + value.shape[0], :] = value

    for tile in range(8):
        lanes = slice(LANES * tile, LANES * tile + LANES)
        values = side_by_side(gate_ref[second, 0, :, lanes], gate_ref[second, 1, :, lanes])
        for half in range(2):
            for block_i in range(BLOCKS_I):
                eight = 8 * (block_i % 2)
                put(block_i, 2 * tile + half, ROW_SECOND, values[half][eight : eight + 8])
    for block_i in range(BLOCKS_I):
        parts = []
        for four in range(4):
            for part in range(2):
                rows = slice(4 * four, 4 * four + 4)
                parts.append(
                    jnp.concatenate(
                        [
                            gate_ref[third, part, rows, 512 * h + LANES * block_i : 512 * h + LANES * block_i + LANES]
                            for h in range(2)
                        ],
                        axis=0,
                    )
                )
        for group in range(8):
            value = regrouped(parts, group)
            put(block_i, group, ROW_THIRD, value[:4])
            put(block_i, 8 + group, ROW_THIRD, value[4:])
    for block_i in range(BLOCKS_I):
        for block_j in range(BLOCKS_J):
            put(block_i, block_j, ROW_BITS, bits)

    sign_tables(cut_ref, string_ref, third_row, third_move, pair_ref, j_ref, fixed_ref, chosen_ref)

    def split(step):
        large[step].wait()
        flat = boundary_ref.at[step].reshape(2048, 32)
        for half in range(2):
            right = jnp.concatenate([flat[pl.ds(2 * half + one, 512, stride=4), :] for one in range(2)], axis=1)
            high_ref[2 * step + half], low_ref[2 * step + half] = split_high_low(right)

    def multiplied(step):
        values = []
        for half in range(2 * step, 2 * step + 2):
            by_high = dot(left_ref[...], high_ref[half])
            values.append(by_high[:32] + by_high[32:] + dot(left_ref[:32], low_ref[half]))
        for half in range(2):
            value = jnp.concatenate((values[half][:16], values[half][16:]), axis=1)
            for block_i in range(BLOCKS_I):
                put(block_i, 2 * step + half, ROW_FIRST, value[4 * block_i : 4 * block_i + 4])

    split(0)
    for step in range(1, 8):
        split(step)
        multiplied(step - 1)
    multiplied(7)


def select_kernel(chosen_ref, got_ref, out_ref, half_ref):
    rows = [got_ref[pl.ds(ROW_THIRD + row, 64, stride=PIECE), :] for row in range(4)]
    high, rest = split_high_rest(jnp.concatenate(rows, axis=0))
    middle, rest = split_high_rest(rest)
    chosen = chosen_ref[...]
    found = dot(chosen, high) + (dot(chosen, middle) + dot(chosen, rest.astype(jnp.bfloat16)))
    total = found[:64]
    for move in range(1, 4):
        total = total + pltpu.roll(found[64 * move : 64 * move + 64], 32 * move, 1)
    lane, value = lane_of((16, LANES)), total[:16]
    for four in range(1, 4):
        value = jnp.where(lane >= 32 * four, total[16 * four : 16 * four + 16], value)
    for to in range(16):
        out_ref[to] = value
    for source in range(64):
        half_ref[8 * source : 8 * source + 8, :] = got_ref[PIECE * source : PIECE * source + 8, :]


def inner_kernel(row_ref, pair_ref, j_ref, string_ref, got_ref, mine_ref, theirs_ref, same_ref, other_ref, pairs_ref, allowed_ref, fixed_ref, sum_ref, whole_ref, second_ref, turned_ref, by_same_ref, by_other_ref, even_ref, odd_ref):
    lane = lane_of((1, LANES))
    signs = 1.0 - 2.0 * got_ref[pl.ds(ROW_BITS, 64, stride=PIECE), :]
    signs = jnp.where(lane < 6, signs, jnp.where(lane == 6, 1.0, 0.0)).astype(jnp.bfloat16)

    def one_if_all(differing, kind):
        return jnp.where(differing == 0.0, 1.0, 0.0).astype(kind)

    def against_slices(table):
        return lax.dot_general(table, signs, (((1,), (1,)), ((), ())), preferred_element_type=jnp.float32)

    fixed_ref[...] = one_if_all(against_slices(string_ref[...].astype(jnp.bfloat16)), jnp.float32)
    pairs_ref[...] = one_if_all(against_slices(pair_ref[...]), jnp.bfloat16)
    allowed_ref[...] = one_if_all(dot(signs[:, :8], j_ref[...].astype(jnp.bfloat16)), jnp.bfloat16)

    core = lax.axis_index(CORES)
    for ref, half in ((mine_ref, core), (theirs_ref, 1 - core)):
        for source in range(64):
            rows = ref[8 * source : 8 * source + 8, :]
            at = pl.ds(half * HALF + SPACED * source, 8)
            second_ref[at, :] = rows
            turned_ref[at, :] = pltpu.roll(rows, 64, 1)
    low = lane_of((8, LANES)) < 64
    for g0 in range(32):
        start = 2 * g0 * PIECE + ROW_FIRST
        first = jnp.concatenate((got_ref[start : start + 4, :], got_ref[start + PIECE : start + PIECE + 4, :]), axis=0)
        turned = pltpu.roll(first, 64, 1)
        by_same_ref[8 * g0 : 8 * g0 + 8, :] = jnp.where(low, first, turned)
        by_other_ref[8 * g0 : 8 * g0 + 8, :] = jnp.where(low, -turned, first)

    def counted(count_ref, b, inside):
        row_b = fixed_ref[pl.ds(b, 1), :].astype(jnp.bfloat16)
        count_ref[256 * inside : 256 * inside + 256, :] = dot(pairs_ref[...] * row_b, allowed_ref[...])

    def summed(count_ref, b, inside):
        start = row_ref[1, b]
        eight = pl.ds(pl.multiple_of(row_ref[0, b], 8), 8)
        by_same, by_other = by_same_ref[eight, :], by_other_ref[eight, :]
        second = second_ref[pl.ds(start, 32, stride=2 * SPACED), :]
        other = turned_ref[pl.ds(start, 32, stride=2 * SPACED), :]
        for h in range(2):
            terms = []
            for e in range(4):
                q = 4 * h + e
                term = by_same[q : q + 1] * second + by_other[q : q + 1] * other
                terms.append(term * count_ref[256 * inside + 32 * q : 256 * inside + 32 * q + 32, :])
            columns = jnp.concatenate(terms, axis=0).T
            for part in range(2):
                total = jnp.sum(columns[64 * part : 64 * part + 64].reshape(8, 8, LANES), axis=0)
                sum_ref[2 * part + h, pl.ds(pl.multiple_of(8 * b, 8), 8), :] = total

    def several(base, carry):
        b = 2 * UNROLL * base
        for inside in range(UNROLL):
            counted(odd_ref, b + UNROLL + inside, inside)
            summed(even_ref, b + inside, inside)
        for inside in range(UNROLL):
            counted(even_ref, (b + 2 * UNROLL + inside) % 64, inside)
            summed(odd_ref, b + UNROLL + inside, inside)
        return carry

    for inside in range(UNROLL):
        counted(even_ref, inside, inside)
    lax.fori_loop(0, 32 // UNROLL, several, 0)
    for part in range(2):
        for h in range(2):
            total = jnp.zeros((64, LANES), jnp.float32)
            for sublane in range(8):
                total += sum_ref[2 * part + h, pl.ds(sublane, 64, stride=8), :]
            whole_ref[2 * part + h] = total
    for h in range(2):
        parts = [whole_ref[2 * part + h, 16 * four : 16 * four + 16] for four in range(4) for part in range(2)]
        for group in range(8):
            value = regrouped(parts, group)
            imag = (lane_of(value.shape) & 16) != 0
            same_ref[8 * h + group] = jnp.where(imag, -value, value)
            other_ref[8 * h + group] = jnp.where(imag, pltpu.roll(value, 16, 1), pltpu.roll(value, LANES - 16, 1))


def outer_kernel(third_ref, same_ref, other_ref, out_ref):
    third = third_ref[...]
    real = jnp.sum(third * same_ref[...], axis=0)
    imag = jnp.sum(third * other_ref[...], axis=0)
    columns = jnp.concatenate((real, imag, jnp.zeros((96, LANES), jnp.float32)), axis=0).T
    sums = [jnp.sum(columns[32 * four : 32 * four + 32, :32], axis=0, keepdims=True) for four in range(4)]
    unused = [jnp.zeros((1, 64), jnp.float32)]
    real = jnp.concatenate([x[:, :16] for x in sums] + unused, axis=1)
    imag = jnp.concatenate([x[:, 16:] for x in sums] + unused, axis=1)
    for to in range(16):
        out_ref[to, 0:1, :] = real
        out_ref[to, 1:2, :] = imag


def all_reduced(copies, axes, rows):
    got = lax.all_to_all(copies, axes, 0, 0, tiled=True)
    total = jnp.sum(got, axis=0, keepdims=True)
    return jnp.broadcast_to(total, (rows,) + total.shape[1:])


def on_device(boundary, gate_stack, layer_order, cut_index, slice_bits, bitstrings):
    smem = pl.BlockSpec(memory_space=pltpu.SMEM)
    vmem = pl.BlockSpec(memory_space=pltpu.VMEM)
    hbm = pl.BlockSpec(memory_space=pltpu.HBM)
    in_hbm = partial(pltpu.with_memory_space_constraint, memory_space=pltpu.HBM)
    strings = bitstrings.T
    pieces, rows, chosen, *tables = pl.pallas_call(
        pack_kernel,
        out_shape=(
            jax.ShapeDtypeStruct((64 * PIECE, LANES), jnp.float32),
            jax.ShapeDtypeStruct((8, 64), jnp.int32),
            jax.ShapeDtypeStruct((256, 256), jnp.bfloat16),
            jax.ShapeDtypeStruct((256, LANES), jnp.bfloat16),
            jax.ShapeDtypeStruct((8, LANES), jnp.float32),
            jax.ShapeDtypeStruct((64, LANES), jnp.float32),
        ),
        in_specs=[hbm] * 6,
        out_specs=(vmem,) * 6,
        scratch_shapes=[
            pltpu.SMEM((3,), jnp.int32),
            pltpu.SMEM((3, 6), jnp.int32),
            pltpu.SMEM((1, 6), jnp.int32),
            pltpu.VMEM((20, 64), jnp.int32),
            pltpu.VMEM((3, 2, 16, 1024), jnp.float32),
            pltpu.VMEM((8, 512, 4, 32), jnp.float32),
            pltpu.VMEM((64, 512), jnp.bfloat16),
            pltpu.VMEM((16, 512, 64), jnp.bfloat16),
            pltpu.VMEM((16, 512, 64), jnp.bfloat16),
            pltpu.SemaphoreType.DMA((13,)),
        ],
        compiler_params=pltpu.CompilerParams(vmem_limit_bytes=24 << 20),
        name="pack",
    )(*(in_hbm(x) for x in (layer_order, cut_index.T, slice_bits, strings, gate_stack, boundary.reshape(512, 32, 32))))
    pieces = pieces.reshape(64, 1, PIECE * LANES)
    got = lax.all_to_all(pieces, CUTS, 0, 0, tiled=True).reshape(64 * PIECE, LANES)
    third, mine = pl.pallas_call(
        select_kernel,
        out_shape=(
            jax.ShapeDtypeStruct((16, 16, LANES), jnp.float32),
            jax.ShapeDtypeStruct((512, LANES), jnp.float32),
        ),
        in_specs=[vmem, vmem],
        out_specs=(vmem, vmem),
        compiler_params=pltpu.CompilerParams(vmem_limit_bytes=8 << 20),
        name="select",
    )(chosen, got)
    theirs = lax.ppermute(mine, CORES, [(0, 1), (1, 0)])
    third = lax.all_to_all(third, WAVE, 0, 0, tiled=True)
    same, other = pl.pallas_call(
        inner_kernel,
        out_shape=(jax.ShapeDtypeStruct((16, 16, LANES), jnp.float32),) * 2,
        in_specs=[smem] + [vmem] * 6,
        out_specs=(vmem, vmem),
        scratch_shapes=[
            pltpu.VMEM((256, 64), jnp.bfloat16),
            pltpu.VMEM((64, LANES), jnp.bfloat16),
            pltpu.VMEM((64, 64), jnp.float32),
            pltpu.VMEM((4, 512, LANES), jnp.float32),
            pltpu.VMEM((4, 64, LANES), jnp.float32),
            pltpu.VMEM((2 * HALF, LANES), jnp.float32),
            pltpu.VMEM((2 * HALF, LANES), jnp.float32),
            pltpu.VMEM((256, LANES), jnp.float32),
            pltpu.VMEM((256, LANES), jnp.float32),
            pltpu.VMEM((256 * UNROLL, LANES), jnp.float32),
            pltpu.VMEM((256 * UNROLL, LANES), jnp.float32),
        ],
        compiler_params=pltpu.CompilerParams(vmem_limit_bytes=16 << 20),
        cost_estimate=pl.CostEstimate(flops=1 << 30, bytes_accessed=1 << 20, transcendentals=0),
        name="inner",
    )(rows, *tables, got, mine, theirs)
    partial_sums = pl.pallas_call(
        outer_kernel,
        out_shape=jax.ShapeDtypeStruct((16, 2, LANES), jnp.float32),
        in_specs=[vmem, vmem, vmem],
        out_specs=vmem,
        compiler_params=pltpu.CompilerParams(vmem_limit_bytes=8 << 20),
        name="outer",
    )(third, same, other)
    total = all_reduced(partial_sums, COLUMN, 16)
    total = all_reduced(total, PLANE, 1)
    return total[0, :, :64].T


def solution(mesh):
    finer = Mesh(
        mesh.devices.reshape(AXES + (mesh.shape["grp"],)),
        CUTS + ("grp",),
    )
    return jax.shard_map(
        on_device,
        mesh=finer,
        in_specs=(
            P("grp", None, None, None, None),
            P(None, None, CUTS, None),
            P(),
            P(),
            P(CUTS, None),
            P(),
        ),
        out_specs=P(),
        check_vma=False,
    )
```

```python
from functools import partial

import jax
import jax.numpy as jnp
from jax import lax
from jax.experimental import pallas as pl
from jax.experimental.pallas import tpu as pltpu
from jax.sharding import Mesh
from jax.sharding import PartitionSpec as P

AXES = (2, 2, 4, 2, 2)
CUTS = ("cuts_0", "cuts_1", "cuts_2", "cuts_3", "cuts_4")
WAVE = ("cuts_1", "cuts_2", "cuts_3")
CORES = "cuts_4"
CHIPS = ("cuts_3", "grp", "cuts_0", "cuts_1", "cuts_2")

BLOCKS_I, BLOCKS_J = 4, 16
LANES = 128
UNROLL = 8
ROW_SECOND, ROW_FIRST, ROW_THIRD, ROW_BITS, PIECE = 0, 8, 12, 16, 17
SPACED, HALF = 9, 64 * 9


def split_high_rest(array):
    high = array.astype(jnp.bfloat16)
    return high, array - high.astype(jnp.float32)


def split_high_low(array):
    high, rest = split_high_rest(array)
    return high, rest.astype(jnp.bfloat16)


def dot(left, right):
    return jnp.dot(left, right, preferred_element_type=jnp.float32)


def lane_of(shape):
    return lax.broadcasted_iota(jnp.int32, shape, 1)


def side_by_side(real, imag):
    low = lane_of(real.shape) < 64
    return jnp.where(low, real, pltpu.roll(imag, 64, 1)), jnp.where(low, pltpu.roll(real, 64, 1), imag)


def regrouped(parts, group):
    lane = lane_of(parts[0].shape)
    result = None
    for place, part in enumerate(parts):
        shift = 16 * (place - group) % LANES
        moved = pltpu.roll(part, shift, 1) if shift else part
        result = moved if place == 0 else jnp.where(lane >= 16 * place, moved, result)
    return result


def place_in_blocks():
    block_j = 0
    for axis, size in zip(WAVE, AXES[1:4], strict=True):
        block_j = block_j * size + lax.axis_index(axis)
    return 2 * lax.axis_index(CUTS[0]) + lax.axis_index(CORES), block_j


def sign_tables(cut_ref, string_ref, third_row, third_move, pair_ref, j_ref, fixed_ref, chosen_ref):
    block_i, block_j = place_in_blocks()
    lane, sublane = lane_of((1, LANES)), lax.broadcasted_iota(jnp.int32, (8, 1), 0)
    zero_row, zero_column = jnp.zeros((1, LANES), jnp.int32), jnp.zeros((8, 1), jnp.int32)
    pair_on, pair_bit, pair_i1 = zero_row, zero_row, zero_row
    j_on, j_bit, j_j2 = zero_column, zero_column, zero_column
    pair_count, j_count, fixed_count = 0, 0, 0
    strings = jnp.zeros((8, 64), jnp.int32)
    for cut in range(6):
        layer, group, bit = cut_ref[0, cut], cut_ref[1, cut], cut_ref[2, cut]
        on_i1 = jnp.where((group == 1) & (layer < 2), 1, 0)
        on_i2 = jnp.where((group == 2) & (layer == 1), 1, 0)
        on_j2 = jnp.where((group == 2) & (layer == 0), 1, 0)
        on_j3 = jnp.where((group == 3) & (layer == 0), 1, 0)
        on_fixed = 1 - on_i1 - on_i2 - on_j2 - on_j3
        pair_on = jnp.where(lane == cut, on_i1 + on_i2, pair_on)
        pair_bit = jnp.where(lane == cut, bit, pair_bit)
        pair_i1 = jnp.where(lane == cut, on_i1, pair_i1)
        j_on = jnp.where(sublane == cut, on_j2 + on_j3, j_on)
        j_bit = jnp.where(sublane == cut, bit, j_bit)
        j_j2 = jnp.where(sublane == cut, on_j2, j_j2)
        pair_count, j_count, fixed_count = pair_count + on_i1 + on_i2, j_count + on_j2 + on_j3, fixed_count + on_fixed
        sign = on_fixed * (1 - 2 * string_ref[pl.ds(5 * group + bit, 1), :])
        strings = jnp.where(sublane == cut, sign, strings)

    row = lax.broadcasted_iota(jnp.int32, (256, 1), 0)
    i1 = 16 * (row >> 7) + 4 * block_i + ((row >> 5) & 3)
    index = jnp.where(pair_i1 != 0, i1, row & 31)
    signs = jnp.where(lane == 6, -pair_count, pair_on * (1 - 2 * ((index >> pair_bit) & 1)))
    pair_ref[...] = signs.astype(jnp.float32).astype(jnp.bfloat16)
    j = lane & 63
    index = jnp.where(j_j2 != 0, 2 * block_j + (j >> 5), j & 31)
    signs = jnp.where(sublane == 6, -j_count, j_on * (1 - 2 * ((index >> j_bit) & 1)))
    j_ref[...] = signs.astype(jnp.float32)
    strings = jnp.where(sublane == 6, -fixed_count, strings)
    strings = jnp.concatenate((strings, third_row, third_move), axis=0).astype(jnp.float32)
    strings = jnp.concatenate((strings, jnp.zeros((118, 64), jnp.float32)), axis=0)
    columns = jnp.concatenate((strings, jnp.zeros_like(strings)), axis=1).T[:64]
    fixed_ref[...] = columns
    hit = lane_of((64, 256)).astype(jnp.float32) == columns[:, 8:9]
    for move in range(4):
        one = jnp.where(hit & (columns[:, 9:10] == move), 1.0, 0.0)
        chosen_ref[64 * move : 64 * move + 64, :] = one.astype(jnp.bfloat16)


def pack_kernel(order_hbm, cut_hbm, bits_hbm, string_hbm, gate_hbm, boundary_hbm, piece_ref, row_ref, chosen_ref, pair_ref, j_ref, fixed_ref, order_ref, cut_ref, bits_ref, string_ref, gate_ref, boundary_ref, left_ref, high_ref, low_ref, sems):
    small = [
        pltpu.make_async_copy(order_hbm, order_ref, sems.at[0]),
        pltpu.make_async_copy(bits_hbm, bits_ref, sems.at[1]),
        pltpu.make_async_copy(string_hbm, string_ref, sems.at[2]),
        pltpu.make_async_copy(gate_hbm, gate_ref, sems.at[3]),
        pltpu.make_async_copy(cut_hbm, cut_ref, sems.at[4]),
    ]
    large = [
        pltpu.make_async_copy(boundary_hbm.at[:, pl.ds(4 * step, 4), :], boundary_ref.at[step], sems.at[5 + step])
        for step in range(8)
    ]
    for copy in small + large:
        copy.start()
    for copy in small:
        copy.wait()

    first, second, third = order_ref[0], order_ref[1], order_ref[2]
    member = lax.axis_index("grp")
    columns = pl.ds(pl.multiple_of(member * 256, 256), 256)
    real, imag = gate_ref[first, 0, :, columns], gate_ref[first, 1, :, columns]

    def interleaved(even, odd):
        parts = []
        for k0 in range(8):
            parts += [even[:, 32 * k0 : 32 * k0 + 32], odd[:, 32 * k0 : 32 * k0 + 32]]
        return jnp.concatenate(parts, axis=1)

    left = jnp.concatenate((interleaved(real, -imag), interleaved(imag, real)), axis=0)
    high, low = split_high_low(left)
    left_ref[...] = jnp.concatenate((high, low), axis=0)

    strings = string_ref[...]

    def digit(group):
        total = strings[5 * group : 5 * group + 1]
        for bit in range(1, 5):
            total = total + (strings[5 * group + bit : 5 * group + bit + 1] << bit)
        return total

    g0, g1, g2, g3 = (digit(group) for group in range(4))
    row_ref[0:1, :] = 8 * g0
    row_ref[1:2, :] = ((g3 & 15) >> 3) * HALF + (g3 >> 4) * SPACED + (g3 & 7)
    third_row = (g2 & 3) * 64 + 2 * g1 + (g2 >> 4)
    third_move = ((lane_of((1, 64)) >> 4) - ((g2 & 15) >> 2)) & 3

    lane = lane_of((1, LANES))
    bits = jnp.zeros((1, LANES), jnp.float32)
    for cut in range(6):
        bits = jnp.where(lane == cut, bits_ref[0, cut].astype(jnp.float32), bits)

    def put(block_i, block_j, at, value):
        start = ((block_i // 2 * BLOCKS_J + block_j) * 2 + block_i % 2) * PIECE + at
        piece_ref[start : start + value.shape[0], :] = value

    for tile in range(8):
        lanes = slice(LANES * tile, LANES * tile + LANES)
        values = side_by_side(gate_ref[second, 0, :, lanes], gate_ref[second, 1, :, lanes])
        for half in range(2):
            for block_i in range(BLOCKS_I):
                eight = 8 * (block_i % 2)
                put(block_i, 2 * tile + half, ROW_SECOND, values[half][eight : eight + 8])
    for block_i in range(BLOCKS_I):
        parts = []
        for four in range(4):
            for part in range(2):
                rows = slice(4 * four, 4 * four + 4)
                parts.append(
                    jnp.concatenate(
                        [
                            gate_ref[third, part, rows, 512 * h + LANES * block_i : 512 * h + LANES * block_i + LANES]
                            for h in range(2)
                        ],
                        axis=0,
                    )
                )
        for group in range(8):
            value = regrouped(parts, group)
            put(block_i, group, ROW_THIRD, value[:4])
            put(block_i, 8 + group, ROW_THIRD, value[4:])
    for block_i in range(BLOCKS_I):
        for block_j in range(BLOCKS_J):
            put(block_i, block_j, ROW_BITS, bits)

    sign_tables(cut_ref, string_ref, third_row, third_move, pair_ref, j_ref, fixed_ref, chosen_ref)

    def split(step):
        large[step].wait()
        flat = boundary_ref.at[step].reshape(2048, 32)
        for half in range(2):
            right = jnp.concatenate([flat[pl.ds(2 * half + one, 512, stride=4), :] for one in range(2)], axis=1)
            high_ref[2 * step + half], low_ref[2 * step + half] = split_high_low(right)

    def multiplied(step):
        values = []
        for half in range(2 * step, 2 * step + 2):
            by_high = dot(left_ref[...], high_ref[half])
            values.append(by_high[:32] + by_high[32:] + dot(left_ref[:32], low_ref[half]))
        for half in range(2):
            value = jnp.concatenate((values[half][:16], values[half][16:]), axis=1)
            for block_i in range(BLOCKS_I):
                put(block_i, 2 * step + half, ROW_FIRST, value[4 * block_i : 4 * block_i + 4])

    split(0)
    for step in range(1, 8):
        split(step)
        multiplied(step - 1)
    multiplied(7)


def select_kernel(chosen_ref, got_ref, out_ref, half_ref):
    rows = [got_ref[pl.ds(ROW_THIRD + row, 64, stride=PIECE), :] for row in range(4)]
    high, rest = split_high_rest(jnp.concatenate(rows, axis=0))
    middle, rest = split_high_rest(rest)
    chosen = chosen_ref[...]
    found = dot(chosen, high) + (dot(chosen, middle) + dot(chosen, rest.astype(jnp.bfloat16)))
    total = found[:64]
    for move in range(1, 4):
        total = total + pltpu.roll(found[64 * move : 64 * move + 64], 32 * move, 1)
    lane, value = lane_of((16, LANES)), total[:16]
    for four in range(1, 4):
        value = jnp.where(lane >= 32 * four, total[16 * four : 16 * four + 16], value)
    for to in range(16):
        out_ref[to] = value
    for source in range(64):
        half_ref[8 * source : 8 * source + 8, :] = got_ref[PIECE * source : PIECE * source + 8, :]


def inner_kernel(row_vmem, pair_ref, j_ref, string_ref, got_ref, mine_ref, theirs_ref, same_ref, other_ref, pairs_ref, allowed_ref, fixed_ref, sum_ref, whole_ref, second_ref, turned_ref, by_same_ref, by_other_ref, even_ref, odd_ref, row_ref, row_sem):
    to_smem = pltpu.make_async_copy(row_vmem, row_ref, row_sem)
    to_smem.start()
    lane = lane_of((1, LANES))
    signs = 1.0 - 2.0 * got_ref[pl.ds(ROW_BITS, 64, stride=PIECE), :]
    signs = jnp.where(lane < 6, signs, jnp.where(lane == 6, 1.0, 0.0)).astype(jnp.bfloat16)

    def one_if_all(differing, kind):
        return jnp.where(differing == 0.0, 1.0, 0.0).astype(kind)

    def against_slices(table):
        return lax.dot_general(table, signs, (((1,), (1,)), ((), ())), preferred_element_type=jnp.float32)

    fixed_ref[...] = one_if_all(against_slices(string_ref[...].astype(jnp.bfloat16)), jnp.float32)
    pairs_ref[...] = one_if_all(against_slices(pair_ref[...]), jnp.bfloat16)
    allowed_ref[...] = one_if_all(dot(signs[:, :8], j_ref[...].astype(jnp.bfloat16)), jnp.bfloat16)

    core = lax.axis_index(CORES)
    for ref, half in ((mine_ref, core), (theirs_ref, 1 - core)):
        for source in range(64):
            rows = ref[8 * source : 8 * source + 8, :]
            at = pl.ds(half * HALF + SPACED * source, 8)
            second_ref[at, :] = rows
            turned_ref[at, :] = pltpu.roll(rows, 64, 1)
    low = lane_of((8, LANES)) < 64
    for g0 in range(32):
        start = 2 * g0 * PIECE + ROW_FIRST
        first = jnp.concatenate((got_ref[start : start + 4, :], got_ref[start + PIECE : start + PIECE + 4, :]), axis=0)
        turned = pltpu.roll(first, 64, 1)
        by_same_ref[8 * g0 : 8 * g0 + 8, :] = jnp.where(low, first, turned)
        by_other_ref[8 * g0 : 8 * g0 + 8, :] = jnp.where(low, -turned, first)

    def counted(count_ref, b, inside):
        row_b = fixed_ref[pl.ds(b, 1), :].astype(jnp.bfloat16)
        count_ref[256 * inside : 256 * inside + 256, :] = dot(pairs_ref[...] * row_b, allowed_ref[...])

    def summed(count_ref, b, inside):
        start = row_ref[1, b]
        eight = pl.ds(pl.multiple_of(row_ref[0, b], 8), 8)
        by_same, by_other = by_same_ref[eight, :], by_other_ref[eight, :]
        second = second_ref[pl.ds(start, 32, stride=2 * SPACED), :]
        other = turned_ref[pl.ds(start, 32, stride=2 * SPACED), :]
        for h in range(2):
            terms = []
            for e in range(4):
                q = 4 * h + e
                term = by_same[q : q + 1] * second + by_other[q : q + 1] * other
                terms.append(term * count_ref[256 * inside + 32 * q : 256 * inside + 32 * q + 32, :])
            columns = jnp.concatenate(terms, axis=0).T
            for part in range(2):
                total = jnp.sum(columns[64 * part : 64 * part + 64].reshape(8, 8, LANES), axis=0)
                sum_ref[2 * part + h, pl.ds(pl.multiple_of(8 * b, 8), 8), :] = total

    def several(base, carry):
        b = 2 * UNROLL * base
        for inside in range(UNROLL):
            counted(odd_ref, b + UNROLL + inside, inside)
            summed(even_ref, b + inside, inside)
        for inside in range(UNROLL):
            counted(even_ref, (b + 2 * UNROLL + inside) % 64, inside)
            summed(odd_ref, b + UNROLL + inside, inside)
        return carry

    for inside in range(UNROLL):
        counted(even_ref, inside, inside)
    to_smem.wait()
    lax.fori_loop(0, 32 // UNROLL, several, 0)
    for part in range(2):
        for h in range(2):
            total = jnp.zeros((64, LANES), jnp.float32)
            for sublane in range(8):
                total += sum_ref[2 * part + h, pl.ds(sublane, 64, stride=8), :]
            whole_ref[2 * part + h] = total
    for h in range(2):
        parts = [whole_ref[2 * part + h, 16 * four : 16 * four + 16] for four in range(4) for part in range(2)]
        for group in range(8):
            value = regrouped(parts, group)
            imag = (lane_of(value.shape) & 16) != 0
            same_ref[8 * h + group] = jnp.where(imag, -value, value)
            other_ref[8 * h + group] = jnp.where(imag, pltpu.roll(value, 16, 1), pltpu.roll(value, LANES - 16, 1))


def outer_kernel(third_ref, same_ref, other_ref, out_ref):
    third = third_ref[...]
    real = jnp.sum(third * same_ref[...], axis=0)
    imag = jnp.sum(third * other_ref[...], axis=0)
    columns = jnp.concatenate((real, imag, jnp.zeros((96, LANES), jnp.float32)), axis=0).T
    sums = [jnp.sum(columns[32 * four : 32 * four + 32, :32], axis=0, keepdims=True) for four in range(4)]
    out_ref[...] = jnp.concatenate([x[:, :16] for x in sums] + [x[:, 16:] for x in sums], axis=1)


def on_device(boundary, gate_stack, layer_order, cut_index, slice_bits, bitstrings):
    smem = pl.BlockSpec(memory_space=pltpu.SMEM)
    vmem = pl.BlockSpec(memory_space=pltpu.VMEM)
    hbm = pl.BlockSpec(memory_space=pltpu.HBM)
    in_hbm = partial(pltpu.with_memory_space_constraint, memory_space=pltpu.HBM)
    strings = bitstrings.T
    pieces, rows, chosen, *tables = pl.pallas_call(
        pack_kernel,
        out_shape=(
            jax.ShapeDtypeStruct((64 * PIECE, LANES), jnp.float32),
            jax.ShapeDtypeStruct((8, 64), jnp.int32),
            jax.ShapeDtypeStruct((256, 256), jnp.bfloat16),
            jax.ShapeDtypeStruct((256, LANES), jnp.bfloat16),
            jax.ShapeDtypeStruct((8, LANES), jnp.float32),
            jax.ShapeDtypeStruct((64, LANES), jnp.float32),
        ),
        in_specs=[hbm] * 6,
        out_specs=(vmem,) * 6,
        scratch_shapes=[
            pltpu.SMEM((3,), jnp.int32),
            pltpu.SMEM((3, 6), jnp.int32),
            pltpu.SMEM((1, 6), jnp.int32),
            pltpu.VMEM((20, 64), jnp.int32),
            pltpu.VMEM((3, 2, 16, 1024), jnp.float32),
            pltpu.VMEM((8, 512, 4, 32), jnp.float32),
            pltpu.VMEM((64, 512), jnp.bfloat16),
            pltpu.VMEM((16, 512, 64), jnp.bfloat16),
            pltpu.VMEM((16, 512, 64), jnp.bfloat16),
            pltpu.SemaphoreType.DMA((13,)),
        ],
        compiler_params=pltpu.CompilerParams(vmem_limit_bytes=24 << 20),
        name="pack",
    )(*(in_hbm(x) for x in (layer_order, cut_index.T, slice_bits, strings, gate_stack, boundary.reshape(512, 32, 32))))
    pieces = pieces.reshape(64, 1, PIECE * LANES)
    got = lax.all_to_all(pieces, CUTS, 0, 0, tiled=True).reshape(64 * PIECE, LANES)
    third, mine = pl.pallas_call(
        select_kernel,
        out_shape=(
            jax.ShapeDtypeStruct((16, 16, LANES), jnp.float32),
            jax.ShapeDtypeStruct((512, LANES), jnp.float32),
        ),
        in_specs=[vmem, vmem],
        out_specs=(vmem, vmem),
        compiler_params=pltpu.CompilerParams(vmem_limit_bytes=8 << 20),
        name="select",
    )(chosen, got)
    theirs = lax.ppermute(mine, CORES, [(0, 1), (1, 0)])
    third = lax.all_to_all(third, WAVE, 0, 0, tiled=True)
    same, other = pl.pallas_call(
        inner_kernel,
        out_shape=(jax.ShapeDtypeStruct((16, 16, LANES), jnp.float32),) * 2,
        in_specs=[vmem] * 7,
        out_specs=(vmem, vmem),
        scratch_shapes=[
            pltpu.VMEM((256, 64), jnp.bfloat16),
            pltpu.VMEM((64, LANES), jnp.bfloat16),
            pltpu.VMEM((64, 64), jnp.float32),
            pltpu.VMEM((4, 512, LANES), jnp.float32),
            pltpu.VMEM((4, 64, LANES), jnp.float32),
            pltpu.VMEM((2 * HALF, LANES), jnp.float32),
            pltpu.VMEM((2 * HALF, LANES), jnp.float32),
            pltpu.VMEM((256, LANES), jnp.float32),
            pltpu.VMEM((256, LANES), jnp.float32),
            pltpu.VMEM((256 * UNROLL, LANES), jnp.float32),
            pltpu.VMEM((256 * UNROLL, LANES), jnp.float32),
            pltpu.SMEM((8, 64), jnp.int32),
            pltpu.SemaphoreType.DMA,
        ],
        compiler_params=pltpu.CompilerParams(vmem_limit_bytes=16 << 20),
        cost_estimate=pl.CostEstimate(flops=1 << 30, bytes_accessed=1 << 20, transcendentals=0),
        name="inner",
    )(rows, *tables, got, mine, theirs)
    partial_sums = pl.pallas_call(
        outer_kernel,
        out_shape=jax.ShapeDtypeStruct((1, LANES), jnp.float32),
        in_specs=[vmem, vmem, vmem],
        out_specs=vmem,
        compiler_params=pltpu.CompilerParams(vmem_limit_bytes=8 << 20),
        name="outer",
    )(third, same, other)
    chip_sums = partial_sums + lax.ppermute(partial_sums, CORES, [(0, 1), (1, 0)])
    copies = jnp.broadcast_to(chip_sums[None], (lax.axis_size(CHIPS), 1, LANES))
    total = jnp.sum(lax.all_to_all(copies, CHIPS, 0, 0, tiled=True), axis=0)
    return total.reshape(2, 64).T


def solution(mesh):
    finer = Mesh(
        mesh.devices.reshape(AXES + (mesh.shape["grp"],)),
        CUTS + ("grp",),
    )
    return jax.shard_map(
        on_device,
        mesh=finer,
        in_specs=(
            P("grp", None, None, None, None),
            P(None, None, CUTS, None),
            P(),
            P(),
            P(CUTS, None),
            P(),
        ),
        out_specs=P(),
        check_vma=False,
    )
```

```python
from functools import partial

import jax
import jax.numpy as jnp
from jax import lax
from jax.experimental import pallas as pl
from jax.experimental.pallas import tpu as pltpu
from jax.sharding import Mesh
from jax.sharding import PartitionSpec as P

AXES = (2, 2, 2, 2, 2, 2, 2, 2)
CUTS = ("cuts_0", "cuts_1", "cuts_2", "cuts_3", "cuts_4", "cuts_5")
GRP = ("grp_0", "grp_1")
WAVE = ("cuts_1", "cuts_2", "cuts_3", "cuts_4")
CORES = "cuts_5"
CHIPS = ("cuts_4", "grp_0", "cuts_2", "cuts_0", "grp_1", "cuts_1", "cuts_3")

BLOCKS_I, BLOCKS_J = 4, 16
LANES = 128
UNROLL = 8
ROW_SECOND, ROW_FIRST, ROW_THIRD, ROW_BITS, PIECE = 0, 8, 12, 16, 17
SPACED, HALF = 9, 64 * 9


def split_high_rest(array):
    high = array.astype(jnp.bfloat16)
    return high, array - high.astype(jnp.float32)


def split_high_low(array):
    high, rest = split_high_rest(array)
    return high, rest.astype(jnp.bfloat16)


def dot(left, right):
    return jnp.dot(left, right, preferred_element_type=jnp.float32)


def lane_of(shape):
    return lax.broadcasted_iota(jnp.int32, shape, 1)


def side_by_side(real, imag):
    low = lane_of(real.shape) < 64
    return jnp.where(low, real, pltpu.roll(imag, 64, 1)), jnp.where(low, pltpu.roll(real, 64, 1), imag)


def regrouped(parts, group):
    lane = lane_of(parts[0].shape)
    result = None
    for place, part in enumerate(parts):
        shift = 16 * (place - group) % LANES
        moved = pltpu.roll(part, shift, 1) if shift else part
        result = moved if place == 0 else jnp.where(lane >= 16 * place, moved, result)
    return result


def place_in_blocks():
    block_j = 0
    for axis in WAVE:
        block_j = block_j * 2 + lax.axis_index(axis)
    return 2 * lax.axis_index(CUTS[0]) + lax.axis_index(CORES), block_j


def sign_tables(cut_ref, string_ref, third_row, third_move, pair_ref, j_ref, fixed_ref, chosen_ref):
    block_i, block_j = place_in_blocks()
    lane, sublane = lane_of((1, LANES)), lax.broadcasted_iota(jnp.int32, (8, 1), 0)
    zero_row, zero_column = jnp.zeros((1, LANES), jnp.int32), jnp.zeros((8, 1), jnp.int32)
    pair_on, pair_bit, pair_i1 = zero_row, zero_row, zero_row
    j_on, j_bit, j_j2 = zero_column, zero_column, zero_column
    pair_count, j_count, fixed_count = 0, 0, 0
    strings = jnp.zeros((8, 64), jnp.int32)
    for cut in range(6):
        layer, group, bit = cut_ref[0, cut], cut_ref[1, cut], cut_ref[2, cut]
        on_i1 = jnp.where((group == 1) & (layer < 2), 1, 0)
        on_i2 = jnp.where((group == 2) & (layer == 1), 1, 0)
        on_j2 = jnp.where((group == 2) & (layer == 0), 1, 0)
        on_j3 = jnp.where((group == 3) & (layer == 0), 1, 0)
        on_fixed = 1 - on_i1 - on_i2 - on_j2 - on_j3
        pair_on = jnp.where(lane == cut, on_i1 + on_i2, pair_on)
        pair_bit = jnp.where(lane == cut, bit, pair_bit)
        pair_i1 = jnp.where(lane == cut, on_i1, pair_i1)
        j_on = jnp.where(sublane == cut, on_j2 + on_j3, j_on)
        j_bit = jnp.where(sublane == cut, bit, j_bit)
        j_j2 = jnp.where(sublane == cut, on_j2, j_j2)
        pair_count, j_count, fixed_count = pair_count + on_i1 + on_i2, j_count + on_j2 + on_j3, fixed_count + on_fixed
        sign = on_fixed * (1 - 2 * string_ref[pl.ds(5 * group + bit, 1), :])
        strings = jnp.where(sublane == cut, sign, strings)

    row = lax.broadcasted_iota(jnp.int32, (256, 1), 0)
    i1 = 16 * (row >> 7) + 4 * block_i + ((row >> 5) & 3)
    index = jnp.where(pair_i1 != 0, i1, row & 31)
    signs = jnp.where(lane == 6, -pair_count, pair_on * (1 - 2 * ((index >> pair_bit) & 1)))
    pair_ref[...] = signs.astype(jnp.float32).astype(jnp.bfloat16)
    j = lane & 63
    index = jnp.where(j_j2 != 0, 2 * block_j + (j >> 5), j & 31)
    signs = jnp.where(sublane == 6, -j_count, j_on * (1 - 2 * ((index >> j_bit) & 1)))
    j_ref[...] = signs.astype(jnp.float32)
    strings = jnp.where(sublane == 6, -fixed_count, strings)
    strings = jnp.concatenate((strings, third_row, third_move), axis=0).astype(jnp.float32)
    strings = jnp.concatenate((strings, jnp.zeros((118, 64), jnp.float32)), axis=0)
    columns = jnp.concatenate((strings, jnp.zeros_like(strings)), axis=1).T[:64]
    fixed_ref[...] = columns
    hit = lane_of((64, 256)).astype(jnp.float32) == columns[:, 8:9]
    for move in range(4):
        one = jnp.where(hit & (columns[:, 9:10] == move), 1.0, 0.0)
        chosen_ref[64 * move : 64 * move + 64, :] = one.astype(jnp.bfloat16)


def pack_kernel(order_hbm, cut_hbm, bits_hbm, string_hbm, gate_hbm, boundary_hbm, piece_ref, row_ref, chosen_ref, pair_ref, j_ref, fixed_ref, order_ref, cut_ref, bits_ref, string_ref, gate_ref, boundary_ref, left_ref, high_ref, low_ref, sems):
    small = [
        pltpu.make_async_copy(order_hbm, order_ref, sems.at[0]),
        pltpu.make_async_copy(bits_hbm, bits_ref, sems.at[1]),
        pltpu.make_async_copy(string_hbm, string_ref, sems.at[2]),
        pltpu.make_async_copy(gate_hbm, gate_ref, sems.at[3]),
        pltpu.make_async_copy(cut_hbm, cut_ref, sems.at[4]),
    ]
    large = [
        pltpu.make_async_copy(boundary_hbm.at[:, pl.ds(4 * step, 4), :], boundary_ref.at[step], sems.at[5 + step])
        for step in range(8)
    ]
    for copy in small + large:
        copy.start()
    for copy in small:
        copy.wait()

    first, second, third = order_ref[0], order_ref[1], order_ref[2]
    member = lax.axis_index(GRP)
    columns = pl.ds(pl.multiple_of(member * 256, 256), 256)
    real, imag = gate_ref[first, 0, :, columns], gate_ref[first, 1, :, columns]

    def interleaved(even, odd):
        parts = []
        for k0 in range(8):
            parts += [even[:, 32 * k0 : 32 * k0 + 32], odd[:, 32 * k0 : 32 * k0 + 32]]
        return jnp.concatenate(parts, axis=1)

    left = jnp.concatenate((interleaved(real, -imag), interleaved(imag, real)), axis=0)
    high, low = split_high_low(left)
    left_ref[...] = jnp.concatenate((high, low), axis=0)

    strings = string_ref[...]

    def digit(group):
        total = strings[5 * group : 5 * group + 1]
        for bit in range(1, 5):
            total = total + (strings[5 * group + bit : 5 * group + bit + 1] << bit)
        return total

    g0, g1, g2, g3 = (digit(group) for group in range(4))
    row_ref[0:1, :] = 8 * g0
    row_ref[1:2, :] = ((g3 & 15) >> 3) * HALF + (g3 >> 4) * SPACED + (g3 & 7)
    third_row = (g2 & 3) * 64 + 2 * g1 + (g2 >> 4)
    third_move = ((lane_of((1, 64)) >> 4) - ((g2 & 15) >> 2)) & 3

    lane = lane_of((1, LANES))
    bits = jnp.zeros((1, LANES), jnp.float32)
    for cut in range(6):
        bits = jnp.where(lane == cut, bits_ref[0, cut].astype(jnp.float32), bits)

    def put(block_i, block_j, at, value):
        start = ((block_i // 2 * BLOCKS_J + block_j) * 2 + block_i % 2) * PIECE + at
        piece_ref[start : start + value.shape[0], :] = value

    for tile in range(8):
        lanes = slice(LANES * tile, LANES * tile + LANES)
        values = side_by_side(gate_ref[second, 0, :, lanes], gate_ref[second, 1, :, lanes])
        for half in range(2):
            for block_i in range(BLOCKS_I):
                eight = 8 * (block_i % 2)
                put(block_i, 2 * tile + half, ROW_SECOND, values[half][eight : eight + 8])
    for block_i in range(BLOCKS_I):
        parts = []
        for four in range(4):
            for part in range(2):
                rows = slice(4 * four, 4 * four + 4)
                parts.append(
                    jnp.concatenate(
                        [
                            gate_ref[third, part, rows, 512 * h + LANES * block_i : 512 * h + LANES * block_i + LANES]
                            for h in range(2)
                        ],
                        axis=0,
                    )
                )
        for group in range(8):
            value = regrouped(parts, group)
            put(block_i, group, ROW_THIRD, value[:4])
            put(block_i, 8 + group, ROW_THIRD, value[4:])
    for block_i in range(BLOCKS_I):
        for block_j in range(BLOCKS_J):
            put(block_i, block_j, ROW_BITS, bits)

    sign_tables(cut_ref, string_ref, third_row, third_move, pair_ref, j_ref, fixed_ref, chosen_ref)

    def split(step):
        large[step].wait()
        flat = boundary_ref.at[step].reshape(2048, 32)
        for half in range(2):
            right = jnp.concatenate([flat[pl.ds(2 * half + one, 512, stride=4), :] for one in range(2)], axis=1)
            high_ref[2 * step + half], low_ref[2 * step + half] = split_high_low(right)

    def multiplied(step):
        values = []
        for half in range(2 * step, 2 * step + 2):
            by_high = dot(left_ref[...], high_ref[half])
            values.append(by_high[:32] + by_high[32:] + dot(left_ref[:32], low_ref[half]))
        for half in range(2):
            value = jnp.concatenate((values[half][:16], values[half][16:]), axis=1)
            for block_i in range(BLOCKS_I):
                put(block_i, 2 * step + half, ROW_FIRST, value[4 * block_i : 4 * block_i + 4])

    split(0)
    for step in range(1, 8):
        split(step)
        multiplied(step - 1)
    multiplied(7)


def select_kernel(chosen_ref, got_ref, out_ref, half_ref):
    rows = [got_ref[pl.ds(ROW_THIRD + row, 64, stride=PIECE), :] for row in range(4)]
    high, rest = split_high_rest(jnp.concatenate(rows, axis=0))
    middle, rest = split_high_rest(rest)
    chosen = chosen_ref[...]
    found = dot(chosen, high) + (dot(chosen, middle) + dot(chosen, rest.astype(jnp.bfloat16)))
    total = found[:64]
    for move in range(1, 4):
        total = total + pltpu.roll(found[64 * move : 64 * move + 64], 32 * move, 1)
    lane, value = lane_of((16, LANES)), total[:16]
    for four in range(1, 4):
        value = jnp.where(lane >= 32 * four, total[16 * four : 16 * four + 16], value)
    for to in range(16):
        out_ref[to] = value
    for source in range(64):
        half_ref[8 * source : 8 * source + 8, :] = got_ref[PIECE * source : PIECE * source + 8, :]


def inner_kernel(row_vmem, pair_ref, j_ref, string_ref, got_ref, mine_ref, theirs_ref, same_ref, other_ref, pairs_ref, allowed_ref, fixed_ref, sum_ref, whole_ref, second_ref, turned_ref, by_same_ref, by_other_ref, even_ref, odd_ref, row_ref, row_sem):
    to_smem = pltpu.make_async_copy(row_vmem, row_ref, row_sem)
    to_smem.start()
    lane = lane_of((1, LANES))
    signs = 1.0 - 2.0 * got_ref[pl.ds(ROW_BITS, 64, stride=PIECE), :]
    signs = jnp.where(lane < 6, signs, jnp.where(lane == 6, 1.0, 0.0)).astype(jnp.bfloat16)

    def one_if_all(differing, kind):
        return jnp.where(differing == 0.0, 1.0, 0.0).astype(kind)

    def against_slices(table):
        return lax.dot_general(table, signs, (((1,), (1,)), ((), ())), preferred_element_type=jnp.float32)

    fixed_ref[...] = one_if_all(against_slices(string_ref[...].astype(jnp.bfloat16)), jnp.float32)
    pairs_ref[...] = one_if_all(against_slices(pair_ref[...]), jnp.bfloat16)
    allowed_ref[...] = one_if_all(dot(signs[:, :8], j_ref[...].astype(jnp.bfloat16)), jnp.bfloat16)

    core = lax.axis_index(CORES)
    for ref, half in ((mine_ref, core), (theirs_ref, 1 - core)):
        for source in range(64):
            rows = ref[8 * source : 8 * source + 8, :]
            at = pl.ds(half * HALF + SPACED * source, 8)
            second_ref[at, :] = rows
            turned_ref[at, :] = pltpu.roll(rows, 64, 1)
    low = lane_of((8, LANES)) < 64
    for g0 in range(32):
        start = 2 * g0 * PIECE + ROW_FIRST
        first = jnp.concatenate((got_ref[start : start + 4, :], got_ref[start + PIECE : start + PIECE + 4, :]), axis=0)
        turned = pltpu.roll(first, 64, 1)
        by_same_ref[8 * g0 : 8 * g0 + 8, :] = jnp.where(low, first, turned)
        by_other_ref[8 * g0 : 8 * g0 + 8, :] = jnp.where(low, -turned, first)

    def counted(count_ref, b, inside):
        row_b = fixed_ref[pl.ds(b, 1), :].astype(jnp.bfloat16)
        count_ref[256 * inside : 256 * inside + 256, :] = dot(pairs_ref[...] * row_b, allowed_ref[...])

    def summed(count_ref, b, inside):
        start = row_ref[1, b]
        eight = pl.ds(pl.multiple_of(row_ref[0, b], 8), 8)
        by_same, by_other = by_same_ref[eight, :], by_other_ref[eight, :]
        second = second_ref[pl.ds(start, 32, stride=2 * SPACED), :]
        other = turned_ref[pl.ds(start, 32, stride=2 * SPACED), :]
        for h in range(2):
            terms = []
            for e in range(4):
                q = 4 * h + e
                term = by_same[q : q + 1] * second + by_other[q : q + 1] * other
                terms.append(term * count_ref[256 * inside + 32 * q : 256 * inside + 32 * q + 32, :])
            columns = jnp.concatenate(terms, axis=0).T
            for part in range(2):
                total = jnp.sum(columns[64 * part : 64 * part + 64].reshape(8, 8, LANES), axis=0)
                sum_ref[2 * part + h, pl.ds(pl.multiple_of(8 * b, 8), 8), :] = total

    def several(base, carry):
        b = 2 * UNROLL * base
        for inside in range(UNROLL):
            counted(odd_ref, b + UNROLL + inside, inside)
            summed(even_ref, b + inside, inside)
        for inside in range(UNROLL):
            counted(even_ref, (b + 2 * UNROLL + inside) % 64, inside)
            summed(odd_ref, b + UNROLL + inside, inside)
        return carry

    for inside in range(UNROLL):
        counted(even_ref, inside, inside)
    to_smem.wait()
    lax.fori_loop(0, 32 // UNROLL, several, 0)
    for part in range(2):
        for h in range(2):
            total = jnp.zeros((64, LANES), jnp.float32)
            for sublane in range(8):
                total += sum_ref[2 * part + h, pl.ds(sublane, 64, stride=8), :]
            whole_ref[2 * part + h] = total
    for h in range(2):
        parts = [whole_ref[2 * part + h, 16 * four : 16 * four + 16] for four in range(4) for part in range(2)]
        for group in range(8):
            value = regrouped(parts, group)
            imag = (lane_of(value.shape) & 16) != 0
            same_ref[8 * h + group] = jnp.where(imag, -value, value)
            other_ref[8 * h + group] = jnp.where(imag, pltpu.roll(value, 16, 1), pltpu.roll(value, LANES - 16, 1))


def outer_kernel(third_ref, same_ref, other_ref, out_ref):
    third = third_ref[...]
    real = jnp.sum(third * same_ref[...], axis=0)
    imag = jnp.sum(third * other_ref[...], axis=0)
    columns = jnp.concatenate((real, imag, jnp.zeros((96, LANES), jnp.float32)), axis=0).T
    sums = [jnp.sum(columns[32 * four : 32 * four + 32, :32], axis=0, keepdims=True) for four in range(4)]
    out_ref[...] = jnp.concatenate([x[:, :16] for x in sums] + [x[:, 16:] for x in sums], axis=1)


def on_device(boundary, gate_stack, layer_order, cut_index, slice_bits, bitstrings):
    smem = pl.BlockSpec(memory_space=pltpu.SMEM)
    vmem = pl.BlockSpec(memory_space=pltpu.VMEM)
    hbm = pl.BlockSpec(memory_space=pltpu.HBM)
    in_hbm = partial(pltpu.with_memory_space_constraint, memory_space=pltpu.HBM)
    strings = bitstrings.T
    pieces, rows, chosen, *tables = pl.pallas_call(
        pack_kernel,
        out_shape=(
            jax.ShapeDtypeStruct((64 * PIECE, LANES), jnp.float32),
            jax.ShapeDtypeStruct((8, 64), jnp.int32),
            jax.ShapeDtypeStruct((256, 256), jnp.bfloat16),
            jax.ShapeDtypeStruct((256, LANES), jnp.bfloat16),
            jax.ShapeDtypeStruct((8, LANES), jnp.float32),
            jax.ShapeDtypeStruct((64, LANES), jnp.float32),
        ),
        in_specs=[hbm] * 6,
        out_specs=(vmem,) * 6,
        scratch_shapes=[
            pltpu.SMEM((3,), jnp.int32),
            pltpu.SMEM((3, 6), jnp.int32),
            pltpu.SMEM((1, 6), jnp.int32),
            pltpu.VMEM((20, 64), jnp.int32),
            pltpu.VMEM((3, 2, 16, 1024), jnp.float32),
            pltpu.VMEM((8, 512, 4, 32), jnp.float32),
            pltpu.VMEM((64, 512), jnp.bfloat16),
            pltpu.VMEM((16, 512, 64), jnp.bfloat16),
            pltpu.VMEM((16, 512, 64), jnp.bfloat16),
            pltpu.SemaphoreType.DMA((13,)),
        ],
        compiler_params=pltpu.CompilerParams(vmem_limit_bytes=24 << 20),
        name="pack",
    )(*(in_hbm(x) for x in (layer_order, cut_index.T, slice_bits, strings, gate_stack, boundary.reshape(512, 32, 32))))
    pieces = pieces.reshape(64, 1, PIECE * LANES)
    got = lax.all_to_all(pieces, CUTS, 0, 0, tiled=True).reshape(64 * PIECE, LANES)
    third, mine = pl.pallas_call(
        select_kernel,
        out_shape=(
            jax.ShapeDtypeStruct((16, 16, LANES), jnp.float32),
            jax.ShapeDtypeStruct((512, LANES), jnp.float32),
        ),
        in_specs=[vmem, vmem],
        out_specs=(vmem, vmem),
        compiler_params=pltpu.CompilerParams(vmem_limit_bytes=8 << 20),
        name="select",
    )(chosen, got)
    theirs = lax.ppermute(mine, CORES, [(0, 1), (1, 0)])
    third = lax.all_to_all(third, WAVE, 0, 0, tiled=True)
    same, other = pl.pallas_call(
        inner_kernel,
        out_shape=(jax.ShapeDtypeStruct((16, 16, LANES), jnp.float32),) * 2,
        in_specs=[vmem] * 7,
        out_specs=(vmem, vmem),
        scratch_shapes=[
            pltpu.VMEM((256, 64), jnp.bfloat16),
            pltpu.VMEM((64, LANES), jnp.bfloat16),
            pltpu.VMEM((64, 64), jnp.float32),
            pltpu.VMEM((4, 512, LANES), jnp.float32),
            pltpu.VMEM((4, 64, LANES), jnp.float32),
            pltpu.VMEM((2 * HALF, LANES), jnp.float32),
            pltpu.VMEM((2 * HALF, LANES), jnp.float32),
            pltpu.VMEM((256, LANES), jnp.float32),
            pltpu.VMEM((256, LANES), jnp.float32),
            pltpu.VMEM((256 * UNROLL, LANES), jnp.float32),
            pltpu.VMEM((256 * UNROLL, LANES), jnp.float32),
            pltpu.SMEM((8, 64), jnp.int32),
            pltpu.SemaphoreType.DMA,
        ],
        compiler_params=pltpu.CompilerParams(vmem_limit_bytes=16 << 20),
        cost_estimate=pl.CostEstimate(flops=1 << 30, bytes_accessed=1 << 20, transcendentals=0),
        name="inner",
    )(rows, *tables, got, mine, theirs)
    partial_sums = pl.pallas_call(
        outer_kernel,
        out_shape=jax.ShapeDtypeStruct((1, LANES), jnp.float32),
        in_specs=[vmem, vmem, vmem],
        out_specs=vmem,
        compiler_params=pltpu.CompilerParams(vmem_limit_bytes=8 << 20),
        name="outer",
    )(third, same, other)
    chip_sums = partial_sums + lax.ppermute(partial_sums, CORES, [(0, 1), (1, 0)])
    copies = jnp.broadcast_to(chip_sums[None], (lax.axis_size(CHIPS), 1, LANES))
    total = jnp.sum(lax.all_to_all(copies, CHIPS, 0, 0, tiled=True), axis=0)
    return total.reshape(2, 64).T


def solution(mesh):
    finer = Mesh(mesh.devices.reshape(AXES), CUTS + GRP)
    return jax.shard_map(
        on_device,
        mesh=finer,
        in_specs=(
            P(GRP, None, None, None, None),
            P(None, None, CUTS, None),
            P(),
            P(),
            P(CUTS, None),
            P(),
        ),
        out_specs=P(),
        check_vma=False,
    )
```

```python
from functools import partial

import jax
import jax.numpy as jnp
from jax import lax
from jax.experimental import pallas as pl
from jax.experimental.pallas import tpu as pltpu
from jax.sharding import Mesh
from jax.sharding import PartitionSpec as P

AXES = (2, 2, 2, 2, 2, 2, 2, 2)
CUTS = ("cuts_0", "cuts_1", "cuts_2", "cuts_3", "cuts_4", "cuts_5")
GRP = ("grp_0", "grp_1")
WAVE = ("cuts_1", "cuts_2", "cuts_3", "cuts_4")
CORES = "cuts_5"
CHIPS = ("cuts_4", "grp_0", "cuts_2", "cuts_0", "grp_1", "cuts_1", "cuts_3")

BLOCKS_I, BLOCKS_J = 4, 16
LANES = 128
UNROLL = 16
ROW_SECOND, ROW_FIRST, ROW_THIRD, ROW_BITS, PIECE = 0, 8, 12, 16, 17
SPACED, HALF = 9, 64 * 9


def split_high_rest(array):
    high = array.astype(jnp.bfloat16)
    return high, array - high.astype(jnp.float32)


def split_high_low(array):
    high, rest = split_high_rest(array)
    return high, rest.astype(jnp.bfloat16)


def dot(left, right):
    return jnp.dot(left, right, preferred_element_type=jnp.float32)


def lane_of(shape):
    return lax.broadcasted_iota(jnp.int32, shape, 1)


def side_by_side(real, imag):
    low = lane_of(real.shape) < 64
    return jnp.where(low, real, pltpu.roll(imag, 64, 1)), jnp.where(low, pltpu.roll(real, 64, 1), imag)


def regrouped(parts, group):
    lane = lane_of(parts[0].shape)
    result = None
    for place, part in enumerate(parts):
        shift = 16 * (place - group) % LANES
        moved = pltpu.roll(part, shift, 1) if shift else part
        result = moved if place == 0 else jnp.where(lane >= 16 * place, moved, result)
    return result


def place_in_blocks():
    block_j = 0
    for axis in WAVE:
        block_j = block_j * 2 + lax.axis_index(axis)
    return 2 * lax.axis_index(CUTS[0]) + lax.axis_index(CORES), block_j


def sign_tables(cut_ref, string_ref, third_row, third_move, pair_ref, j_ref, fixed_ref, chosen_ref):
    block_i, block_j = place_in_blocks()
    lane, sublane = lane_of((1, LANES)), lax.broadcasted_iota(jnp.int32, (8, 1), 0)
    zero_row, zero_column = jnp.zeros((1, LANES), jnp.int32), jnp.zeros((8, 1), jnp.int32)
    pair_on, pair_bit, pair_i1 = zero_row, zero_row, zero_row
    j_on, j_bit, j_j2 = zero_column, zero_column, zero_column
    pair_count, j_count, fixed_count = 0, 0, 0
    strings = jnp.zeros((8, 64), jnp.int32)
    for cut in range(6):
        layer, group, bit = cut_ref[0, cut], cut_ref[1, cut], cut_ref[2, cut]
        on_i1 = jnp.where((group == 1) & (layer < 2), 1, 0)
        on_i2 = jnp.where((group == 2) & (layer == 1), 1, 0)
        on_j2 = jnp.where((group == 2) & (layer == 0), 1, 0)
        on_j3 = jnp.where((group == 3) & (layer == 0), 1, 0)
        on_fixed = 1 - on_i1 - on_i2 - on_j2 - on_j3
        pair_on = jnp.where(lane == cut, on_i1 + on_i2, pair_on)
        pair_bit = jnp.where(lane == cut, bit, pair_bit)
        pair_i1 = jnp.where(lane == cut, on_i1, pair_i1)
        j_on = jnp.where(sublane == cut, on_j2 + on_j3, j_on)
        j_bit = jnp.where(sublane == cut, bit, j_bit)
        j_j2 = jnp.where(sublane == cut, on_j2, j_j2)
        pair_count, j_count, fixed_count = pair_count + on_i1 + on_i2, j_count + on_j2 + on_j3, fixed_count + on_fixed
        sign = on_fixed * (1 - 2 * string_ref[pl.ds(5 * group + bit, 1), :])
        strings = jnp.where(sublane == cut, sign, strings)

    row = lax.broadcasted_iota(jnp.int32, (256, 1), 0)
    i1 = 16 * (row >> 7) + 4 * block_i + ((row >> 5) & 3)
    index = jnp.where(pair_i1 != 0, i1, row & 31)
    signs = jnp.where(lane == 6, -pair_count, pair_on * (1 - 2 * ((index >> pair_bit) & 1)))
    pair_ref[...] = signs.astype(jnp.float32).astype(jnp.bfloat16)
    j = lane & 63
    index = jnp.where(j_j2 != 0, 2 * block_j + (j >> 5), j & 31)
    signs = jnp.where(sublane == 6, -j_count, j_on * (1 - 2 * ((index >> j_bit) & 1)))
    j_ref[...] = signs.astype(jnp.float32)
    strings = jnp.where(sublane == 6, -fixed_count, strings)
    strings = jnp.concatenate((strings, third_row, third_move), axis=0).astype(jnp.float32)
    strings = jnp.concatenate((strings, jnp.zeros((118, 64), jnp.float32)), axis=0)
    columns = jnp.concatenate((strings, jnp.zeros_like(strings)), axis=1).T[:64]
    fixed_ref[...] = columns
    hit = lane_of((64, 256)).astype(jnp.float32) == columns[:, 8:9]
    for move in range(4):
        one = jnp.where(hit & (columns[:, 9:10] == move), 1.0, 0.0)
        chosen_ref[64 * move : 64 * move + 64, :] = one.astype(jnp.bfloat16)


def pack_kernel(order_hbm, cut_hbm, bits_hbm, string_hbm, gate_hbm, boundary_hbm, piece_ref, row_ref, chosen_ref, pair_ref, j_ref, fixed_ref, order_ref, cut_ref, bits_ref, string_ref, gate_ref, boundary_ref, left_ref, high_ref, low_ref, sems):
    small = [
        pltpu.make_async_copy(order_hbm, order_ref, sems.at[0]),
        pltpu.make_async_copy(bits_hbm, bits_ref, sems.at[1]),
        pltpu.make_async_copy(string_hbm, string_ref, sems.at[2]),
        pltpu.make_async_copy(gate_hbm, gate_ref, sems.at[3]),
        pltpu.make_async_copy(cut_hbm, cut_ref, sems.at[4]),
    ]
    large = [
        pltpu.make_async_copy(boundary_hbm.at[:, pl.ds(4 * step, 4), :], boundary_ref.at[step], sems.at[5 + step])
        for step in range(8)
    ]
    for copy in small + large:
        copy.start()
    for copy in small:
        copy.wait()

    first, second, third = order_ref[0], order_ref[1], order_ref[2]
    member = lax.axis_index(GRP)
    columns = pl.ds(pl.multiple_of(member * 256, 256), 256)
    real, imag = gate_ref[first, 0, :, columns], gate_ref[first, 1, :, columns]

    def interleaved(even, odd):
        parts = []
        for k0 in range(8):
            parts += [even[:, 32 * k0 : 32 * k0 + 32], odd[:, 32 * k0 : 32 * k0 + 32]]
        return jnp.concatenate(parts, axis=1)

    left = jnp.concatenate((interleaved(real, -imag), interleaved(imag, real)), axis=0)
    high, low = split_high_low(left)
    left_ref[...] = jnp.concatenate((high, low), axis=0)

    strings = string_ref[...]

    def digit(group):
        total = strings[5 * group : 5 * group + 1]
        for bit in range(1, 5):
            total = total + (strings[5 * group + bit : 5 * group + bit + 1] << bit)
        return total

    g0, g1, g2, g3 = (digit(group) for group in range(4))
    row_ref[0:1, :] = 8 * g0
    row_ref[1:2, :] = ((g3 & 15) >> 3) * HALF + (g3 >> 4) * SPACED + (g3 & 7)
    third_row = (g2 & 3) * 64 + 2 * g1 + (g2 >> 4)
    third_move = ((lane_of((1, 64)) >> 4) - ((g2 & 15) >> 2)) & 3

    lane = lane_of((1, LANES))
    bits = jnp.zeros((1, LANES), jnp.float32)
    for cut in range(6):
        bits = jnp.where(lane == cut, bits_ref[0, cut].astype(jnp.float32), bits)

    def put(block_i, block_j, at, value):
        start = ((block_i // 2 * BLOCKS_J + block_j) * 2 + block_i % 2) * PIECE + at
        piece_ref[start : start + value.shape[0], :] = value

    for tile in range(8):
        lanes = slice(LANES * tile, LANES * tile + LANES)
        values = side_by_side(gate_ref[second, 0, :, lanes], gate_ref[second, 1, :, lanes])
        for half in range(2):
            for block_i in range(BLOCKS_I):
                eight = 8 * (block_i % 2)
                put(block_i, 2 * tile + half, ROW_SECOND, values[half][eight : eight + 8])
    for block_i in range(BLOCKS_I):
        parts = []
        for four in range(4):
            for part in range(2):
                rows = slice(4 * four, 4 * four + 4)
                parts.append(
                    jnp.concatenate(
                        [
                            gate_ref[third, part, rows, 512 * h + LANES * block_i : 512 * h + LANES * block_i + LANES]
                            for h in range(2)
                        ],
                        axis=0,
                    )
                )
        for group in range(8):
            value = regrouped(parts, group)
            put(block_i, group, ROW_THIRD, value[:4])
            put(block_i, 8 + group, ROW_THIRD, value[4:])
    for block_i in range(BLOCKS_I):
        for block_j in range(BLOCKS_J):
            put(block_i, block_j, ROW_BITS, bits)

    sign_tables(cut_ref, string_ref, third_row, third_move, pair_ref, j_ref, fixed_ref, chosen_ref)

    def split(step):
        large[step].wait()
        flat = boundary_ref.at[step].reshape(2048, 32)
        for half in range(2):
            right = jnp.concatenate([flat[pl.ds(2 * half + one, 512, stride=4), :] for one in range(2)], axis=1)
            high_ref[2 * step + half], low_ref[2 * step + half] = split_high_low(right)

    def multiplied(step):
        values = []
        for half in range(2 * step, 2 * step + 2):
            by_high = dot(left_ref[...], high_ref[half])
            values.append(by_high[:32] + by_high[32:] + dot(left_ref[:32], low_ref[half]))
        for half in range(2):
            value = jnp.concatenate((values[half][:16], values[half][16:]), axis=1)
            for block_i in range(BLOCKS_I):
                put(block_i, 2 * step + half, ROW_FIRST, value[4 * block_i : 4 * block_i + 4])

    split(0)
    for step in range(1, 8):
        split(step)
        multiplied(step - 1)
    multiplied(7)


def select_kernel(chosen_ref, got_ref, out_ref, half_ref):
    rows = [got_ref[pl.ds(ROW_THIRD + row, 64, stride=PIECE), :] for row in range(4)]
    high, rest = split_high_rest(jnp.concatenate(rows, axis=0))
    middle, rest = split_high_rest(rest)
    chosen = chosen_ref[...]
    found = dot(chosen, high) + (dot(chosen, middle) + dot(chosen, rest.astype(jnp.bfloat16)))
    total = found[:64]
    for move in range(1, 4):
        total = total + pltpu.roll(found[64 * move : 64 * move + 64], 32 * move, 1)
    lane, value = lane_of((16, LANES)), total[:16]
    for four in range(1, 4):
        value = jnp.where(lane >= 32 * four, total[16 * four : 16 * four + 16], value)
    for to in range(16):
        out_ref[to] = value
    for source in range(64):
        half_ref[8 * source : 8 * source + 8, :] = got_ref[PIECE * source : PIECE * source + 8, :]


def inner_kernel(row_vmem, pair_ref, j_ref, string_ref, got_ref, mine_ref, theirs_ref, same_ref, other_ref, pairs_ref, allowed_ref, fixed_ref, sum_ref, whole_ref, second_ref, turned_ref, by_same_ref, by_other_ref, even_ref, odd_ref, row_ref, row_sem):
    to_smem = pltpu.make_async_copy(row_vmem, row_ref, row_sem)
    to_smem.start()
    lane = lane_of((1, LANES))
    signs = 1.0 - 2.0 * got_ref[pl.ds(ROW_BITS, 64, stride=PIECE), :]
    signs = jnp.where(lane < 6, signs, jnp.where(lane == 6, 1.0, 0.0)).astype(jnp.bfloat16)

    def one_if_all(differing, kind):
        return jnp.where(differing == 0.0, 1.0, 0.0).astype(kind)

    def against_slices(table):
        return lax.dot_general(table, signs, (((1,), (1,)), ((), ())), preferred_element_type=jnp.float32)

    fixed_ref[...] = one_if_all(against_slices(string_ref[...].astype(jnp.bfloat16)), jnp.float32)
    pairs_ref[...] = one_if_all(against_slices(pair_ref[...]), jnp.bfloat16)
    allowed_ref[...] = one_if_all(dot(signs[:, :8], j_ref[...].astype(jnp.bfloat16)), jnp.bfloat16)

    core = lax.axis_index(CORES)
    for ref, half in ((mine_ref, core), (theirs_ref, 1 - core)):
        for source in range(64):
            rows = ref[8 * source : 8 * source + 8, :]
            at = pl.ds(half * HALF + SPACED * source, 8)
            second_ref[at, :] = rows
            turned_ref[at, :] = pltpu.roll(rows, 64, 1)
    low = lane_of((8, LANES)) < 64
    for g0 in range(32):
        start = 2 * g0 * PIECE + ROW_FIRST
        first = jnp.concatenate((got_ref[start : start + 4, :], got_ref[start + PIECE : start + PIECE + 4, :]), axis=0)
        turned = pltpu.roll(first, 64, 1)
        by_same_ref[8 * g0 : 8 * g0 + 8, :] = jnp.where(low, first, turned)
        by_other_ref[8 * g0 : 8 * g0 + 8, :] = jnp.where(low, -turned, first)

    def counted(count_ref, b, inside):
        row_b = fixed_ref[pl.ds(b, 1), :].astype(jnp.bfloat16)
        count_ref[256 * inside : 256 * inside + 256, :] = dot(pairs_ref[...] * row_b, allowed_ref[...])

    def summed(count_ref, b, inside):
        start = row_ref[1, b]
        eight = pl.ds(pl.multiple_of(row_ref[0, b], 8), 8)
        by_same, by_other = by_same_ref[eight, :], by_other_ref[eight, :]
        second = second_ref[pl.ds(start, 32, stride=2 * SPACED), :]
        other = turned_ref[pl.ds(start, 32, stride=2 * SPACED), :]
        for h in range(2):
            terms = []
            for e in range(4):
                q = 4 * h + e
                term = by_same[q : q + 1] * second + by_other[q : q + 1] * other
                terms.append(term * count_ref[256 * inside + 32 * q : 256 * inside + 32 * q + 32, :])
            columns = jnp.concatenate(terms, axis=0).T
            for part in range(2):
                total = jnp.sum(columns[64 * part : 64 * part + 64].reshape(8, 8, LANES), axis=0)
                sum_ref[2 * part + h, pl.ds(pl.multiple_of(8 * b, 8), 8), :] = total

    def several(base, carry):
        b = 2 * UNROLL * base
        for inside in range(UNROLL):
            counted(odd_ref, b + UNROLL + inside, inside)
            summed(even_ref, b + inside, inside)
        for inside in range(UNROLL):
            counted(even_ref, (b + 2 * UNROLL + inside) % 64, inside)
            summed(odd_ref, b + UNROLL + inside, inside)
        return carry

    for inside in range(UNROLL):
        counted(even_ref, inside, inside)
    to_smem.wait()
    lax.fori_loop(0, 32 // UNROLL, several, 0)
    for part in range(2):
        for h in range(2):
            total = jnp.zeros((64, LANES), jnp.float32)
            for sublane in range(8):
                total += sum_ref[2 * part + h, pl.ds(sublane, 64, stride=8), :]
            whole_ref[2 * part + h] = total
    for h in range(2):
        parts = [whole_ref[2 * part + h, 16 * four : 16 * four + 16] for four in range(4) for part in range(2)]
        for group in range(8):
            value = regrouped(parts, group)
            imag = (lane_of(value.shape) & 16) != 0
            same_ref[8 * h + group] = jnp.where(imag, -value, value)
            other_ref[8 * h + group] = jnp.where(imag, pltpu.roll(value, 16, 1), pltpu.roll(value, LANES - 16, 1))


def outer_kernel(third_ref, same_ref, other_ref, out_ref):
    third = third_ref[...]
    real = jnp.sum(third * same_ref[...], axis=0)
    imag = jnp.sum(third * other_ref[...], axis=0)
    columns = jnp.concatenate((real, imag, jnp.zeros((96, LANES), jnp.float32)), axis=0).T
    sums = [jnp.sum(columns[32 * four : 32 * four + 32, :32], axis=0, keepdims=True) for four in range(4)]
    out_ref[...] = jnp.concatenate([x[:, :16] for x in sums] + [x[:, 16:] for x in sums], axis=1)


def on_device(boundary, gate_stack, layer_order, cut_index, slice_bits, bitstrings):
    smem = pl.BlockSpec(memory_space=pltpu.SMEM)
    vmem = pl.BlockSpec(memory_space=pltpu.VMEM)
    hbm = pl.BlockSpec(memory_space=pltpu.HBM)
    in_hbm = partial(pltpu.with_memory_space_constraint, memory_space=pltpu.HBM)
    strings = bitstrings.T
    pieces, rows, chosen, *tables = pl.pallas_call(
        pack_kernel,
        out_shape=(
            jax.ShapeDtypeStruct((64 * PIECE, LANES), jnp.float32),
            jax.ShapeDtypeStruct((8, 64), jnp.int32),
            jax.ShapeDtypeStruct((256, 256), jnp.bfloat16),
            jax.ShapeDtypeStruct((256, LANES), jnp.bfloat16),
            jax.ShapeDtypeStruct((8, LANES), jnp.float32),
            jax.ShapeDtypeStruct((64, LANES), jnp.float32),
        ),
        in_specs=[hbm] * 6,
        out_specs=(vmem,) * 6,
        scratch_shapes=[
            pltpu.SMEM((3,), jnp.int32),
            pltpu.SMEM((3, 6), jnp.int32),
            pltpu.SMEM((1, 6), jnp.int32),
            pltpu.VMEM((20, 64), jnp.int32),
            pltpu.VMEM((3, 2, 16, 1024), jnp.float32),
            pltpu.VMEM((8, 512, 4, 32), jnp.float32),
            pltpu.VMEM((64, 512), jnp.bfloat16),
            pltpu.VMEM((16, 512, 64), jnp.bfloat16),
            pltpu.VMEM((16, 512, 64), jnp.bfloat16),
            pltpu.SemaphoreType.DMA((13,)),
        ],
        compiler_params=pltpu.CompilerParams(vmem_limit_bytes=24 << 20),
        name="pack",
    )(*(in_hbm(x) for x in (layer_order, cut_index.T, slice_bits, strings, gate_stack, boundary.reshape(512, 32, 32))))
    pieces = pieces.reshape(64, 1, PIECE * LANES)
    got = lax.all_to_all(pieces, CUTS, 0, 0, tiled=True).reshape(64 * PIECE, LANES)
    third, mine = pl.pallas_call(
        select_kernel,
        out_shape=(
            jax.ShapeDtypeStruct((16, 16, LANES), jnp.float32),
            jax.ShapeDtypeStruct((512, LANES), jnp.float32),
        ),
        in_specs=[vmem, vmem],
        out_specs=(vmem, vmem),
        compiler_params=pltpu.CompilerParams(vmem_limit_bytes=8 << 20),
        name="select",
    )(chosen, got)
    theirs = lax.ppermute(mine, CORES, [(0, 1), (1, 0)])
    third = lax.all_to_all(third, WAVE, 0, 0, tiled=True)
    same, other = pl.pallas_call(
        inner_kernel,
        out_shape=(jax.ShapeDtypeStruct((16, 16, LANES), jnp.float32),) * 2,
        in_specs=[vmem] * 7,
        out_specs=(vmem, vmem),
        scratch_shapes=[
            pltpu.VMEM((256, 64), jnp.bfloat16),
            pltpu.VMEM((64, LANES), jnp.bfloat16),
            pltpu.VMEM((64, 64), jnp.float32),
            pltpu.VMEM((4, 512, LANES), jnp.float32),
            pltpu.VMEM((4, 64, LANES), jnp.float32),
            pltpu.VMEM((2 * HALF, LANES), jnp.float32),
            pltpu.VMEM((2 * HALF, LANES), jnp.float32),
            pltpu.VMEM((256, LANES), jnp.float32),
            pltpu.VMEM((256, LANES), jnp.float32),
            pltpu.VMEM((256 * UNROLL, LANES), jnp.float32),
            pltpu.VMEM((256 * UNROLL, LANES), jnp.float32),
            pltpu.SMEM((8, 64), jnp.int32),
            pltpu.SemaphoreType.DMA,
        ],
        compiler_params=pltpu.CompilerParams(vmem_limit_bytes=16 << 20),
        cost_estimate=pl.CostEstimate(flops=1 << 30, bytes_accessed=1 << 20, transcendentals=0),
        name="inner",
    )(rows, *tables, got, mine, theirs)
    partial_sums = pl.pallas_call(
        outer_kernel,
        out_shape=jax.ShapeDtypeStruct((1, LANES), jnp.float32),
        in_specs=[vmem, vmem, vmem],
        out_specs=vmem,
        compiler_params=pltpu.CompilerParams(vmem_limit_bytes=8 << 20),
        name="outer",
    )(third, same, other)
    chip_sums = partial_sums + lax.ppermute(partial_sums, CORES, [(0, 1), (1, 0)])
    copies = jnp.broadcast_to(chip_sums[None], (lax.axis_size(CHIPS), 1, LANES))
    total = jnp.sum(lax.all_to_all(copies, CHIPS, 0, 0, tiled=True), axis=0)
    return total.reshape(2, 64).T


def solution(mesh):
    finer = Mesh(mesh.devices.reshape(AXES), CUTS + GRP)
    return jax.shard_map(
        on_device,
        mesh=finer,
        in_specs=(
            P(GRP, None, None, None, None),
            P(None, None, CUTS, None),
            P(),
            P(),
            P(CUTS, None),
            P(),
        ),
        out_specs=P(),
        check_vma=False,
    )
```

```python
from functools import partial

import jax
import jax.numpy as jnp
from jax import lax
from jax.experimental import pallas as pl
from jax.experimental.pallas import tpu as pltpu
from jax.sharding import Mesh
from jax.sharding import PartitionSpec as P

AXES = (2, 2, 2, 2, 2, 2, 2, 2)
CUTS = ("cuts_0", "cuts_1", "cuts_2", "cuts_3", "cuts_4", "cuts_5")
GRP = ("grp_0", "grp_1")
WAVE = ("cuts_1", "cuts_2", "cuts_3", "cuts_4")
CORES = "cuts_5"
CHIPS = ("cuts_4", "cuts_2", "grp_0", "cuts_0", "grp_1", "cuts_3", "cuts_1")

BLOCKS_I, BLOCKS_J = 4, 16
LANES = 128
UNROLL = 8
ROW_SECOND, ROW_FIRST, ROW_THIRD, ROW_BITS, PIECE = 0, 8, 12, 16, 17
SPACED, HALF = 9, 64 * 9


def split_high_rest(array):
    high = array.astype(jnp.bfloat16)
    return high, array - high.astype(jnp.float32)


def split_high_low(array):
    high, rest = split_high_rest(array)
    return high, rest.astype(jnp.bfloat16)


def dot(left, right):
    return jnp.dot(left, right, preferred_element_type=jnp.float32)


def lane_of(shape):
    return lax.broadcasted_iota(jnp.int32, shape, 1)


def side_by_side(real, imag):
    low = lane_of(real.shape) < 64
    return jnp.where(low, real, pltpu.roll(imag, 64, 1)), jnp.where(low, pltpu.roll(real, 64, 1), imag)


def regrouped(parts, group):
    lane = lane_of(parts[0].shape)
    result = None
    for place, part in enumerate(parts):
        shift = 16 * (place - group) % LANES
        moved = pltpu.roll(part, shift, 1) if shift else part
        result = moved if place == 0 else jnp.where(lane >= 16 * place, moved, result)
    return result


def place_in_blocks():
    block_j = 0
    for axis in WAVE:
        block_j = block_j * 2 + lax.axis_index(axis)
    return 2 * lax.axis_index(CUTS[0]) + lax.axis_index(CORES), block_j


def sign_tables(cut_ref, string_ref, third_row, third_move, pair_ref, j_ref, fixed_ref, chosen_ref):
    block_i, block_j = place_in_blocks()
    lane, sublane = lane_of((1, LANES)), lax.broadcasted_iota(jnp.int32, (8, 1), 0)
    zero_row, zero_column = jnp.zeros((1, LANES), jnp.int32), jnp.zeros((8, 1), jnp.int32)
    pair_on, pair_bit, pair_i1 = zero_row, zero_row, zero_row
    j_on, j_bit, j_j2 = zero_column, zero_column, zero_column
    pair_count, j_count, fixed_count = 0, 0, 0
    strings = jnp.zeros((8, 64), jnp.int32)
    for cut in range(6):
        layer, group, bit = cut_ref[0, cut], cut_ref[1, cut], cut_ref[2, cut]
        on_i1 = jnp.where((group == 1) & (layer < 2), 1, 0)
        on_i2 = jnp.where((group == 2) & (layer == 1), 1, 0)
        on_j2 = jnp.where((group == 2) & (layer == 0), 1, 0)
        on_j3 = jnp.where((group == 3) & (layer == 0), 1, 0)
        on_fixed = 1 - on_i1 - on_i2 - on_j2 - on_j3
        pair_on = jnp.where(lane == cut, on_i1 + on_i2, pair_on)
        pair_bit = jnp.where(lane == cut, bit, pair_bit)
        pair_i1 = jnp.where(lane == cut, on_i1, pair_i1)
        j_on = jnp.where(sublane == cut, on_j2 + on_j3, j_on)
        j_bit = jnp.where(sublane == cut, bit, j_bit)
        j_j2 = jnp.where(sublane == cut, on_j2, j_j2)
        pair_count, j_count, fixed_count = pair_count + on_i1 + on_i2, j_count + on_j2 + on_j3, fixed_count + on_fixed
        sign = on_fixed * (1 - 2 * string_ref[pl.ds(5 * group + bit, 1), :])
        strings = jnp.where(sublane == cut, sign, strings)

    row = lax.broadcasted_iota(jnp.int32, (256, 1), 0)
    i1 = 16 * (row >> 7) + 4 * block_i + ((row >> 5) & 3)
    index = jnp.where(pair_i1 != 0, i1, row & 31)
    signs = jnp.where(lane == 6, -pair_count, pair_on * (1 - 2 * ((index >> pair_bit) & 1)))
    pair_ref[...] = signs.astype(jnp.float32).astype(jnp.bfloat16)
    j = lane & 63
    index = jnp.where(j_j2 != 0, 2 * block_j + (j >> 5), j & 31)
    signs = jnp.where(sublane == 6, -j_count, j_on * (1 - 2 * ((index >> j_bit) & 1)))
    j_ref[...] = signs.astype(jnp.float32)
    strings = jnp.where(sublane == 6, -fixed_count, strings)
    strings = jnp.concatenate((strings, third_row, third_move), axis=0).astype(jnp.float32)
    strings = jnp.concatenate((strings, jnp.zeros((118, 64), jnp.float32)), axis=0)
    columns = jnp.concatenate((strings, jnp.zeros_like(strings)), axis=1).T[:64]
    fixed_ref[...] = columns
    hit = lane_of((64, 256)).astype(jnp.float32) == columns[:, 8:9]
    for move in range(4):
        one = jnp.where(hit & (columns[:, 9:10] == move), 1.0, 0.0)
        chosen_ref[64 * move : 64 * move + 64, :] = one.astype(jnp.bfloat16)


def pack_kernel(order_hbm, cut_hbm, bits_hbm, string_hbm, gate_hbm, boundary_hbm, piece_ref, row_ref, chosen_ref, pair_ref, j_ref, fixed_ref, order_ref, cut_ref, bits_ref, string_ref, gate_ref, boundary_ref, left_ref, high_ref, low_ref, sems):
    small = [
        pltpu.make_async_copy(order_hbm, order_ref, sems.at[0]),
        pltpu.make_async_copy(bits_hbm, bits_ref, sems.at[1]),
        pltpu.make_async_copy(string_hbm, string_ref, sems.at[2]),
        pltpu.make_async_copy(gate_hbm, gate_ref, sems.at[3]),
        pltpu.make_async_copy(cut_hbm, cut_ref, sems.at[4]),
    ]
    large = [
        pltpu.make_async_copy(boundary_hbm.at[:, pl.ds(4 * step, 4), :], boundary_ref.at[step], sems.at[5 + step])
        for step in range(8)
    ]
    for copy in small + large:
        copy.start()
    for copy in small:
        copy.wait()

    first, second, third = order_ref[0], order_ref[1], order_ref[2]
    member = lax.axis_index(GRP)
    columns = pl.ds(pl.multiple_of(member * 256, 256), 256)
    real, imag = gate_ref[first, 0, :, columns], gate_ref[first, 1, :, columns]

    def interleaved(even, odd):
        parts = []
        for k0 in range(8):
            parts += [even[:, 32 * k0 : 32 * k0 + 32], odd[:, 32 * k0 : 32 * k0 + 32]]
        return jnp.concatenate(parts, axis=1)

    left = jnp.concatenate((interleaved(real, -imag), interleaved(imag, real)), axis=0)
    high, low = split_high_low(left)
    left_ref[...] = jnp.concatenate((high, low), axis=0)

    strings = string_ref[...]

    def digit(group):
        total = strings[5 * group : 5 * group + 1]
        for bit in range(1, 5):
            total = total + (strings[5 * group + bit : 5 * group + bit + 1] << bit)
        return total

    g0, g1, g2, g3 = (digit(group) for group in range(4))
    row_ref[0:1, :] = 8 * g0
    row_ref[1:2, :] = ((g3 & 15) >> 3) * HALF + (g3 >> 4) * SPACED + (g3 & 7)
    third_row = (g2 & 3) * 64 + 2 * g1 + (g2 >> 4)
    third_move = ((lane_of((1, 64)) >> 4) - ((g2 & 15) >> 2)) & 3

    lane = lane_of((1, LANES))
    bits = jnp.zeros((1, LANES), jnp.float32)
    for cut in range(6):
        bits = jnp.where(lane == cut, bits_ref[0, cut].astype(jnp.float32), bits)

    def put(block_i, block_j, at, value):
        start = ((block_i // 2 * BLOCKS_J + block_j) * 2 + block_i % 2) * PIECE + at
        piece_ref[start : start + value.shape[0], :] = value

    for tile in range(8):
        lanes = slice(LANES * tile, LANES * tile + LANES)
        values = side_by_side(gate_ref[second, 0, :, lanes], gate_ref[second, 1, :, lanes])
        for half in range(2):
            for block_i in range(BLOCKS_I):
                eight = 8 * (block_i % 2)
                put(block_i, 2 * tile + half, ROW_SECOND, values[half][eight : eight + 8])
    for block_i in range(BLOCKS_I):
        parts = []
        for four in range(4):
            for part in range(2):
                rows = slice(4 * four, 4 * four + 4)
                parts.append(
                    jnp.concatenate(
                        [
                            gate_ref[third, part, rows, 512 * h + LANES * block_i : 512 * h + LANES * block_i + LANES]
                            for h in range(2)
                        ],
                        axis=0,
                    )
                )
        for group in range(8):
            value = regrouped(parts, group)
            put(block_i, group, ROW_THIRD, value[:4])
            put(block_i, 8 + group, ROW_THIRD, value[4:])
    for block_i in range(BLOCKS_I):
        for block_j in range(BLOCKS_J):
            put(block_i, block_j, ROW_BITS, bits)

    sign_tables(cut_ref, string_ref, third_row, third_move, pair_ref, j_ref, fixed_ref, chosen_ref)

    def split(step):
        large[step].wait()
        flat = boundary_ref.at[step].reshape(2048, 32)
        for half in range(2):
            right = jnp.concatenate([flat[pl.ds(2 * half + one, 512, stride=4), :] for one in range(2)], axis=1)
            high_ref[2 * step + half], low_ref[2 * step + half] = split_high_low(right)

    def multiplied(step):
        values = []
        for half in range(2 * step, 2 * step + 2):
            by_high = dot(left_ref[...], high_ref[half])
            values.append(by_high[:32] + by_high[32:] + dot(left_ref[:32], low_ref[half]))
        for half in range(2):
            value = jnp.concatenate((values[half][:16], values[half][16:]), axis=1)
            for block_i in range(BLOCKS_I):
                put(block_i, 2 * step + half, ROW_FIRST, value[4 * block_i : 4 * block_i + 4])

    split(0)
    for step in range(1, 8):
        split(step)
        multiplied(step - 1)
    multiplied(7)


def select_kernel(chosen_ref, got_ref, out_ref, half_ref):
    rows = [got_ref[pl.ds(ROW_THIRD + row, 64, stride=PIECE), :] for row in range(4)]
    high, rest = split_high_rest(jnp.concatenate(rows, axis=0))
    middle, rest = split_high_rest(rest)
    chosen = chosen_ref[...]
    found = dot(chosen, high) + (dot(chosen, middle) + dot(chosen, rest.astype(jnp.bfloat16)))
    total = found[:64]
    for move in range(1, 4):
        total = total + pltpu.roll(found[64 * move : 64 * move + 64], 32 * move, 1)
    lane, value = lane_of((16, LANES)), total[:16]
    for four in range(1, 4):
        value = jnp.where(lane >= 32 * four, total[16 * four : 16 * four + 16], value)
    for to in range(16):
        out_ref[to] = value
    for source in range(64):
        half_ref[8 * source : 8 * source + 8, :] = got_ref[PIECE * source : PIECE * source + 8, :]


def inner_kernel(row_vmem, pair_ref, j_ref, string_ref, got_ref, mine_ref, theirs_ref, same_ref, other_ref, pairs_ref, allowed_ref, fixed_ref, sum_ref, whole_ref, second_ref, turned_ref, by_same_ref, by_other_ref, even_ref, odd_ref, row_ref, row_sem):
    to_smem = pltpu.make_async_copy(row_vmem, row_ref, row_sem)
    to_smem.start()
    lane = lane_of((1, LANES))
    signs = 1.0 - 2.0 * got_ref[pl.ds(ROW_BITS, 64, stride=PIECE), :]
    signs = jnp.where(lane < 6, signs, jnp.where(lane == 6, 1.0, 0.0)).astype(jnp.bfloat16)

    def one_if_all(differing, kind):
        return jnp.where(differing == 0.0, 1.0, 0.0).astype(kind)

    def against_slices(table):
        return lax.dot_general(table, signs, (((1,), (1,)), ((), ())), preferred_element_type=jnp.float32)

    fixed_ref[...] = one_if_all(against_slices(string_ref[...].astype(jnp.bfloat16)), jnp.float32)
    pairs_ref[...] = one_if_all(against_slices(pair_ref[...]), jnp.bfloat16)
    allowed_ref[...] = one_if_all(dot(signs[:, :8], j_ref[...].astype(jnp.bfloat16)), jnp.bfloat16)

    core = lax.axis_index(CORES)
    for ref, half in ((mine_ref, core), (theirs_ref, 1 - core)):
        for source in range(64):
            rows = ref[8 * source : 8 * source + 8, :]
            at = pl.ds(half * HALF + SPACED * source, 8)
            second_ref[at, :] = rows
            turned_ref[at, :] = pltpu.roll(rows, 64, 1)
    low = lane_of((8, LANES)) < 64
    for g0 in range(32):
        start = 2 * g0 * PIECE + ROW_FIRST
        first = jnp.concatenate((got_ref[start : start + 4, :], got_ref[start + PIECE : start + PIECE + 4, :]), axis=0)
        turned = pltpu.roll(first, 64, 1)
        by_same_ref[8 * g0 : 8 * g0 + 8, :] = jnp.where(low, first, turned)
        by_other_ref[8 * g0 : 8 * g0 + 8, :] = jnp.where(low, -turned, first)

    def counted(count_ref, b, inside):
        row_b = fixed_ref[pl.ds(b, 1), :].astype(jnp.bfloat16)
        count_ref[256 * inside : 256 * inside + 256, :] = dot(pairs_ref[...] * row_b, allowed_ref[...])

    def summed(count_ref, b, inside):
        start = row_ref[1, b]
        eight = pl.ds(pl.multiple_of(row_ref[0, b], 8), 8)
        by_same, by_other = by_same_ref[eight, :], by_other_ref[eight, :]
        second = second_ref[pl.ds(start, 32, stride=2 * SPACED), :]
        other = turned_ref[pl.ds(start, 32, stride=2 * SPACED), :]
        for h in range(2):
            terms = []
            for e in range(4):
                q = 4 * h + e
                term = by_same[q : q + 1] * second + by_other[q : q + 1] * other
                terms.append(term * count_ref[256 * inside + 32 * q : 256 * inside + 32 * q + 32, :])
            columns = jnp.concatenate(terms, axis=0).T
            for part in range(2):
                total = jnp.sum(columns[64 * part : 64 * part + 64].reshape(8, 8, LANES), axis=0)
                sum_ref[2 * part + h, pl.ds(pl.multiple_of(8 * b, 8), 8), :] = total

    def several(base, carry):
        b = 2 * UNROLL * base
        for inside in range(UNROLL):
            counted(odd_ref, b + UNROLL + inside, inside)
            summed(even_ref, b + inside, inside)
        for inside in range(UNROLL):
            counted(even_ref, (b + 2 * UNROLL + inside) % 64, inside)
            summed(odd_ref, b + UNROLL + inside, inside)
        return carry

    for inside in range(UNROLL):
        counted(even_ref, inside, inside)
    to_smem.wait()
    lax.fori_loop(0, 32 // UNROLL, several, 0)
    for part in range(2):
        for h in range(2):
            total = jnp.zeros((64, LANES), jnp.float32)
            for sublane in range(8):
                total += sum_ref[2 * part + h, pl.ds(sublane, 64, stride=8), :]
            whole_ref[2 * part + h] = total
    for h in range(2):
        parts = [whole_ref[2 * part + h, 16 * four : 16 * four + 16] for four in range(4) for part in range(2)]
        for group in range(8):
            value = regrouped(parts, group)
            imag = (lane_of(value.shape) & 16) != 0
            same_ref[8 * h + group] = jnp.where(imag, -value, value)
            other_ref[8 * h + group] = jnp.where(imag, pltpu.roll(value, 16, 1), pltpu.roll(value, LANES - 16, 1))


def outer_kernel(third_ref, same_ref, other_ref, out_ref):
    third = third_ref[...]
    real = jnp.sum(third * same_ref[...], axis=0)
    imag = jnp.sum(third * other_ref[...], axis=0)
    columns = jnp.concatenate((real, imag, jnp.zeros((96, LANES), jnp.float32)), axis=0).T
    sums = [jnp.sum(columns[32 * four : 32 * four + 32, :32], axis=0, keepdims=True) for four in range(4)]
    out_ref[...] = jnp.concatenate([x[:, :16] for x in sums] + [x[:, 16:] for x in sums], axis=1)


def on_device(boundary, gate_stack, layer_order, cut_index, slice_bits, bitstrings):
    smem = pl.BlockSpec(memory_space=pltpu.SMEM)
    vmem = pl.BlockSpec(memory_space=pltpu.VMEM)
    hbm = pl.BlockSpec(memory_space=pltpu.HBM)
    in_hbm = partial(pltpu.with_memory_space_constraint, memory_space=pltpu.HBM)
    strings = bitstrings.T
    pieces, rows, chosen, *tables = pl.pallas_call(
        pack_kernel,
        out_shape=(
            jax.ShapeDtypeStruct((64 * PIECE, LANES), jnp.float32),
            jax.ShapeDtypeStruct((8, 64), jnp.int32),
            jax.ShapeDtypeStruct((256, 256), jnp.bfloat16),
            jax.ShapeDtypeStruct((256, LANES), jnp.bfloat16),
            jax.ShapeDtypeStruct((8, LANES), jnp.float32),
            jax.ShapeDtypeStruct((64, LANES), jnp.float32),
        ),
        in_specs=[hbm] * 6,
        out_specs=(vmem,) * 6,
        scratch_shapes=[
            pltpu.SMEM((3,), jnp.int32),
            pltpu.SMEM((3, 6), jnp.int32),
            pltpu.SMEM((1, 6), jnp.int32),
            pltpu.VMEM((20, 64), jnp.int32),
            pltpu.VMEM((3, 2, 16, 1024), jnp.float32),
            pltpu.VMEM((8, 512, 4, 32), jnp.float32),
            pltpu.VMEM((64, 512), jnp.bfloat16),
            pltpu.VMEM((16, 512, 64), jnp.bfloat16),
            pltpu.VMEM((16, 512, 64), jnp.bfloat16),
            pltpu.SemaphoreType.DMA((13,)),
        ],
        compiler_params=pltpu.CompilerParams(vmem_limit_bytes=24 << 20),
        name="pack",
    )(*(in_hbm(x) for x in (layer_order, cut_index.T, slice_bits, strings, gate_stack, boundary.reshape(512, 32, 32))))
    pieces = pieces.reshape(64, 1, PIECE * LANES)
    got = lax.all_to_all(pieces, CUTS, 0, 0, tiled=True).reshape(64 * PIECE, LANES)
    third, mine = pl.pallas_call(
        select_kernel,
        out_shape=(
            jax.ShapeDtypeStruct((16, 16, LANES), jnp.float32),
            jax.ShapeDtypeStruct((512, LANES), jnp.float32),
        ),
        in_specs=[vmem, vmem],
        out_specs=(vmem, vmem),
        compiler_params=pltpu.CompilerParams(vmem_limit_bytes=8 << 20),
        name="select",
    )(chosen, got)
    theirs = lax.ppermute(mine, CORES, [(0, 1), (1, 0)])
    third = lax.all_to_all(third, WAVE, 0, 0, tiled=True)
    same, other = pl.pallas_call(
        inner_kernel,
        out_shape=(jax.ShapeDtypeStruct((16, 16, LANES), jnp.float32),) * 2,
        in_specs=[vmem] * 7,
        out_specs=(vmem, vmem),
        scratch_shapes=[
            pltpu.VMEM((256, 64), jnp.bfloat16),
            pltpu.VMEM((64, LANES), jnp.bfloat16),
            pltpu.VMEM((64, 64), jnp.float32),
            pltpu.VMEM((4, 512, LANES), jnp.float32),
            pltpu.VMEM((4, 64, LANES), jnp.float32),
            pltpu.VMEM((2 * HALF, LANES), jnp.float32),
            pltpu.VMEM((2 * HALF, LANES), jnp.float32),
            pltpu.VMEM((256, LANES), jnp.float32),
            pltpu.VMEM((256, LANES), jnp.float32),
            pltpu.VMEM((256 * UNROLL, LANES), jnp.float32),
            pltpu.VMEM((256 * UNROLL, LANES), jnp.float32),
            pltpu.SMEM((8, 64), jnp.int32),
            pltpu.SemaphoreType.DMA,
        ],
        compiler_params=pltpu.CompilerParams(vmem_limit_bytes=16 << 20),
        cost_estimate=pl.CostEstimate(flops=1 << 30, bytes_accessed=1 << 20, transcendentals=0),
        name="inner",
    )(rows, *tables, got, mine, theirs)
    partial_sums = pl.pallas_call(
        outer_kernel,
        out_shape=jax.ShapeDtypeStruct((1, LANES), jnp.float32),
        in_specs=[vmem, vmem, vmem],
        out_specs=vmem,
        compiler_params=pltpu.CompilerParams(vmem_limit_bytes=8 << 20),
        name="outer",
    )(third, same, other)
    chip_sums = partial_sums + lax.ppermute(partial_sums, CORES, [(0, 1), (1, 0)])
    copies = jnp.broadcast_to(chip_sums[None], (lax.axis_size(CHIPS), 1, LANES))
    total = jnp.sum(lax.all_to_all(copies, CHIPS, 0, 0, tiled=True), axis=0)
    return total.reshape(2, 64).T


def solution(mesh):
    finer = Mesh(mesh.devices.reshape(AXES), CUTS + GRP)
    return jax.shard_map(
        on_device,
        mesh=finer,
        in_specs=(
            P(GRP, None, None, None, None),
            P(None, None, CUTS, None),
            P(),
            P(),
            P(CUTS, None),
            P(),
        ),
        out_specs=P(),
        check_vma=False,
    )
```

```python
from functools import partial

import jax
import jax.numpy as jnp
from jax import lax
from jax.experimental import pallas as pl
from jax.experimental.pallas import tpu as pltpu
from jax.sharding import Mesh
from jax.sharding import PartitionSpec as P

AXES = (2, 2, 2, 2, 2, 2, 2, 2)
CUTS = ("cuts_0", "cuts_1", "cuts_2", "cuts_3", "cuts_4", "cuts_5")
GRP = ("grp_0", "grp_1")
WAVE = ("cuts_1", "cuts_2", "cuts_3", "cuts_4")
CORES = "cuts_5"
CHIPS = ("cuts_4", "cuts_2", "grp_0", "cuts_0", "grp_1", "cuts_1", "cuts_3")

BLOCKS_I, BLOCKS_J = 4, 16
LANES = 128
UNROLL = 8
ROW_SECOND, ROW_FIRST, ROW_THIRD, ROW_BITS, PIECE = 0, 8, 12, 16, 17
SPACED, HALF = 9, 64 * 9


def split_high_rest(array):
    high = array.astype(jnp.bfloat16)
    return high, array - high.astype(jnp.float32)


def split_high_low(array):
    high, rest = split_high_rest(array)
    return high, rest.astype(jnp.bfloat16)


def dot(left, right):
    return jnp.dot(left, right, preferred_element_type=jnp.float32)


def lane_of(shape):
    return lax.broadcasted_iota(jnp.int32, shape, 1)


def side_by_side(real, imag):
    low = lane_of(real.shape) < 64
    return jnp.where(low, real, pltpu.roll(imag, 64, 1)), jnp.where(low, pltpu.roll(real, 64, 1), imag)


def regrouped(parts, group):
    lane = lane_of(parts[0].shape)
    result = None
    for place, part in enumerate(parts):
        shift = 16 * (place - group) % LANES
        moved = pltpu.roll(part, shift, 1) if shift else part
        result = moved if place == 0 else jnp.where(lane >= 16 * place, moved, result)
    return result


def place_in_blocks():
    block_j = 0
    for axis in WAVE:
        block_j = block_j * 2 + lax.axis_index(axis)
    return 2 * lax.axis_index(CUTS[0]) + lax.axis_index(CORES), block_j


def sign_tables(cut_ref, string_ref, third_row, third_move, pair_ref, j_ref, fixed_ref, chosen_ref):
    block_i, block_j = place_in_blocks()
    lane, sublane = lane_of((1, LANES)), lax.broadcasted_iota(jnp.int32, (8, 1), 0)
    zero_row, zero_column = jnp.zeros((1, LANES), jnp.int32), jnp.zeros((8, 1), jnp.int32)
    pair_on, pair_bit, pair_i1 = zero_row, zero_row, zero_row
    j_on, j_bit, j_j2 = zero_column, zero_column, zero_column
    pair_count, j_count, fixed_count = 0, 0, 0
    strings = jnp.zeros((8, 64), jnp.int32)
    for cut in range(6):
        layer, group, bit = cut_ref[0, cut], cut_ref[1, cut], cut_ref[2, cut]
        on_i1 = jnp.where((group == 1) & (layer < 2), 1, 0)
        on_i2 = jnp.where((group == 2) & (layer == 1), 1, 0)
        on_j2 = jnp.where((group == 2) & (layer == 0), 1, 0)
        on_j3 = jnp.where((group == 3) & (layer == 0), 1, 0)
        on_fixed = 1 - on_i1 - on_i2 - on_j2 - on_j3
        pair_on = jnp.where(lane == cut, on_i1 + on_i2, pair_on)
        pair_bit = jnp.where(lane == cut, bit, pair_bit)
        pair_i1 = jnp.where(lane == cut, on_i1, pair_i1)
        j_on = jnp.where(sublane == cut, on_j2 + on_j3, j_on)
        j_bit = jnp.where(sublane == cut, bit, j_bit)
        j_j2 = jnp.where(sublane == cut, on_j2, j_j2)
        pair_count, j_count, fixed_count = pair_count + on_i1 + on_i2, j_count + on_j2 + on_j3, fixed_count + on_fixed
        sign = on_fixed * (1 - 2 * string_ref[pl.ds(5 * group + bit, 1), :])
        strings = jnp.where(sublane == cut, sign, strings)

    row = lax.broadcasted_iota(jnp.int32, (256, 1), 0)
    i1 = 16 * (row >> 7) + 4 * block_i + ((row >> 5) & 3)
    index = jnp.where(pair_i1 != 0, i1, row & 31)
    signs = jnp.where(lane == 6, -pair_count, pair_on * (1 - 2 * ((index >> pair_bit) & 1)))
    pair_ref[...] = signs.astype(jnp.float32).astype(jnp.bfloat16)
    j = lane & 63
    index = jnp.where(j_j2 != 0, 2 * block_j + (j >> 5), j & 31)
    signs = jnp.where(sublane == 6, -j_count, j_on * (1 - 2 * ((index >> j_bit) & 1)))
    j_ref[...] = signs.astype(jnp.float32)
    strings = jnp.where(sublane == 6, -fixed_count, strings)
    strings = jnp.concatenate((strings, third_row, third_move), axis=0).astype(jnp.float32)
    strings = jnp.concatenate((strings, jnp.zeros((118, 64), jnp.float32)), axis=0)
    columns = jnp.concatenate((strings, jnp.zeros_like(strings)), axis=1).T[:64]
    fixed_ref[...] = columns
    hit = lane_of((64, 256)).astype(jnp.float32) == columns[:, 8:9]
    for move in range(4):
        one = jnp.where(hit & (columns[:, 9:10] == move), 1.0, 0.0)
        chosen_ref[64 * move : 64 * move + 64, :] = one.astype(jnp.bfloat16)


def pack_kernel(order_hbm, cut_hbm, bits_hbm, string_hbm, gate_hbm, boundary_hbm, piece_ref, row_ref, chosen_ref, pair_ref, j_ref, fixed_ref, order_ref, cut_ref, bits_ref, string_ref, gate_ref, boundary_ref, left_ref, high_ref, low_ref, sems):
    small = [
        pltpu.make_async_copy(order_hbm, order_ref, sems.at[0]),
        pltpu.make_async_copy(bits_hbm, bits_ref, sems.at[1]),
        pltpu.make_async_copy(string_hbm, string_ref, sems.at[2]),
        pltpu.make_async_copy(gate_hbm, gate_ref, sems.at[3]),
        pltpu.make_async_copy(cut_hbm, cut_ref, sems.at[4]),
    ]
    large = [
        pltpu.make_async_copy(boundary_hbm.at[:, pl.ds(4 * step, 4), :], boundary_ref.at[step], sems.at[5 + step])
        for step in range(8)
    ]
    for copy in small + large:
        copy.start()
    for copy in small:
        copy.wait()

    first, second, third = order_ref[0], order_ref[1], order_ref[2]
    member = lax.axis_index(GRP)
    columns = pl.ds(pl.multiple_of(member * 256, 256), 256)
    real, imag = gate_ref[first, 0, :, columns], gate_ref[first, 1, :, columns]

    def interleaved(even, odd):
        parts = []
        for k0 in range(8):
            parts += [even[:, 32 * k0 : 32 * k0 + 32], odd[:, 32 * k0 : 32 * k0 + 32]]
        return jnp.concatenate(parts, axis=1)

    left = jnp.concatenate((interleaved(real, -imag), interleaved(imag, real)), axis=0)
    high, low = split_high_low(left)
    left_ref[...] = jnp.concatenate((high, low), axis=0)

    strings = string_ref[...]

    def digit(group):
        total = strings[5 * group : 5 * group + 1]
        for bit in range(1, 5):
            total = total + (strings[5 * group + bit : 5 * group + bit + 1] << bit)
        return total

    g0, g1, g2, g3 = (digit(group) for group in range(4))
    row_ref[0:1, :] = 8 * g0
    row_ref[1:2, :] = ((g3 & 15) >> 3) * HALF + (g3 >> 4) * SPACED + (g3 & 7)
    third_row = (g2 & 3) * 64 + 2 * g1 + (g2 >> 4)
    third_move = ((lane_of((1, 64)) >> 4) - ((g2 & 15) >> 2)) & 3

    lane = lane_of((1, LANES))
    bits = jnp.zeros((1, LANES), jnp.float32)
    for cut in range(6):
        bits = jnp.where(lane == cut, bits_ref[0, cut].astype(jnp.float32), bits)

    def put(block_i, block_j, at, value):
        start = ((block_i // 2 * BLOCKS_J + block_j) * 2 + block_i % 2) * PIECE + at
        piece_ref[start : start + value.shape[0], :] = value

    for tile in range(8):
        lanes = slice(LANES * tile, LANES * tile + LANES)
        values = side_by_side(gate_ref[second, 0, :, lanes], gate_ref[second, 1, :, lanes])
        for half in range(2):
            for block_i in range(BLOCKS_I):
                eight = 8 * (block_i % 2)
                put(block_i, 2 * tile + half, ROW_SECOND, values[half][eight : eight + 8])
    for block_i in range(BLOCKS_I):
        parts = []
        for four in range(4):
            for part in range(2):
                rows = slice(4 * four, 4 * four + 4)
                parts.append(
                    jnp.concatenate(
                        [
                            gate_ref[third, part, rows, 512 * h + LANES * block_i : 512 * h + LANES * block_i + LANES]
                            for h in range(2)
                        ],
                        axis=0,
                    )
                )
        for group in range(8):
            value = regrouped(parts, group)
            put(block_i, group, ROW_THIRD, value[:4])
            put(block_i, 8 + group, ROW_THIRD, value[4:])
    for block_i in range(BLOCKS_I):
        for block_j in range(BLOCKS_J):
            put(block_i, block_j, ROW_BITS, bits)

    sign_tables(cut_ref, string_ref, third_row, third_move, pair_ref, j_ref, fixed_ref, chosen_ref)

    def split(step):
        large[step].wait()
        flat = boundary_ref.at[step].reshape(2048, 32)
        for half in range(2):
            right = jnp.concatenate([flat[pl.ds(2 * half + one, 512, stride=4), :] for one in range(2)], axis=1)
            high_ref[2 * step + half], low_ref[2 * step + half] = split_high_low(right)

    def multiplied(step):
        values = []
        for half in range(2 * step, 2 * step + 2):
            by_high = dot(left_ref[...], high_ref[half])
            values.append(by_high[:32] + by_high[32:] + dot(left_ref[:32], low_ref[half]))
        for half in range(2):
            value = jnp.concatenate((values[half][:16], values[half][16:]), axis=1)
            for block_i in range(BLOCKS_I):
                put(block_i, 2 * step + half, ROW_FIRST, value[4 * block_i : 4 * block_i + 4])

    split(0)
    for step in range(1, 8):
        split(step)
        multiplied(step - 1)
    multiplied(7)


def select_kernel(chosen_ref, got_ref, out_ref, half_ref):
    rows = [got_ref[pl.ds(ROW_THIRD + row, 64, stride=PIECE), :] for row in range(4)]
    high, rest = split_high_rest(jnp.concatenate(rows, axis=0))
    middle, rest = split_high_rest(rest)
    chosen = chosen_ref[...]
    found = dot(chosen, high) + (dot(chosen, middle) + dot(chosen, rest.astype(jnp.bfloat16)))
    total = found[:64]
    for move in range(1, 4):
        total = total + pltpu.roll(found[64 * move : 64 * move + 64], 32 * move, 1)
    lane, value = lane_of((16, LANES)), total[:16]
    for four in range(1, 4):
        value = jnp.where(lane >= 32 * four, total[16 * four : 16 * four + 16], value)
    for to in range(16):
        out_ref[to] = value
    for source in range(64):
        half_ref[8 * source : 8 * source + 8, :] = got_ref[PIECE * source : PIECE * source + 8, :]


def inner_kernel(row_vmem, pair_ref, j_ref, string_ref, got_ref, mine_ref, theirs_ref, same_ref, other_ref, pairs_ref, allowed_ref, fixed_ref, sum_ref, whole_ref, second_ref, turned_ref, by_same_ref, by_other_ref, even_ref, odd_ref, row_ref, row_sem):
    to_smem = pltpu.make_async_copy(row_vmem, row_ref, row_sem)
    to_smem.start()
    lane = lane_of((1, LANES))
    signs = 1.0 - 2.0 * got_ref[pl.ds(ROW_BITS, 64, stride=PIECE), :]
    signs = jnp.where(lane < 6, signs, jnp.where(lane == 6, 1.0, 0.0)).astype(jnp.bfloat16)

    def one_if_all(differing, kind):
        return jnp.where(differing == 0.0, 1.0, 0.0).astype(kind)

    def against_slices(table):
        return lax.dot_general(table, signs, (((1,), (1,)), ((), ())), preferred_element_type=jnp.float32)

    fixed_ref[...] = one_if_all(against_slices(string_ref[...].astype(jnp.bfloat16)), jnp.float32)
    pairs_ref[...] = one_if_all(against_slices(pair_ref[...]), jnp.bfloat16)
    allowed_ref[...] = one_if_all(dot(signs[:, :8], j_ref[...].astype(jnp.bfloat16)), jnp.bfloat16)

    core = lax.axis_index(CORES)
    for ref, half in ((mine_ref, core), (theirs_ref, 1 - core)):
        for source in range(64):
            rows = ref[8 * source : 8 * source + 8, :]
            at = pl.ds(half * HALF + SPACED * source, 8)
            second_ref[at, :] = rows
            turned_ref[at, :] = pltpu.roll(rows, 64, 1)
    low = lane_of((8, LANES)) < 64
    for g0 in range(32):
        start = 2 * g0 * PIECE + ROW_FIRST
        first = jnp.concatenate((got_ref[start : start + 4, :], got_ref[start + PIECE : start + PIECE + 4, :]), axis=0)
        turned = pltpu.roll(first, 64, 1)
        by_same_ref[8 * g0 : 8 * g0 + 8, :] = jnp.where(low, first, turned)
        by_other_ref[8 * g0 : 8 * g0 + 8, :] = jnp.where(low, -turned, first)

    def counted(count_ref, b, inside):
        row_b = fixed_ref[pl.ds(b, 1), :].astype(jnp.bfloat16)
        count_ref[256 * inside : 256 * inside + 256, :] = dot(pairs_ref[...] * row_b, allowed_ref[...])

    def summed(count_ref, b, inside):
        start = row_ref[1, b]
        eight = pl.ds(pl.multiple_of(row_ref[0, b], 8), 8)
        by_same, by_other = by_same_ref[eight, :], by_other_ref[eight, :]
        second = second_ref[pl.ds(start, 32, stride=2 * SPACED), :]
        other = turned_ref[pl.ds(start, 32, stride=2 * SPACED), :]
        for h in range(2):
            terms = []
            for e in range(4):
                q = 4 * h + e
                term = by_same[q : q + 1] * second + by_other[q : q + 1] * other
                terms.append(term * count_ref[256 * inside + 32 * q : 256 * inside + 32 * q + 32, :])
            columns = jnp.concatenate(terms, axis=0).T
            for part in range(2):
                total = jnp.sum(columns[64 * part : 64 * part + 64].reshape(8, 8, LANES), axis=0)
                sum_ref[2 * part + h, pl.ds(pl.multiple_of(8 * b, 8), 8), :] = total

    def several(base, carry):
        b = 2 * UNROLL * base
        for inside in range(UNROLL):
            counted(odd_ref, b + UNROLL + inside, inside)
            summed(even_ref, b + inside, inside)
        for inside in range(UNROLL):
            counted(even_ref, (b + 2 * UNROLL + inside) % 64, inside)
            summed(odd_ref, b + UNROLL + inside, inside)
        return carry

    for inside in range(UNROLL):
        counted(even_ref, inside, inside)
    to_smem.wait()
    lax.fori_loop(0, 32 // UNROLL, several, 0)
    for part in range(2):
        for h in range(2):
            total = jnp.zeros((64, LANES), jnp.float32)
            for sublane in range(8):
                total += sum_ref[2 * part + h, pl.ds(sublane, 64, stride=8), :]
            whole_ref[2 * part + h] = total
    for h in range(2):
        parts = [whole_ref[2 * part + h, 16 * four : 16 * four + 16] for four in range(4) for part in range(2)]
        for group in range(8):
            value = regrouped(parts, group)
            imag = (lane_of(value.shape) & 16) != 0
            same_ref[8 * h + group] = jnp.where(imag, -value, value)
            other_ref[8 * h + group] = jnp.where(imag, pltpu.roll(value, 16, 1), pltpu.roll(value, LANES - 16, 1))


def outer_kernel(third_ref, same_ref, other_ref, out_ref):
    third = third_ref[...]
    real = jnp.sum(third * same_ref[...], axis=0)
    imag = jnp.sum(third * other_ref[...], axis=0)
    columns = jnp.concatenate((real, imag, jnp.zeros((96, LANES), jnp.float32)), axis=0).T
    sums = [jnp.sum(columns[32 * four : 32 * four + 32, :32], axis=0, keepdims=True) for four in range(4)]
    out_ref[...] = jnp.concatenate([x[:, :16] for x in sums] + [x[:, 16:] for x in sums], axis=1)


def on_device(boundary, gate_stack, layer_order, cut_index, slice_bits, bitstrings):
    smem = pl.BlockSpec(memory_space=pltpu.SMEM)
    vmem = pl.BlockSpec(memory_space=pltpu.VMEM)
    hbm = pl.BlockSpec(memory_space=pltpu.HBM)
    in_hbm = partial(pltpu.with_memory_space_constraint, memory_space=pltpu.HBM)
    strings = bitstrings.T
    pieces, rows, chosen, *tables = pl.pallas_call(
        pack_kernel,
        out_shape=(
            jax.ShapeDtypeStruct((64 * PIECE, LANES), jnp.float32),
            jax.ShapeDtypeStruct((8, 64), jnp.int32),
            jax.ShapeDtypeStruct((256, 256), jnp.bfloat16),
            jax.ShapeDtypeStruct((256, LANES), jnp.bfloat16),
            jax.ShapeDtypeStruct((8, LANES), jnp.float32),
            jax.ShapeDtypeStruct((64, LANES), jnp.float32),
        ),
        in_specs=[hbm] * 6,
        out_specs=(vmem,) * 6,
        scratch_shapes=[
            pltpu.SMEM((3,), jnp.int32),
            pltpu.SMEM((3, 6), jnp.int32),
            pltpu.SMEM((1, 6), jnp.int32),
            pltpu.VMEM((20, 64), jnp.int32),
            pltpu.VMEM((3, 2, 16, 1024), jnp.float32),
            pltpu.VMEM((8, 512, 4, 32), jnp.float32),
            pltpu.VMEM((64, 512), jnp.bfloat16),
            pltpu.VMEM((16, 512, 64), jnp.bfloat16),
            pltpu.VMEM((16, 512, 64), jnp.bfloat16),
            pltpu.SemaphoreType.DMA((13,)),
        ],
        compiler_params=pltpu.CompilerParams(vmem_limit_bytes=24 << 20),
        name="pack",
    )(*(in_hbm(x) for x in (layer_order, cut_index.T, slice_bits, strings, gate_stack, boundary.reshape(512, 32, 32))))
    pieces = pieces.reshape(64, 1, PIECE * LANES)
    got = lax.all_to_all(pieces, CUTS, 0, 0, tiled=True).reshape(64 * PIECE, LANES)
    third, mine = pl.pallas_call(
        select_kernel,
        out_shape=(
            jax.ShapeDtypeStruct((16, 16, LANES), jnp.float32),
            jax.ShapeDtypeStruct((512, LANES), jnp.float32),
        ),
        in_specs=[vmem, vmem],
        out_specs=(vmem, vmem),
        compiler_params=pltpu.CompilerParams(vmem_limit_bytes=8 << 20),
        name="select",
    )(chosen, got)
    theirs = lax.ppermute(mine, CORES, [(0, 1), (1, 0)])
    third = lax.all_to_all(third, WAVE, 0, 0, tiled=True)
    same, other = pl.pallas_call(
        inner_kernel,
        out_shape=(jax.ShapeDtypeStruct((16, 16, LANES), jnp.float32),) * 2,
        in_specs=[vmem] * 7,
        out_specs=(vmem, vmem),
        scratch_shapes=[
            pltpu.VMEM((256, 64), jnp.bfloat16),
            pltpu.VMEM((64, LANES), jnp.bfloat16),
            pltpu.VMEM((64, 64), jnp.float32),
            pltpu.VMEM((4, 512, LANES), jnp.float32),
            pltpu.VMEM((4, 64, LANES), jnp.float32),
            pltpu.VMEM((2 * HALF, LANES), jnp.float32),
            pltpu.VMEM((2 * HALF, LANES), jnp.float32),
            pltpu.VMEM((256, LANES), jnp.float32),
            pltpu.VMEM((256, LANES), jnp.float32),
            pltpu.VMEM((256 * UNROLL, LANES), jnp.float32),
            pltpu.VMEM((256 * UNROLL, LANES), jnp.float32),
            pltpu.SMEM((8, 64), jnp.int32),
            pltpu.SemaphoreType.DMA,
        ],
        compiler_params=pltpu.CompilerParams(vmem_limit_bytes=16 << 20),
        cost_estimate=pl.CostEstimate(flops=1 << 30, bytes_accessed=1 << 20, transcendentals=0),
        name="inner",
    )(rows, *tables, got, mine, theirs)
    partial_sums = pl.pallas_call(
        outer_kernel,
        out_shape=jax.ShapeDtypeStruct((1, LANES), jnp.float32),
        in_specs=[vmem, vmem, vmem],
        out_specs=vmem,
        compiler_params=pltpu.CompilerParams(vmem_limit_bytes=8 << 20),
        name="outer",
    )(third, same, other)
    chip_sums = partial_sums + lax.ppermute(partial_sums, CORES, [(0, 1), (1, 0)])
    copies = jnp.broadcast_to(chip_sums[None], (lax.axis_size(CHIPS), 1, LANES))
    total = jnp.sum(lax.all_to_all(copies, CHIPS, 0, 0, tiled=True), axis=0)
    return total.reshape(2, 64).T


def solution(mesh):
    finer = Mesh(mesh.devices.reshape(AXES), CUTS + GRP)
    return jax.shard_map(
        on_device,
        mesh=finer,
        in_specs=(
            P(GRP, None, None, None, None),
            P(None, None, CUTS, None),
            P(),
            P(),
            P(CUTS, None),
            P(),
        ),
        out_specs=P(),
        check_vma=False,
    )
```
